32 devices in a mesh: orig: 8 (over z, y), link: 4 (over x, core).
Axes of the slice: x: 2, y: 2, z: 4, core: 2. Of those that a mesh axis runs over, the one named last changes fastest.
Arguments:
- background: bfloat16 [16384, 256], P('orig'), may hold values from -6 to 6
- live_counts: int32 [128], P('orig'), may hold values from 1 to 128
- patterns: bfloat16 [4, 256, 128, 128], P('link', 'orig'), may hold values from -0.0390625 to 0.0390625
- pattern_ids: int32 [4, 128, 12], P('link', 'orig'), may hold values from 0 to 31
- link_targets: int32 [4, 128, 12], P('link', 'orig'), may hold values from 0 to 7
- counts_obs: float32 [4, 1024], P('link', 'orig'), may hold values from -6 to 6
- obs_var: float32 [4, 1024], P('link', 'orig'), may hold values from 1 to 10
Outputs:
- analysis: bfloat16 [16384, 256], P(('orig', 'link'))
The draws below stay inside these ranges and needn't reach their ends.
All inputs are finite; a program needn't handle non-finite values. Where the reference program divides by a largest or mean magnitude, that divisor is 1e-20 or more.
Results may differ from the reference program's by a relative error of at most 0.001.
Values sent between devices are 32-bit elements; how exact they have to be, the bound alone decides.
A program may use at most 64 MiB of HBM per device.

```python
import math
import jax
import jax.numpy as jnp
from jax import lax

M = 256
SB = 128
NB_DEV = 16
TPB = 12
NPAT_DEV = 32
LB = 128
NLB = 8
NS_ITERS = 4
BLOCKS = 128
STATES = 16384
PATTERNS = 256
LINKS = 1024
N_ORIG = 8
N_LINK = 4


def touch_ends(array, own_key, least, high):
    dims = array.shape
    index_at = [jax.random.randint(jax.random.fold_in(own_key, axis), (), 0, dims[axis]) for axis in range(len(dims))]
    array = array.at[tuple(index_at)].set(least)
    longest = dims.index(max(dims))
    index_at[longest] = (index_at[longest] + 1) % dims[longest]
    return array.at[tuple(index_at)].set(high)


def levels(stream_key, dims, shards, smallest, largest):
    loudness = 1.0
    for dim, shards_of in shards:
        draws = jax.random.uniform(jax.random.fold_in(jax.random.fold_in(stream_key, 6), dim), (shards_of,), jnp.float32, smallest / len(shards), largest / len(shards))
        loudness = loudness * jnp.repeat(jnp.exp(draws), dims[dim] // shards_of).reshape((-1,) + (1,) * (len(dims) - 1 - dim))
    return loudness


def noise(stream_key, shape, scale, bound, split=(), held_as=jnp.bfloat16):
    gain = levels(stream_key, shape, split, -0.22, 0.18) if split else 1.0
    result = jax.random.normal(stream_key, shape, jnp.float32) * scale * gain
    return jnp.minimum(jnp.maximum(result, -bound), bound).astype(held_as)


def setup_inputs(seed: int = 0) -> dict:
    splits = jax.random.split(jax.random.key(seed), 8)
    background = noise(splits[0], (STATES, M), 1.0, 6.0, ((0, 8),))
    live_counts = touch_ends(jax.random.randint(splits[1], (BLOCKS,), 1, SB + 1), jax.random.fold_in(splits[1], 1), 1, SB).astype(jnp.int32)
    patterns = noise(splits[2], (N_LINK, PATTERNS, LB, SB), (SB * TPB * NB_DEV * N_ORIG // NLB) ** -0.5, 0.0390625, ((0, 4), (1, 8)))
    pattern_ids = touch_ends(jax.random.randint(splits[3], (N_LINK, BLOCKS, TPB), 0, NPAT_DEV), jax.random.fold_in(splits[3], 1), 0, NPAT_DEV - 1).astype(jnp.int32)
    link_targets = touch_ends(jax.random.randint(splits[4], (N_LINK, BLOCKS, TPB), 0, NLB), jax.random.fold_in(splits[4], 1), 0, NLB - 1).astype(jnp.int32)
    counts_obs = noise(splits[5], (N_LINK, LINKS), 1.0, 6.0, ((0, 4), (1, 8)), jnp.float32)
    obs_var = jnp.clip(jnp.exp(math.log(10.0) - 2.3025851 * jax.random.uniform(splits[6], (N_LINK, LINKS), jnp.float32) ** levels(splits[6], (N_LINK, LINKS), ((0, 4), (1, 8)), -0.2, 0.2)), 1.0, 10.0)
    return dict(background=background, live_counts=live_counts, patterns=patterns, pattern_ids=pattern_ids, link_targets=link_targets, counts_obs=counts_obs, obs_var=obs_var)


def transform_of(ensemble_gram, forcing):
    members = ensemble_gram.shape[0]
    identity = jnp.eye(members, dtype=jnp.float32)
    system = identity + ensemble_gram / (members - 1.0)
    row_bound = jnp.max(lax.optimization_barrier(jnp.sum(jnp.abs(system), axis=1)))
    square_root = system / row_bound
    inverse = identity
    for sweep_index in range(NS_ITERS):
        middle = 0.5 * (3.0 * identity - jnp.dot(inverse, square_root, precision=lax.Precision.HIGHEST))
        square_root = jnp.dot(square_root, middle, precision=lax.Precision.HIGHEST)
        inverse = jnp.dot(middle, inverse, precision=lax.Precision.HIGHEST)
    spread_weights = inverse / jnp.sqrt(row_bound)
    inner = jnp.dot(inverse, forcing, precision=lax.Precision.HIGHEST)
    mean_weights = jnp.dot(inverse, inner, precision=lax.Precision.HIGHEST) / (row_bound * (members - 1.0))
    return spread_weights + mean_weights[:, None]

def group_predictions(group_index, masked, patterns, pattern_ids, link_targets):
    tile_bank = patterns[group_index]
    shard_states = masked.reshape(N_ORIG, NB_DEV, SB, M)
    shard_ids = pattern_ids[group_index].reshape(N_ORIG, NB_DEV, TPB)
    shard_targets = link_targets[group_index].reshape(N_ORIG, NB_DEV, TPB)
    block_numbers = jnp.arange(NLB, dtype=jnp.int32)

    def add_shard(running, inputs):
        shard_index, states_part, tile_ids, targets = inputs
        global_ids = (tile_ids + shard_index * NPAT_DEV).astype(jnp.int32)
        chosen = jnp.take(tile_bank, global_ids, axis=0).astype(jnp.float32)
        products = jnp.einsum('btls,bsm->btlm', chosen, states_part.astype(jnp.float32), precision=lax.Precision.HIGHEST)
        onehot = (targets[:, :, None] == block_numbers[None, None, :]).astype(jnp.float32)
        return (running + jnp.einsum('btj,btlm->jlm', onehot, products, precision=lax.Precision.HIGHEST), None)
    start = jnp.zeros((NLB, LB, M), jnp.float32)
    shard_numbers = jnp.arange(N_ORIG, dtype=jnp.int32)
    total, unused = lax.scan(add_shard, start, (shard_numbers, shard_states, shard_ids, shard_targets))
    return total.reshape(NLB * LB, M)

def reference(background, live_counts, patterns, pattern_ids, link_targets, counts_obs, obs_var):
    position = jnp.arange(SB, dtype=jnp.int32)
    living = position[None, :] < live_counts[:, None]
    masked = background.reshape(BLOCKS, SB, M) * living[:, :, None].astype(jnp.bfloat16)

    def one_group(group_index):
        return group_predictions(group_index, masked, patterns, pattern_ids, link_targets)
    predicted = lax.map(one_group, jnp.arange(N_LINK, dtype=jnp.int32))
    pred_mean = lax.optimization_barrier(jnp.mean(predicted, axis=2))
    spread = (predicted - pred_mean[:, :, None]).reshape(N_LINK * LINKS, M)
    weights = (1.0 / obs_var).reshape(N_LINK * LINKS)
    innovation = (counts_obs - pred_mean).reshape(N_LINK * LINKS)
    ensemble_gram = jnp.dot(spread.T, spread * weights[:, None], precision=lax.Precision.HIGHEST)
    forcing = jnp.dot(spread.T, weights * innovation, precision=lax.Precision.HIGHEST)
    transform_mat = transform_of(ensemble_gram, forcing)
    states_f = background.astype(jnp.float32)
    centre = lax.optimization_barrier(jnp.mean(states_f, axis=1, keepdims=True))
    updated = centre + jnp.dot(states_f - centre, transform_mat, precision=lax.Precision.HIGHEST)
    live_flat = living.reshape(STATES)
    return jnp.where(live_flat[:, None], updated, states_f).astype(jnp.bfloat16)
```

```python
import functools

import jax
import jax.numpy as jnp
from jax import lax
from jax.experimental import pallas as pl
from jax.experimental.pallas import tpu as pltpu
from jax.sharding import PartitionSpec as P

NS_ITERS = 4
CUTS = 4
UNROLL = 2
WIDE_GRANT = 67043328 - 900 * 1024
MESH = pl.DeviceIdType.MESH
F32 = jnp.float32
BF16 = jnp.bfloat16


def repeat(count, body):
    if count <= 16:
        for step in range(count):
            body(step)
    else:
        lax.fori_loop(0, count, lambda step, carry: (body(step), carry)[1], 0)


def xor(a, b, size):
    total = 0
    bit = 1
    while bit < size:
        total = total + ((a // bit) % 2 + (b // bit) % 2) % 2 * bit
        bit *= 2
    return total


def split(x):
    high = x.astype(BF16)
    return high, (x - high.astype(F32)).astype(BF16)


def mm3(a, b):
    a_high, a_low = split(a)
    b_high, b_low = split(b)
    return (
        jnp.dot(a_high, b_low, preferred_element_type=F32)
        + jnp.dot(a_low, b_high, preferred_element_type=F32)
    ) + jnp.dot(a_high, b_high, preferred_element_type=F32)


def sort_slots(ids_ref, targets_ref, words_ref, bits):
    slots = ids_ref.shape[0]
    blocks = ids_ref.shape[2]
    per_word = 31 // bits
    n_words = pl.cdiv(slots, per_word)

    def sort_block(block, carry):
        amounts = [targets_ref[slot, 0, block] * 4 for slot in range(slots)]
        ones = [jnp.left_shift(1, amount) for amount in amounts]
        tally = functools.reduce(lambda a, b: a + b, ones)
        starts = jnp.int32(0)
        for shift in range(1, 8):
            starts = starts + jnp.left_shift(tally, 4 * shift)
        place = starts
        words = [jnp.int32(0) for _ in range(n_words)]
        for slot in range(slots):
            rank = jnp.bitwise_and(jnp.right_shift(place, amounts[slot]), 15)
            place = place + ones[slot]
            tile = ids_ref[slot, 0, block]
            for word in range(n_words):
                local = rank - word * per_word
                inside = (local >= 0) & (local < per_word)
                shift = jnp.where(inside, local * bits, 0)
                words[word] = words[word] + jnp.where(inside, jnp.left_shift(tile, shift), 0)
        words_ref[0, block] = starts
        words_ref[1, block] = place
        for word in range(n_words):
            words_ref[2 + word, block] = words[word]
        return carry

    lax.fori_loop(0, blocks, sort_block, 0)


def predict_cut(words_ref, tiles_ref, states_ref, prefix_refs, term_ref, cut_index, cut_rows, slots, bits):
    link_rows, block_rows = tiles_ref.shape[1:]
    link_blocks = term_ref.shape[0] // link_rows
    per_word = 31 // bits
    span = len(prefix_refs)
    steps = states_ref.shape[0] // (span * block_rows)
    rows_at = pl.ds(cut_index * cut_rows, cut_rows)

    def add_step(step, carry):
        highs, lows = [], []
        for index, prefix_ref in enumerate(prefix_refs):
            block = step * span + index
            words = [words_ref[2 + word, block] for word in range(pl.cdiv(slots, per_word))]
            total = jnp.zeros((cut_rows, block_rows), F32)
            for slot in range(slots):
                shifted = jnp.right_shift(words[slot // per_word], slot % per_word * bits)
                tile = jnp.bitwise_and(shifted, 2**bits - 1)
                total = total + tiles_ref[tile, rows_at, :].astype(F32)
                prefix_ref[slot + 1, 0:cut_rows] = total
            starts, ends = words_ref[0, block], words_ref[1, block]
            high_parts, low_parts = [], []
            for target in range(link_blocks):
                first = jnp.bitwise_and(jnp.right_shift(starts, 4 * target), 15)
                last = jnp.bitwise_and(jnp.right_shift(ends, 4 * target), 15)
                high, low = split(prefix_ref[last, 0:cut_rows] - prefix_ref[first, 0:cut_rows])
                high_parts.append(high)
                low_parts.append(low)
            highs.append(jnp.concatenate(high_parts, axis=0))
            lows.append(jnp.concatenate(low_parts, axis=0))
        states = states_ref[pl.ds(pl.multiple_of(step * span * block_rows, span * block_rows), span * block_rows)]
        product = jnp.dot(jnp.concatenate(highs, axis=1), states, preferred_element_type=F32) + jnp.dot(
            jnp.concatenate(lows, axis=1), states, preferred_element_type=F32
        )
        for target in range(link_blocks):
            where = pl.ds(target * link_rows + cut_index * cut_rows, cut_rows)
            term_ref[where] = term_ref[where] + product[target * cut_rows : (target + 1) * cut_rows]
        return carry

    for target in range(link_blocks):
        term_ref[pl.ds(target * link_rows + cut_index * cut_rows, cut_rows)] = jnp.zeros(
            (cut_rows, term_ref.shape[1]), F32
        )
    lax.fori_loop(0, steps, add_step, 0, unroll=UNROLL)


def transform_of(gram, forcing):
    members = gram.shape[0]
    row = lax.broadcasted_iota(jnp.int32, (members, members), 0)
    column = lax.broadcasted_iota(jnp.int32, (members, members), 1)
    identity = (row == column).astype(F32)
    system = identity + gram * (1.0 / (members - 1.0))
    bound = jnp.max(jnp.sum(jnp.abs(system), axis=1, keepdims=True), axis=0, keepdims=True)
    root = system / bound
    middle = 1.5 * identity - 0.5 * root
    inverse = middle
    root = mm3(root, middle)
    for sweep in range(1, NS_ITERS):
        middle = 1.5 * identity - 0.5 * mm3(inverse, root)
        if sweep < NS_ITERS - 1:
            root = mm3(root, middle)
        inverse = mm3(middle, inverse)
    inner = mm3(jnp.broadcast_to(forcing, (8, members)), inverse)
    mean_weights = mm3(inner, inverse)[0:1] / (bound * (members - 1.0))
    whole = inverse / jnp.sqrt(bound) + jnp.broadcast_to(mean_weights, (members, members)).T
    return whole + (1.0 - jnp.sum(whole, axis=0, keepdims=True)) / members


def gram_kernel(
    n_orig, n_link, cuts, ids_ref, targets_ref, counts_ref, tiles_hbm, states_hbm, obs_ref, var_ref, out_ref,
    tiles_ref, states_ref, tiles_sem, states_sem, even_ref, odd_ref, words_ref, term_ref, first_in, sums, side_in, far_in, gram_ref, half_in, half_ref, piece_in, piece_ref, final_ref,
    send1, recv1, send2, recv2, send7, recv7, send3, recv3, send4, recv4, send5, recv5, send6, recv6,
):
    orig = lax.axis_index("orig")
    link = lax.axis_index("link")
    rows = obs_ref.shape[1]
    members = term_ref.shape[1]
    half = members // 2
    pairs = n_orig // 2
    parity = orig % 2
    place = orig // 2
    across = orig + 1 - 2 * parity
    side = link % 2
    twin = link + 1 - 2 * side
    ring = n_orig * n_link // 2
    rank = (link // 2) * n_orig + orig
    owners = min(ring, half // 8)
    piece = half // owners

    def device_of(other):
        return (other % n_orig, (other // n_orig) * 2 + side)

    load_states = pltpu.make_async_copy(states_hbm, states_ref, states_sem)
    load_states.start()
    load_tiles = pltpu.make_async_copy(tiles_hbm, tiles_ref, tiles_sem)
    load_tiles.start()
    near = place % 2
    far = place // 2
    n_far = pairs // 2
    barrier = pltpu.get_barrier_semaphore()

    def greet(other_orig, other_link):
        pl.semaphore_signal(barrier, inc=1, device_id=(other_orig, other_link), device_id_type=MESH)

    greet(across, link)
    greet(2 * (far * 2 + 1 - near) + parity, link)
    repeat(n_far - 1, lambda step: greet(2 * (xor(far, step + 1, n_far) * 2 + near) + parity, link))
    repeat(n_link - 1, lambda step: greet(orig, (link + step + 1) % n_link))

    slots = ids_ref.shape[0]
    blocks = counts_ref.shape[0]
    block_rows = states_ref.shape[0] // blocks
    bits = max(1, (tiles_ref.shape[0] - 1).bit_length())
    sort_slots(ids_ref, targets_ref, words_ref, bits)
    for prefix_ref in (even_ref, odd_ref):
        prefix_ref[...] = jnp.zeros(prefix_ref.shape, F32)
    position = lax.broadcasted_iota(jnp.int32, (block_rows, members), 0)
    load_states.wait()

    def mask_block(block, carry):
        where = pl.ds(pl.multiple_of(block * block_rows, block_rows), block_rows)
        states = states_ref[where]
        states_ref[where] = jnp.where(position < counts_ref[block], states, jnp.zeros_like(states))
        return carry

    lax.fori_loop(0, blocks, mask_block, 0, unroll=2)
    load_tiles.wait()

    cut_rows = rows // cuts
    steps = n_far * cuts

    def owner(step, flip):
        other = xor(far, n_far - 1 - step // cuts, n_far)
        return other * 2 + (near + flip) % 2

    def term_rows(index, step):
        return pl.ds(pl.multiple_of(index * rows + step % cuts * cut_rows, cut_rows), cut_rows)

    def cut(step):
        return pl.ds(pl.multiple_of(step % cuts * cut_rows, cut_rows), cut_rows)

    def slot(step, flip):
        return step // cuts * 2 + 1 - flip

    def first(step, flip):
        index = slot(step, flip) * cuts + step % cuts
        return pltpu.make_async_remote_copy(
            src_ref=term_ref.at[term_rows(2 * owner(step, flip) + 1 - parity, step)],
            dst_ref=first_in.at[slot(step, flip), cut(step)],
            send_sem=send1.at[index], recv_sem=recv1.at[index],
            device_id=(across, link), device_id_type=MESH,
        )

    def beside(step):
        return pltpu.make_async_remote_copy(
            src_ref=sums.at[slot(step, 1), cut(step)], dst_ref=side_in.at[step // cuts, cut(step)],
            send_sem=send2.at[step], recv_sem=recv2.at[step],
            device_id=(2 * (far * 2 + 1 - near) + parity, link), device_id_type=MESH,
        )

    def beyond(step):
        return pltpu.make_async_remote_copy(
            src_ref=sums.at[slot(step, 0), cut(step)], dst_ref=far_in.at[step // cuts, cut(step)],
            send_sem=send7.at[step], recv_sem=recv7.at[step],
            device_id=(2 * owner(step, 0) + parity, link), device_id_type=MESH,
        )

    remote = steps - cuts
    lag = min(2, remote, cuts)

    for index in range(cuts):
        predict_cut(
            words_ref, tiles_ref, states_ref, (even_ref, odd_ref), term_ref,
            index, tiles_ref.shape[1] // cuts, slots, bits,
        )
        if index == 0:
            pl.semaphore_wait(barrier, n_far + n_link)

        def first_start(step):
            first(step * cuts + index, 1).start()
            first(step * cuts + index, 0).start()

        repeat(n_far - 1, first_start)
    repeat(cuts, lambda step: first(step + remote, 1).start())
    repeat(cuts, lambda step: first(step + remote, 0).start())

    def add_first(step, flip):
        first(step, flip).wait_recv()
        sums[slot(step, flip), cut(step)] = (
            term_ref[term_rows(2 * owner(step, flip) + parity, step)] + first_in[slot(step, flip), cut(step)]
        )
        if flip:
            beside(step).start()

    def add_beside(step):
        beside(step).wait_recv()
        sums[slot(step, 0), cut(step)] = sums[slot(step, 0), cut(step)] + side_in[step // cuts, cut(step)]

    def pass_on(step):
        add_beside(step)
        beyond(step).start()

    def enter(step):
        add_first(step, 1)
        add_first(step, 0)

    repeat(lag, enter)

    def middle_step(step):
        enter(step + lag)
        pass_on(step)

    repeat(remote - lag, middle_step)
    for step in range(cuts):
        add_first(step + remote, 1)
        if step < lag:
            pass_on(step + (remote - lag))
    for step in range(cuts):
        add_first(step + remote, 0)
        add_beside(step + remote)

    def gather(step):
        beyond(step).wait_recv()
        sums[pairs - 1, cut(step)] = sums[pairs - 1, cut(step)] + far_in[step // cuts, cut(step)]

    repeat(remote, gather)

    predicted = sums[pairs - 1]
    turned = predicted.T
    weights = 1.0 / var_ref[...]
    mean_row = jnp.sum(turned, axis=0, keepdims=True) / members
    spread = predicted - jnp.sum(predicted, axis=1, keepdims=True) / members
    spread_t = turned - mean_row
    gram_ref[...] = mm3(spread_t * weights, spread)
    pull = jnp.broadcast_to(weights * (obs_ref[...] - mean_row), (8, rows))
    forcing = mm3(pull, spread)
    gram_ref[pl.ds(half, 1), 0:half] = forcing[0:1, 0:half]
    gram_ref[pl.ds(half + 1, 1), 0:half] = forcing[0:1, half:]

    swap = pltpu.make_async_remote_copy(
        src_ref=gram_ref.at[pl.ds(pl.multiple_of((1 - side) * half, half), half)], dst_ref=half_in,
        send_sem=send3, recv_sem=recv3, device_id=(orig, twin), device_id_type=MESH,
    )
    swap.start()
    swap.wait_recv()
    half_ref[...] = gram_ref[pl.ds(pl.multiple_of(side * half, half), half)] + half_in[...]

    def scatter(step):
        other = xor(rank, ring - 1 - step, ring)
        return pltpu.make_async_remote_copy(
            src_ref=half_ref.at[pl.ds(pl.multiple_of(other * piece, piece), piece)], dst_ref=piece_in.at[step],
            send_sem=send4.at[step], recv_sem=recv4.at[step],
            device_id=device_of(other), device_id_type=MESH,
        )

    def spread_out(source, step, other):
        where = pl.ds(pl.multiple_of(side * half + source * piece, piece), piece)
        return pltpu.make_async_remote_copy(
            src_ref=piece_ref, dst_ref=final_ref.at[where],
            send_sem=send5.at[step], recv_sem=recv5.at[step],
            device_id=device_of(other), device_id_type=MESH,
        )

    def guarded(condition, action):
        if owners == ring:
            action()
        else:
            pl.when(condition)(action)

    def scatter_start(step):
        guarded(xor(rank, ring - 1 - step, ring) < owners, lambda: scatter(step).start())

    repeat(ring - 1, scatter_start)

    def reduce_piece():
        piece_ref[...] = half_ref[pl.ds(pl.multiple_of(rank * piece, piece), piece)]

        def add(step):
            scatter(step).wait_recv()
            piece_ref[...] = piece_ref[...] + piece_in[step]

        repeat(ring - 1, add)
        repeat(ring - 1, lambda step: spread_out(rank, step, xor(rank, ring - 1 - step, ring)).start())
        final_ref[pl.ds(pl.multiple_of(side * half + rank * piece, piece), piece)] = piece_ref[...]

    guarded(rank < owners, reduce_piece)

    def spread_wait(step):
        other = xor(rank, ring - 1 - step, ring)
        guarded(other < owners, lambda: spread_out(other, step, other).wait_recv())

    repeat(ring - 1, spread_wait)
    mine = pl.ds(pl.multiple_of(side * half, half), half)
    share = pltpu.make_async_remote_copy(
        src_ref=final_ref.at[mine], dst_ref=final_ref.at[mine],
        send_sem=send6, recv_sem=recv6, device_id=(orig, twin), device_id_type=MESH,
    )
    share.start()
    share.wait_recv()

    out_ref[...] = final_ref[...]

    def first_end(step):
        first(step, 1).wait_send()
        first(step, 0).wait_send()
        beside(step).wait_send()

    repeat(steps, first_end)
    repeat(remote, lambda step: beyond(step).wait_send())
    swap.wait_send()

    def scatter_end(step):
        guarded(xor(rank, ring - 1 - step, ring) < owners, lambda: scatter(step).wait_send())

    repeat(ring - 1, scatter_end)
    guarded(
        rank < owners,
        lambda: repeat(
            ring - 1, lambda step: spread_out(rank, step, xor(rank, ring - 1 - step, ring)).wait_send()
        ),
    )
    share.wait_send()


def update_kernel(counts_ref, final_ref, states_hbm, out_ref, states_ref, states_sem):
    link = lax.axis_index("link")
    own_rows, members = out_ref.shape
    half = members // 2
    fetch = pltpu.make_async_copy(
        states_hbm.at[pl.ds(pl.multiple_of(link * own_rows, own_rows), own_rows)], states_ref, states_sem
    )
    fetch.start()
    upper = final_ref[0:half, half:]
    gram = jnp.concatenate(
        [final_ref[0:half, :], jnp.concatenate([upper.T, final_ref[half:, half:]], axis=1)], axis=0
    )
    forcing = jnp.concatenate(
        [final_ref[pl.ds(half, 1), 0:half], final_ref[pl.ds(half + 1, 1), 0:half]], axis=1
    )
    high, low = split(transform_of(gram, forcing))
    fetch.wait()
    block_rows = states_hbm.shape[0] // counts_ref.shape[0]
    blocks = own_rows // block_rows
    position = lax.broadcasted_iota(jnp.int32, (block_rows, members), 0)
    for index in range(blocks):
        states = states_ref[index * block_rows : (index + 1) * block_rows]
        updated = jnp.dot(states, low, preferred_element_type=F32) + jnp.dot(
            states, high, preferred_element_type=F32
        )
        living = position < counts_ref[link * blocks + index]
        out_ref[index * block_rows : (index + 1) * block_rows] = jnp.where(
            living, updated, states.astype(F32)
        ).astype(BF16)


def per_device(background, live_counts, patterns, pattern_ids, link_targets, counts_obs, obs_var):
    n_orig = lax.axis_size("orig")
    n_link = lax.axis_size("link")
    states_dev, members = background.shape
    blocks_dev = live_counts.shape[0]
    block_rows = states_dev // blocks_dev
    link_rows = patterns.shape[2]
    rows = counts_obs.shape[1]
    link_blocks = rows * n_orig // link_rows
    vmem = pl.BlockSpec(memory_space=pltpu.VMEM)
    smem = pl.BlockSpec(memory_space=pltpu.SMEM)
    hbm = pl.BlockSpec(memory_space=pl.ANY)
    dma = pltpu.SemaphoreType.DMA
    grant = pltpu.CompilerParams(vmem_limit_bytes=WIDE_GRANT)
    pairs = n_orig // 2
    ring = n_orig * n_link // 2
    half = members // 2
    piece = half // min(ring, half // 8)
    cuts = CUTS if rows == link_rows else 1
    slots = pattern_ids.shape[2]
    steps = pairs // 2 * cuts
    gram = pl.pallas_call(
        functools.partial(gram_kernel, n_orig, n_link, cuts),
        out_shape=jax.ShapeDtypeStruct((members, members), F32),
        in_specs=[smem, smem, smem, hbm, hbm, vmem, vmem],
        out_specs=vmem,
        scratch_shapes=[
            pltpu.VMEM(patterns.shape[1:], BF16),
            pltpu.VMEM((states_dev, members), BF16),
            dma,
            dma,
            pltpu.VMEM((16, link_rows // cuts, block_rows), F32),
            pltpu.VMEM((16, link_rows // cuts, block_rows), F32),
            pltpu.SMEM((8, blocks_dev), jnp.int32),
            pltpu.VMEM((link_blocks * link_rows, members), F32),
            pltpu.VMEM((pairs, rows, members), F32),
            pltpu.VMEM((pairs, rows, members), F32),
            pltpu.VMEM((pairs // 2, rows, members), F32),
            pltpu.VMEM((pairs // 2, rows, members), F32),
            pltpu.VMEM((members, members), F32),
            pltpu.VMEM((half, members), F32),
            pltpu.VMEM((half, members), F32),
            pltpu.VMEM((ring - 1, piece, members), F32),
            pltpu.VMEM((piece, members), F32),
            pltpu.VMEM((members, members), F32),
            dma((2 * steps,)), dma((2 * steps,)),
            dma((steps,)), dma((steps,)),
            dma((steps,)), dma((steps,)),
            dma, dma,
            dma((ring,)), dma((ring,)),
            dma((ring,)), dma((ring,)),
            dma, dma,
        ],
        compiler_params=pltpu.CompilerParams(
            collective_id=0, has_side_effects=True, vmem_limit_bytes=WIDE_GRANT
        ),
    )(
        jnp.transpose(pattern_ids, (2, 0, 1)), jnp.transpose(link_targets, (2, 0, 1)), live_counts,
        patterns[0], background, counts_obs, obs_var,
    )
    own_rows = states_dev // n_link
    return pl.pallas_call(
        update_kernel,
        out_shape=jax.ShapeDtypeStruct((own_rows, members), BF16),
        in_specs=[smem, vmem, hbm],
        out_specs=vmem,
        scratch_shapes=[pltpu.VMEM((own_rows, members), BF16), dma],
        compiler_params=grant,
    )(live_counts, gram, background)


def solution(mesh):
    placed = (
        P("orig", None),
        P("orig"),
        P("link", "orig", None, None),
        P("link", "orig", None),
        P("link", "orig", None),
        P("link", "orig"),
        P("link", "orig"),
    )
    return jax.shard_map(
        per_device, mesh=mesh, in_specs=placed, out_specs=P(("orig", "link"), None), check_vma=False
    )
```

```python
import functools

import jax
import jax.numpy as jnp
from jax import lax
from jax.experimental import pallas as pl
from jax.experimental.pallas import tpu as pltpu
from jax.sharding import PartitionSpec as P

NS_ITERS = 4
CUTS = 4
SPAN = 8
WIDE_GRANT = 67043328 - 900 * 1024
MESH = pl.DeviceIdType.MESH
F32 = jnp.float32
BF16 = jnp.bfloat16


def repeat(count, body):
    if count <= 16:
        for step in range(count):
            body(step)
    else:
        lax.fori_loop(0, count, lambda step, carry: (body(step), carry)[1], 0)


def xor(a, b, size):
    total = 0
    bit = 1
    while bit < size:
        total = total + ((a // bit) % 2 + (b // bit) % 2) % 2 * bit
        bit *= 2
    return total


def split(x):
    high = x.astype(BF16)
    return high, (x - high.astype(F32)).astype(BF16)


def mm3(a, b):
    a_high, a_low = split(a)
    b_high, b_low = split(b)
    return (
        jnp.dot(a_high, b_low, preferred_element_type=F32)
        + jnp.dot(a_low, b_high, preferred_element_type=F32)
    ) + jnp.dot(a_high, b_high, preferred_element_type=F32)


def sort_slots(ids_ref, targets_ref, table_ref, tiles, link_blocks):
    slots = ids_ref.shape[0]
    bits = max(1, (tiles - 1).bit_length())
    per_word = 31 // bits
    targets = [targets_ref[slot] for slot in range(slots)]
    ones = [jnp.left_shift(jnp.ones_like(target), target * 4) for target in targets]
    tally = functools.reduce(lambda a, b: a + b, ones)
    starts = jnp.zeros_like(tally)
    for shift in range(1, 8):
        starts = starts + jnp.left_shift(tally, jnp.full_like(tally, 4 * shift))
    place = starts
    words = [jnp.zeros_like(tally) for _ in range(pl.cdiv(slots, per_word))]
    for slot in range(slots):
        rank = jnp.bitwise_and(jnp.right_shift(place, targets[slot] * 4), 15)
        place = place + ones[slot]
        tile = ids_ref[slot]
        for word in range(len(words)):
            local = rank - word * per_word
            inside = (local >= 0) & (local < per_word)
            shifted = jnp.left_shift(tile, jnp.where(inside, local * bits, 0))
            words[word] = words[word] + jnp.where(inside, shifted, 0)
    rows = []
    for slot in range(slots):
        amount = jnp.full_like(tally, slot % per_word * bits)
        rows.append(jnp.bitwise_and(jnp.right_shift(words[slot // per_word], amount), 2**bits - 1))
    for target in range(1, link_blocks):
        rows.append(jnp.bitwise_and(jnp.right_shift(starts, jnp.full_like(tally, 4 * target)), 15))
    for index, row in enumerate(rows):
        table_ref[index : index + 1, 0 : row.shape[1]] = row


def build_group(table_ref, tiles_ref, prefix_refs, lhs_ref, group, cut_index, slots, link_blocks):
    tiles, cut_rows, block_rows = tiles_ref.shape[1:]
    span = lhs_ref.shape[0] // 2
    for index in range(span):
        prefix_ref = prefix_refs[index % len(prefix_refs)]
        block = group * span + index
        total = jnp.zeros((cut_rows, block_rows), F32)
        for slot in range(slots):
            tile = table_ref[slot, block]
            total = total + tiles_ref[cut_index, tile].astype(F32)
            prefix_ref[slot + 1] = total
        before = None
        for target in range(link_blocks):
            upto = total
            if target < link_blocks - 1:
                end = table_ref[slots + target, block]
                upto = prefix_ref[end]
            high, low = split(upto if before is None else upto - before)
            before = upto
            rows = slice(target * cut_rows, (target + 1) * cut_rows)
            lhs_ref[index, rows] = high
            lhs_ref[span + index, rows] = low


def predict_cut(table_ref, tiles_ref, states_ref, prefix_refs, lhs_ref, term_ref, cut_index, cuts, slots):
    cut_rows, block_rows = tiles_ref.shape[2:]
    link_rows = cut_rows * cuts
    link_blocks = term_ref.shape[0] // link_rows
    span = lhs_ref.shape[0] // 2
    depth = span * block_rows
    groups = states_ref.shape[0] // depth

    def rows_of(target):
        return pl.ds(target * link_rows + cut_index * cut_rows, cut_rows)

    def build(place):
        cut_at = jnp.minimum(place // groups, cuts - 1)
        build_group(table_ref, tiles_ref, prefix_refs, lhs_ref, place % groups, cut_at, slots, link_blocks)

    for target in range(link_blocks):
        term_ref[rows_of(target)] = jnp.zeros((cut_rows, term_ref.shape[1]), F32)
    if cut_index == 0:
        build(0)

    def add_group(group, carry):
        states = states_ref[pl.ds(pl.multiple_of(group * depth, depth), depth)]
        left = jnp.concatenate([lhs_ref[index] for index in range(2 * span)], axis=1)
        product = jnp.dot(left, jnp.concatenate([states, states], axis=0), preferred_element_type=F32)
        build(cut_index * groups + group + 1)
        for target in range(link_blocks):
            term_ref[rows_of(target)] = term_ref[rows_of(target)] + product[target * cut_rows : (target + 1) * cut_rows]
        return carry

    lax.fori_loop(0, groups, add_group, 0)


def transform_of(gram, forcing):
    members = gram.shape[0]
    row = lax.broadcasted_iota(jnp.int32, (members, members), 0)
    column = lax.broadcasted_iota(jnp.int32, (members, members), 1)
    identity = (row == column).astype(F32)
    system = identity + gram * (1.0 / (members - 1.0))
    bound = jnp.max(jnp.sum(jnp.abs(system), axis=1, keepdims=True), axis=0, keepdims=True)
    root = system / bound
    middle = 1.5 * identity - 0.5 * root
    inverse = middle
    root = mm3(root, middle)
    for sweep in range(1, NS_ITERS):
        middle = 1.5 * identity - 0.5 * mm3(inverse, root)
        if sweep < NS_ITERS - 1:
            root = mm3(root, middle)
        inverse = mm3(middle, inverse)
    inner = mm3(jnp.broadcast_to(forcing, (8, members)), inverse)
    mean_weights = mm3(inner, inverse)[0:1] / (bound * (members - 1.0))
    whole = inverse / jnp.sqrt(bound) + jnp.broadcast_to(mean_weights, (members, members)).T
    return whole + (1.0 - jnp.sum(whole, axis=0, keepdims=True)) / members


def gram_kernel(
    n_orig, n_link, cuts, ids_ref, targets_ref, counts_ref, tiles_hbm, states_hbm, obs_ref, var_ref, out_ref,
    tiles_ref, states_ref, tiles_sem, states_sem, even_ref, odd_ref, lhs_ref, packed_ref, table_ref, table_sem, term_ref, first_in, sums, side_in, far_in, gram_ref, half_in, half_ref, piece_in, piece_ref, final_ref,
    send1, recv1, send2, recv2, send7, recv7, send3, recv3, send4, recv4, send5, recv5, send6, recv6,
):
    orig = lax.axis_index("orig")
    link = lax.axis_index("link")
    rows = obs_ref.shape[1]
    members = term_ref.shape[1]
    half = members // 2
    pairs = n_orig // 2
    parity = orig % 2
    place = orig // 2
    across = orig + 1 - 2 * parity
    side = link % 2
    twin = link + 1 - 2 * side
    ring = n_orig * n_link // 2
    rank = (link // 2) * n_orig + orig
    owners = min(ring, half // 8)
    piece = half // owners

    def device_of(other):
        return (other % n_orig, (other // n_orig) * 2 + side)

    load_states = pltpu.make_async_copy(states_hbm, states_ref, states_sem)
    load_states.start()

    def load_tiles(index):
        part = tiles_ref.shape[2]
        return pltpu.make_async_copy(
            tiles_hbm.at[:, pl.ds(index * part, part)], tiles_ref.at[index], tiles_sem.at[index]
        )

    for index in range(cuts):
        load_tiles(index).start()
    near = place % 2
    far = place // 2
    n_far = pairs // 2
    barrier = pltpu.get_barrier_semaphore()

    def greet(other_orig, other_link):
        pl.semaphore_signal(barrier, inc=1, device_id=(other_orig, other_link), device_id_type=MESH)

    greet(across, link)
    greet(2 * (far * 2 + 1 - near) + parity, link)
    repeat(n_far - 1, lambda step: greet(2 * (xor(far, step + 1, n_far) * 2 + near) + parity, link))
    repeat(n_link - 1, lambda step: greet(orig, (link + step + 1) % n_link))

    slots = ids_ref.shape[0]
    blocks = counts_ref.shape[0]
    block_rows = states_ref.shape[0] // blocks
    link_rows = tiles_ref.shape[2] * cuts
    sort_slots(ids_ref, targets_ref, packed_ref, tiles_ref.shape[1], rows * n_orig // link_rows)
    move_table = pltpu.make_async_copy(packed_ref, table_ref, table_sem)
    move_table.start()
    for prefix_ref in (even_ref, odd_ref):
        prefix_ref[...] = jnp.zeros(prefix_ref.shape, F32)
    position = lax.broadcasted_iota(jnp.int32, (block_rows, members), 0)
    load_states.wait()

    def mask_block(block, carry):
        where = pl.ds(pl.multiple_of(block * block_rows, block_rows), block_rows)
        states = states_ref[where]
        states_ref[where] = jnp.where(position < counts_ref[block], states, jnp.zeros_like(states))
        return carry

    lax.fori_loop(0, blocks, mask_block, 0, unroll=2)
    for index in range(cuts):
        load_tiles(index).wait()
    move_table.wait()

    cut_rows = rows // cuts
    steps = n_far * cuts

    def owner(step, flip):
        other = xor(far, n_far - 1 - step // cuts, n_far)
        return other * 2 + (near + flip) % 2

    def term_rows(index, step):
        return pl.ds(pl.multiple_of(index * rows + step % cuts * cut_rows, cut_rows), cut_rows)

    def cut(step):
        return pl.ds(pl.multiple_of(step % cuts * cut_rows, cut_rows), cut_rows)

    def slot(step, flip):
        return step // cuts * 2 + 1 - flip

    def first(step, flip):
        index = slot(step, flip) * cuts + step % cuts
        return pltpu.make_async_remote_copy(
            src_ref=term_ref.at[term_rows(2 * owner(step, flip) + 1 - parity, step)],
            dst_ref=first_in.at[slot(step, flip), cut(step)],
            send_sem=send1.at[index], recv_sem=recv1.at[index],
            device_id=(across, link), device_id_type=MESH,
        )

    def beside(step):
        return pltpu.make_async_remote_copy(
            src_ref=sums.at[slot(step, 1), cut(step)], dst_ref=side_in.at[step // cuts, cut(step)],
            send_sem=send2.at[step], recv_sem=recv2.at[step],
            device_id=(2 * (far * 2 + 1 - near) + parity, link), device_id_type=MESH,
        )

    def beyond(step):
        return pltpu.make_async_remote_copy(
            src_ref=sums.at[slot(step, 0), cut(step)], dst_ref=far_in.at[step // cuts, cut(step)],
            send_sem=send7.at[step], recv_sem=recv7.at[step],
            device_id=(2 * owner(step, 0) + parity, link), device_id_type=MESH,
        )

    remote = steps - cuts
    lag = min(2, remote, cuts)

    for index in range(cuts):
        predict_cut(
            table_ref, tiles_ref, states_ref, (even_ref, odd_ref), lhs_ref, term_ref, index, cuts, slots
        )
        if index == 0:
            pl.semaphore_wait(barrier, n_far + n_link)

        def first_start(step):
            first(step * cuts + index, 1).start()
            first(step * cuts + index, 0).start()

        repeat(n_far - 1, first_start)
    repeat(cuts, lambda step: first(step + remote, 1).start())
    repeat(cuts, lambda step: first(step + remote, 0).start())

    def add_first(step, flip):
        first(step, flip).wait_recv()
        sums[slot(step, flip), cut(step)] = (
            term_ref[term_rows(2 * owner(step, flip) + parity, step)] + first_in[slot(step, flip), cut(step)]
        )
        if flip:
            beside(step).start()

    def add_beside(step):
        beside(step).wait_recv()
        sums[slot(step, 0), cut(step)] = sums[slot(step, 0), cut(step)] + side_in[step // cuts, cut(step)]

    def pass_on(step):
        add_beside(step)
        beyond(step).start()

    def enter(step):
        add_first(step, 1)
        add_first(step, 0)

    repeat(lag, enter)

    def middle_step(step):
        enter(step + lag)
        pass_on(step)

    repeat(remote - lag, middle_step)
    for step in range(cuts):
        add_first(step + remote, 1)
        if step < lag:
            pass_on(step + (remote - lag))
    for step in range(cuts):
        add_first(step + remote, 0)
        add_beside(step + remote)

    def gather(step):
        beyond(step).wait_recv()
        sums[pairs - 1, cut(step)] = sums[pairs - 1, cut(step)] + far_in[step // cuts, cut(step)]

    repeat(remote, gather)

    predicted = sums[pairs - 1]
    turned = predicted.T
    weights = 1.0 / var_ref[...]
    mean_row = jnp.sum(turned, axis=0, keepdims=True) / members
    spread = predicted - jnp.sum(predicted, axis=1, keepdims=True) / members
    spread_t = turned - mean_row
    gram_ref[...] = mm3(spread_t * weights, spread)
    pull = jnp.broadcast_to(weights * (obs_ref[...] - mean_row), (8, rows))
    forcing = mm3(pull, spread)
    gram_ref[pl.ds(half, 1), 0:half] = forcing[0:1, 0:half]
    gram_ref[pl.ds(half + 1, 1), 0:half] = forcing[0:1, half:]

    swap = pltpu.make_async_remote_copy(
        src_ref=gram_ref.at[pl.ds(pl.multiple_of((1 - side) * half, half), half)], dst_ref=half_in,
        send_sem=send3, recv_sem=recv3, device_id=(orig, twin), device_id_type=MESH,
    )
    swap.start()
    swap.wait_recv()
    half_ref[...] = gram_ref[pl.ds(pl.multiple_of(side * half, half), half)] + half_in[...]

    def scatter(step):
        other = xor(rank, ring - 1 - step, ring)
        return pltpu.make_async_remote_copy(
            src_ref=half_ref.at[pl.ds(pl.multiple_of(other * piece, piece), piece)], dst_ref=piece_in.at[step],
            send_sem=send4.at[step], recv_sem=recv4.at[step],
            device_id=device_of(other), device_id_type=MESH,
        )

    def spread_out(source, step, other):
        where = pl.ds(pl.multiple_of(side * half + source * piece, piece), piece)
        return pltpu.make_async_remote_copy(
            src_ref=piece_ref, dst_ref=final_ref.at[where],
            send_sem=send5.at[step], recv_sem=recv5.at[step],
            device_id=device_of(other), device_id_type=MESH,
        )

    def guarded(condition, action):
        if owners == ring:
            action()
        else:
            pl.when(condition)(action)

    def scatter_start(step):
        guarded(xor(rank, ring - 1 - step, ring) < owners, lambda: scatter(step).start())

    repeat(ring - 1, scatter_start)

    def reduce_piece():
        piece_ref[...] = half_ref[pl.ds(pl.multiple_of(rank * piece, piece), piece)]

        def add(step):
            scatter(step).wait_recv()
            piece_ref[...] = piece_ref[...] + piece_in[step]

        repeat(ring - 1, add)
        repeat(ring - 1, lambda step: spread_out(rank, step, xor(rank, ring - 1 - step, ring)).start())
        final_ref[pl.ds(pl.multiple_of(side * half + rank * piece, piece), piece)] = piece_ref[...]

    guarded(rank < owners, reduce_piece)

    def spread_wait(step):
        other = xor(rank, ring - 1 - step, ring)
        guarded(other < owners, lambda: spread_out(other, step, other).wait_recv())

    repeat(ring - 1, spread_wait)
    mine = pl.ds(pl.multiple_of(side * half, half), half)
    share = pltpu.make_async_remote_copy(
        src_ref=final_ref.at[mine], dst_ref=final_ref.at[mine],
        send_sem=send6, recv_sem=recv6, device_id=(orig, twin), device_id_type=MESH,
    )
    share.start()
    share.wait_recv()

    out_ref[...] = final_ref[...]

    def first_end(step):
        first(step, 1).wait_send()
        first(step, 0).wait_send()
        beside(step).wait_send()

    repeat(steps, first_end)
    repeat(remote, lambda step: beyond(step).wait_send())
    swap.wait_send()

    def scatter_end(step):
        guarded(xor(rank, ring - 1 - step, ring) < owners, lambda: scatter(step).wait_send())

    repeat(ring - 1, scatter_end)
    guarded(
        rank < owners,
        lambda: repeat(
            ring - 1, lambda step: spread_out(rank, step, xor(rank, ring - 1 - step, ring)).wait_send()
        ),
    )
    share.wait_send()


def update_kernel(counts_ref, final_ref, states_hbm, out_ref, states_ref, states_sem):
    link = lax.axis_index("link")
    own_rows, members = out_ref.shape
    half = members // 2
    fetch = pltpu.make_async_copy(
        states_hbm.at[pl.ds(pl.multiple_of(link * own_rows, own_rows), own_rows)], states_ref, states_sem
    )
    fetch.start()
    upper = final_ref[0:half, half:]
    gram = jnp.concatenate(
        [final_ref[0:half, :], jnp.concatenate([upper.T, final_ref[half:, half:]], axis=1)], axis=0
    )
    forcing = jnp.concatenate(
        [final_ref[pl.ds(half, 1), 0:half], final_ref[pl.ds(half + 1, 1), 0:half]], axis=1
    )
    high, low = split(transform_of(gram, forcing))
    fetch.wait()
    block_rows = states_hbm.shape[0] // counts_ref.shape[0]
    blocks = own_rows // block_rows
    position = lax.broadcasted_iota(jnp.int32, (block_rows, members), 0)
    for index in range(blocks):
        states = states_ref[index * block_rows : (index + 1) * block_rows]
        updated = jnp.dot(states, low, preferred_element_type=F32) + jnp.dot(
            states, high, preferred_element_type=F32
        )
        living = position < counts_ref[link * blocks + index]
        out_ref[index * block_rows : (index + 1) * block_rows] = jnp.where(
            living, updated, states.astype(F32)
        ).astype(BF16)


def per_device(background, live_counts, patterns, pattern_ids, link_targets, counts_obs, obs_var):
    n_orig = lax.axis_size("orig")
    n_link = lax.axis_size("link")
    states_dev, members = background.shape
    blocks_dev = live_counts.shape[0]
    block_rows = states_dev // blocks_dev
    link_rows = patterns.shape[2]
    rows = counts_obs.shape[1]
    link_blocks = rows * n_orig // link_rows
    vmem = pl.BlockSpec(memory_space=pltpu.VMEM)
    smem = pl.BlockSpec(memory_space=pltpu.SMEM)
    hbm = pl.BlockSpec(memory_space=pl.ANY)
    dma = pltpu.SemaphoreType.DMA
    grant = pltpu.CompilerParams(vmem_limit_bytes=WIDE_GRANT)
    pairs = n_orig // 2
    ring = n_orig * n_link // 2
    half = members // 2
    piece = half // min(ring, half // 8)
    cuts = CUTS if rows == link_rows else 1
    slots = pattern_ids.shape[2]
    table_rows = pl.cdiv(slots + link_blocks, 8) * 8
    steps = pairs // 2 * cuts
    gram = pl.pallas_call(
        functools.partial(gram_kernel, n_orig, n_link, cuts),
        out_shape=jax.ShapeDtypeStruct((members, members), F32),
        in_specs=[vmem, vmem, smem, hbm, hbm, vmem, vmem],
        out_specs=vmem,
        scratch_shapes=[
            pltpu.VMEM((cuts, patterns.shape[1], link_rows // cuts, block_rows), BF16),
            pltpu.VMEM((states_dev, members), BF16),
            dma((cuts,)),
            dma,
            pltpu.VMEM((16, link_rows // cuts, block_rows), F32),
            pltpu.VMEM((16, link_rows // cuts, block_rows), F32),
            pltpu.VMEM((2 * SPAN, link_blocks * link_rows // cuts, block_rows), BF16),
            pltpu.VMEM((table_rows, 128), jnp.int32),
            pltpu.SMEM((table_rows, 128), jnp.int32),
            dma,
            pltpu.VMEM((link_blocks * link_rows, members), F32),
            pltpu.VMEM((pairs, rows, members), F32),
            pltpu.VMEM((pairs, rows, members), F32),
            pltpu.VMEM((pairs // 2, rows, members), F32),
            pltpu.VMEM((pairs // 2, rows, members), F32),
            pltpu.VMEM((members, members), F32),
            pltpu.VMEM((half, members), F32),
            pltpu.VMEM((half, members), F32),
            pltpu.VMEM((ring - 1, piece, members), F32),
            pltpu.VMEM((piece, members), F32),
            pltpu.VMEM((members, members), F32),
            dma((2 * steps,)), dma((2 * steps,)),
            dma((steps,)), dma((steps,)),
            dma((steps,)), dma((steps,)),
            dma, dma,
            dma((ring,)), dma((ring,)),
            dma((ring,)), dma((ring,)),
            dma, dma,
        ],
        compiler_params=pltpu.CompilerParams(
            collective_id=0, has_side_effects=True, vmem_limit_bytes=WIDE_GRANT
        ),
    )(
        jnp.transpose(pattern_ids, (2, 0, 1)), jnp.transpose(link_targets, (2, 0, 1)), live_counts,
        patterns[0], background, counts_obs, obs_var,
    )
    own_rows = states_dev // n_link
    return pl.pallas_call(
        update_kernel,
        out_shape=jax.ShapeDtypeStruct((own_rows, members), BF16),
        in_specs=[smem, vmem, hbm],
        out_specs=vmem,
        scratch_shapes=[pltpu.VMEM((own_rows, members), BF16), dma],
        compiler_params=grant,
    )(live_counts, gram, background)


def solution(mesh):
    placed = (
        P("orig", None),
        P("orig"),
        P("link", "orig", None, None),
        P("link", "orig", None),
        P("link", "orig", None),
        P("link", "orig"),
        P("link", "orig"),
    )
    return jax.shard_map(
        per_device, mesh=mesh, in_specs=placed, out_specs=P(("orig", "link"), None), check_vma=False
    )
```

```python
import functools

import jax
import jax.numpy as jnp
from jax import lax
from jax.experimental import pallas as pl
from jax.experimental.pallas import tpu as pltpu
from jax.sharding import PartitionSpec as P

NS_ITERS = 4
CUTS = 4
SPAN = 8
WIDE_GRANT = 67043328-900*1024
MESH = pl.DeviceIdType.MESH
F32 = jnp.float32
BF16 = jnp.bfloat16


def repeat(count, body):
    if count <= 16:
        for step in range(count):
            body(step)
    else:
        lax.fori_loop(0, count, lambda step, carry: (body(step), carry)[1], 0)


def xor(a, b, size):
    total = 0
    bit = 1
    while bit < size:
        total = total + ((a // bit) % 2 + (b // bit) % 2) % 2 * bit
        bit *= 2
    return total


def split(x):
    high = x.astype(BF16)
    return high, (x - high.astype(F32)).astype(BF16)


def mm3(a, b):
    a_high, a_low = split(a)
    b_high, b_low = split(b)
    return (
        jnp.dot(a_high, b_low, preferred_element_type=F32)
        + jnp.dot(a_low, b_high, preferred_element_type=F32)
    ) + jnp.dot(a_high, b_high, preferred_element_type=F32)


def sort_slots(ids_ref, targets_ref, table_ref, tiles, link_blocks):
    slots = ids_ref.shape[0]
    bits = max(1, (tiles - 1).bit_length())
    per_word = 31 // bits
    targets = [targets_ref[slot] for slot in range(slots)]
    ones = [jnp.left_shift(jnp.ones_like(target), target * 4) for target in targets]
    tally = functools.reduce(lambda a, b: a + b, ones)
    starts = jnp.zeros_like(tally)
    for shift in range(1, 8):
        starts = starts + jnp.left_shift(tally, jnp.full_like(tally, 4 * shift))
    place = starts
    words = [jnp.zeros_like(tally) for _ in range(pl.cdiv(slots, per_word))]
    for slot in range(slots):
        rank = jnp.bitwise_and(jnp.right_shift(place, targets[slot] * 4), 15)
        place = place + ones[slot]
        tile = ids_ref[slot]
        for word in range(len(words)):
            local = rank - word * per_word
            inside = (local >= 0) & (local < per_word)
            shifted = jnp.left_shift(tile, jnp.where(inside, local * bits, 0))
            words[word] = words[word] + jnp.where(inside, shifted, 0)
    rows = []
    for slot in range(slots):
        amount = jnp.full_like(tally, slot % per_word * bits)
        rows.append(jnp.bitwise_and(jnp.right_shift(words[slot // per_word], amount), 2**bits - 1))
    for target in range(1, link_blocks):
        rows.append(jnp.bitwise_and(jnp.right_shift(starts, jnp.full_like(tally, 4 * target)), 15))
    for index, row in enumerate(rows):
        table_ref[index : index + 1, 0 : row.shape[1]] = row


def build_group(table_ref, tiles_ref, prefix_refs, lhs_ref, group, cut_index, slots, link_blocks):
    tiles, cut_rows, block_rows = tiles_ref.shape[1:]
    span = lhs_ref.shape[0] // 2
    for index in range(span):
        prefix_ref = prefix_refs[index % len(prefix_refs)]
        block = group * span + index
        total = jnp.zeros((cut_rows, block_rows), F32)
        for slot in range(slots):
            tile = table_ref[slot, block]
            total = total + tiles_ref[cut_index, tile].astype(F32)
            prefix_ref[slot + 1] = total
        before = None
        for target in range(link_blocks):
            upto = total
            if target < link_blocks - 1:
                end = table_ref[slots + target, block]
                upto = prefix_ref[end]
            high, low = split(upto if before is None else upto - before)
            before = upto
            rows = slice(target * cut_rows, (target + 1) * cut_rows)
            lhs_ref[index, rows] = high
            lhs_ref[span + index, rows] = low


def predict_cut(table_ref, tiles_ref, states_ref, prefix_refs, lhs_ref, term_ref, cut_index, cuts, slots):
    cut_rows, block_rows = tiles_ref.shape[2:]
    link_rows = cut_rows * cuts
    link_blocks = term_ref.shape[0] // link_rows
    span = lhs_ref.shape[0] // 2
    depth = span * block_rows
    groups = states_ref.shape[0] // depth

    def rows_of(target):
        return pl.ds(target * link_rows + cut_index * cut_rows, cut_rows)

    def build(place):
        cut_at = jnp.minimum(place // groups, cuts - 1)
        build_group(table_ref, tiles_ref, prefix_refs, lhs_ref, place % groups, cut_at, slots, link_blocks)

    for target in range(link_blocks):
        term_ref[rows_of(target)] = jnp.zeros((cut_rows, term_ref.shape[1]), F32)
    if cut_index == 0:
        build(0)

    def add_group(group, carry):
        states = states_ref[pl.ds(pl.multiple_of(group * depth, depth), depth)]
        left = jnp.concatenate([lhs_ref[index] for index in range(2 * span)], axis=1)
        product = jnp.dot(left, jnp.concatenate([states, states], axis=0), preferred_element_type=F32)
        build(cut_index * groups + group + 1)
        for target in range(link_blocks):
            term_ref[rows_of(target)] = term_ref[rows_of(target)] + product[target * cut_rows : (target + 1) * cut_rows]
        return carry

    lax.fori_loop(0, groups, add_group, 0)


def column_of(row):
    width = row.shape[1]
    return jnp.broadcast_to(row, (width, width)).T


def transform_of(gram, forcing):
    members = gram.shape[0]
    row = lax.broadcasted_iota(jnp.int32, (members, members), 0)
    column = lax.broadcasted_iota(jnp.int32, (members, members), 1)
    identity = (row == column).astype(F32)
    system = identity + gram * (1.0 / (members - 1.0))
    bound = jnp.max(jnp.sum(jnp.abs(system), axis=1, keepdims=True), axis=0, keepdims=True)
    root = system / bound
    middle = 1.5 * identity - 0.5 * root
    inverse = middle
    root = mm3(root, middle)
    for sweep in range(1, NS_ITERS):
        middle = 1.5 * identity - 0.5 * mm3(inverse, root)
        if sweep < NS_ITERS - 1:
            root = mm3(root, middle)
        inverse = mm3(middle, inverse)
    inner = jnp.sum(inverse * column_of(forcing), axis=0, keepdims=True)
    mean_weights = jnp.sum(inverse * inner, axis=1, keepdims=True) / (bound * (members - 1.0))
    whole = inverse / jnp.sqrt(bound) + mean_weights
    return whole + (1.0 - jnp.sum(whole, axis=0, keepdims=True)) / members


def gram_kernel(
    n_orig, n_link, cuts, ids_hbm, targets_hbm, counts_hbm, tiles_hbm, states_hbm, obs_hbm, var_hbm, out_ref,
    ids_ref, targets_ref, counts_ref, obs_ref, var_ref, small_sem, tiles_ref, states_ref, tiles_sem, states_sem, even_ref, odd_ref, lhs_ref, packed_ref, table_ref, table_sem, term_ref, first_in, sums, side_in, far_in, gram_ref, half_in, half_ref, piece_in, piece_ref, final_ref,
    send1, recv1, send2, recv2, send7, recv7, send3, recv3, send4, recv4, send5, recv5, send6, recv6,
):
    orig = lax.axis_index("orig")
    link = lax.axis_index("link")
    rows = obs_ref.shape[1]
    members = term_ref.shape[1]
    half = members // 2
    pairs = n_orig // 2
    parity = orig % 2
    place = orig // 2
    across = orig + 1 - 2 * parity
    side = link % 2
    twin = link + 1 - 2 * side
    ring = n_orig * n_link // 2
    rank = (link // 2) * n_orig + orig
    owners = min(ring, half // 8)
    piece = half // owners

    def device_of(other):
        return (other % n_orig, (other // n_orig) * 2 + side)

    load_small = [
        pltpu.make_async_copy(source, target, small_sem.at[index])
        for index, (source, target) in enumerate(
            [
                (ids_hbm, ids_ref), (targets_hbm, targets_ref), (counts_hbm, counts_ref),
                (obs_hbm, obs_ref), (var_hbm, var_ref),
            ]
        )
    ]
    for copy in load_small[:3]:
        copy.start()
    load_states = pltpu.make_async_copy(states_hbm, states_ref, states_sem)
    load_states.start()

    def load_tiles(index):
        part = tiles_ref.shape[2]
        return pltpu.make_async_copy(
            tiles_hbm.at[:, pl.ds(index * part, part)], tiles_ref.at[index], tiles_sem.at[index]
        )

    for index in range(cuts):
        load_tiles(index).start()
    for copy in load_small[3:]:
        copy.start()
    near = place % 2
    far = place // 2
    n_far = pairs // 2
    barrier = pltpu.get_barrier_semaphore()

    def greet(other_orig, other_link):
        pl.semaphore_signal(barrier, inc=1, device_id=(other_orig, other_link), device_id_type=MESH)

    greet(across, link)
    greet(2 * (far * 2 + 1 - near) + parity, link)
    repeat(n_far - 1, lambda step: greet(2 * (xor(far, step + 1, n_far) * 2 + near) + parity, link))
    repeat(n_link - 1, lambda step: greet(orig, (link + step + 1) % n_link))

    slots = ids_ref.shape[0]
    blocks = counts_ref.shape[0]
    block_rows = states_ref.shape[0] // blocks
    link_rows = tiles_ref.shape[2] * cuts
    load_small[0].wait()
    load_small[1].wait()
    sort_slots(ids_ref, targets_ref, packed_ref, tiles_ref.shape[1], rows * n_orig // link_rows)
    move_table = pltpu.make_async_copy(packed_ref, table_ref, table_sem)
    move_table.start()
    for prefix_ref in (even_ref, odd_ref):
        prefix_ref[...] = jnp.zeros(prefix_ref.shape, F32)
    position = lax.broadcasted_iota(jnp.int32, (block_rows, members), 0)
    load_small[2].wait()
    load_states.wait()

    def mask_block(block, carry):
        where = pl.ds(pl.multiple_of(block * block_rows, block_rows), block_rows)
        states = states_ref[where]
        states_ref[where] = jnp.where(position < counts_ref[block], states, jnp.zeros_like(states))
        return carry

    lax.fori_loop(0, blocks, mask_block, 0, unroll=2)
    for index in range(cuts):
        load_tiles(index).wait()
    move_table.wait()

    cut_rows = rows // cuts
    steps = n_far * cuts

    def owner(step, flip):
        other = xor(far, n_far - 1 - step // cuts, n_far)
        return other * 2 + (near + flip) % 2

    def term_rows(index, step):
        return pl.ds(pl.multiple_of(index * rows + step % cuts * cut_rows, cut_rows), cut_rows)

    def cut(step):
        return pl.ds(pl.multiple_of(step % cuts * cut_rows, cut_rows), cut_rows)

    def slot(step, flip):
        return step // cuts * 2 + 1 - flip

    def first(step, flip):
        index = slot(step, flip) * cuts + step % cuts
        return pltpu.make_async_remote_copy(
            src_ref=term_ref.at[term_rows(2 * owner(step, flip) + 1 - parity, step)],
            dst_ref=first_in.at[slot(step, flip), cut(step)],
            send_sem=send1.at[index], recv_sem=recv1.at[index],
            device_id=(across, link), device_id_type=MESH,
        )

    def beside(step):
        return pltpu.make_async_remote_copy(
            src_ref=sums.at[slot(step, 1), cut(step)], dst_ref=side_in.at[step // cuts, cut(step)],
            send_sem=send2.at[step], recv_sem=recv2.at[step],
            device_id=(2 * (far * 2 + 1 - near) + parity, link), device_id_type=MESH,
        )

    def beyond(step):
        return pltpu.make_async_remote_copy(
            src_ref=sums.at[slot(step, 0), cut(step)], dst_ref=far_in.at[step // cuts, cut(step)],
            send_sem=send7.at[step], recv_sem=recv7.at[step],
            device_id=(2 * owner(step, 0) + parity, link), device_id_type=MESH,
        )

    remote = steps - cuts
    lag = min(2, remote, cuts)

    for index in range(cuts):
        predict_cut(
            table_ref, tiles_ref, states_ref, (even_ref, odd_ref), lhs_ref, term_ref, index, cuts, slots
        )
        if index == 0:
            pl.semaphore_wait(barrier, n_far + n_link)

        def first_start(step):
            first(step * cuts + index, 1).start()
            first(step * cuts + index, 0).start()

        repeat(n_far - 1, first_start)
    repeat(cuts, lambda step: first(step + remote, 1).start())
    repeat(cuts, lambda step: first(step + remote, 0).start())

    def add_first(step, flip):
        first(step, flip).wait_recv()
        sums[slot(step, flip), cut(step)] = (
            term_ref[term_rows(2 * owner(step, flip) + parity, step)] + first_in[slot(step, flip), cut(step)]
        )
        if flip:
            beside(step).start()

    def add_beside(step):
        beside(step).wait_recv()
        sums[slot(step, 0), cut(step)] = sums[slot(step, 0), cut(step)] + side_in[step // cuts, cut(step)]

    def pass_on(step):
        add_beside(step)
        beyond(step).start()

    def enter(step):
        add_first(step, 1)
        add_first(step, 0)

    repeat(lag, enter)

    def middle_step(step):
        enter(step + lag)
        pass_on(step)

    repeat(remote - lag, middle_step)
    for step in range(cuts):
        add_first(step + remote, 1)
        if step < lag:
            pass_on(step + (remote - lag))
    for step in range(cuts):
        add_first(step + remote, 0)
        add_beside(step + remote)

    def gather(step):
        beyond(step).wait_recv()
        sums[pairs - 1, cut(step)] = sums[pairs - 1, cut(step)] + far_in[step // cuts, cut(step)]

    repeat(remote, gather)

    load_small[3].wait()
    load_small[4].wait()
    predicted = sums[pairs - 1]
    turned = predicted.T
    weights = 1.0 / var_ref[...]
    mean_row = jnp.sum(turned, axis=0, keepdims=True) / members
    spread = predicted - jnp.sum(predicted, axis=1, keepdims=True) / members
    spread_t = turned - mean_row
    gram_ref[...] = mm3(spread_t * weights, spread)
    pull = jnp.broadcast_to(weights * (obs_ref[...] - mean_row), (8, rows))
    forcing = mm3(pull, spread)
    gram_ref[pl.ds(half, 1), 0:half] = forcing[0:1, 0:half]
    gram_ref[pl.ds(half + 1, 1), 0:half] = forcing[0:1, half:]

    swap = pltpu.make_async_remote_copy(
        src_ref=gram_ref.at[pl.ds(pl.multiple_of((1 - side) * half, half), half)], dst_ref=half_in,
        send_sem=send3, recv_sem=recv3, device_id=(orig, twin), device_id_type=MESH,
    )
    swap.start()
    swap.wait_recv()
    half_ref[...] = gram_ref[pl.ds(pl.multiple_of(side * half, half), half)] + half_in[...]

    def scatter(step):
        other = xor(rank, ring - 1 - step, ring)
        return pltpu.make_async_remote_copy(
            src_ref=half_ref.at[pl.ds(pl.multiple_of(other * piece, piece), piece)], dst_ref=piece_in.at[step],
            send_sem=send4.at[step], recv_sem=recv4.at[step],
            device_id=device_of(other), device_id_type=MESH,
        )

    def spread_out(source, step, other):
        where = pl.ds(pl.multiple_of(side * half + source * piece, piece), piece)
        return pltpu.make_async_remote_copy(
            src_ref=piece_ref, dst_ref=final_ref.at[where],
            send_sem=send5.at[step], recv_sem=recv5.at[step],
            device_id=device_of(other), device_id_type=MESH,
        )

    def guarded(condition, action):
        if owners == ring:
            action()
        else:
            pl.when(condition)(action)

    def scatter_start(step):
        guarded(xor(rank, ring - 1 - step, ring) < owners, lambda: scatter(step).start())

    repeat(ring - 1, scatter_start)

    def reduce_piece():
        piece_ref[...] = half_ref[pl.ds(pl.multiple_of(rank * piece, piece), piece)]

        def add(step):
            scatter(step).wait_recv()
            piece_ref[...] = piece_ref[...] + piece_in[step]

        repeat(ring - 1, add)
        repeat(ring - 1, lambda step: spread_out(rank, step, xor(rank, ring - 1 - step, ring)).start())
        final_ref[pl.ds(pl.multiple_of(side * half + rank * piece, piece), piece)] = piece_ref[...]

    guarded(rank < owners, reduce_piece)

    def spread_wait(step):
        other = xor(rank, ring - 1 - step, ring)
        guarded(other < owners, lambda: spread_out(other, step, other).wait_recv())

    repeat(ring - 1, spread_wait)
    mine = pl.ds(pl.multiple_of(side * half, half), half)
    share = pltpu.make_async_remote_copy(
        src_ref=final_ref.at[mine], dst_ref=final_ref.at[mine],
        send_sem=send6, recv_sem=recv6, device_id=(orig, twin), device_id_type=MESH,
    )
    share.start()
    share.wait_recv()

    out_ref[...] = final_ref[...]

    def first_end(step):
        first(step, 1).wait_send()
        first(step, 0).wait_send()
        beside(step).wait_send()

    repeat(steps, first_end)
    repeat(remote, lambda step: beyond(step).wait_send())
    swap.wait_send()

    def scatter_end(step):
        guarded(xor(rank, ring - 1 - step, ring) < owners, lambda: scatter(step).wait_send())

    repeat(ring - 1, scatter_end)
    guarded(
        rank < owners,
        lambda: repeat(
            ring - 1, lambda step: spread_out(rank, step, xor(rank, ring - 1 - step, ring)).wait_send()
        ),
    )
    share.wait_send()


def update_kernel(counts_hbm, final_ref, states_hbm, out_hbm, counts_ref, states_ref, done_ref, counts_sem, states_sem, done_sem):
    link = lax.axis_index("link")
    own_rows, members = done_ref.shape
    half = members // 2
    fetch = pltpu.make_async_copy(
        states_hbm.at[pl.ds(pl.multiple_of(link * own_rows, own_rows), own_rows)], states_ref, states_sem
    )
    fetch.start()
    fetch_counts = pltpu.make_async_copy(counts_hbm, counts_ref, counts_sem)
    fetch_counts.start()
    upper = final_ref[0:half, half:]
    gram = jnp.concatenate(
        [final_ref[0:half, :], jnp.concatenate([upper.T, final_ref[half:, half:]], axis=1)], axis=0
    )
    forcing = jnp.concatenate(
        [final_ref[pl.ds(half, 1), 0:half], final_ref[pl.ds(half + 1, 1), 0:half]], axis=1
    )
    high, low = split(transform_of(gram, forcing))
    fetch.wait()
    fetch_counts.wait()
    block_rows = states_hbm.shape[0] // counts_ref.shape[0]
    blocks = own_rows // block_rows
    position = lax.broadcasted_iota(jnp.int32, (block_rows, members), 0)

    def store(index):
        where = slice(index * block_rows, (index + 1) * block_rows)
        return pltpu.make_async_copy(done_ref.at[where], out_hbm.at[where], done_sem.at[index])

    for index in range(blocks):
        states = states_ref[index * block_rows : (index + 1) * block_rows]
        updated = jnp.dot(states, low, preferred_element_type=F32) + jnp.dot(
            states, high, preferred_element_type=F32
        )
        living = position < counts_ref[link * blocks + index]
        done_ref[index * block_rows : (index + 1) * block_rows] = jnp.where(
            living, updated, states.astype(F32)
        ).astype(BF16)
        store(index).start()
    for index in range(blocks):
        store(index).wait()


def per_device(background, live_counts, patterns, pattern_ids, link_targets, counts_obs, obs_var):
    n_orig = lax.axis_size("orig")
    n_link = lax.axis_size("link")
    states_dev, members = background.shape
    blocks_dev = live_counts.shape[0]
    block_rows = states_dev // blocks_dev
    link_rows = patterns.shape[2]
    rows = counts_obs.shape[1]
    link_blocks = rows * n_orig // link_rows
    vmem = pl.BlockSpec(memory_space=pltpu.VMEM)
    hbm = pl.BlockSpec(memory_space=pl.ANY)
    dma = pltpu.SemaphoreType.DMA
    grant = pltpu.CompilerParams(vmem_limit_bytes=WIDE_GRANT)
    pairs = n_orig // 2
    ring = n_orig * n_link // 2
    half = members // 2
    piece = half // min(ring, half // 8)
    cuts = CUTS if rows == link_rows else 1
    slots = pattern_ids.shape[2]
    table_rows = pl.cdiv(slots + link_blocks, 8) * 8
    steps = pairs // 2 * cuts
    gram = pl.pallas_call(
        functools.partial(gram_kernel, n_orig, n_link, cuts),
        out_shape=pltpu.VMEM((members, members), F32),
        in_specs=[hbm] * 7,
        out_specs=vmem,
        scratch_shapes=[
            pltpu.VMEM((slots, 1, blocks_dev), jnp.int32),
            pltpu.VMEM((slots, 1, blocks_dev), jnp.int32),
            pltpu.SMEM((blocks_dev,), jnp.int32),
            pltpu.VMEM((1, rows), F32),
            pltpu.VMEM((1, rows), F32),
            dma((5,)),
            pltpu.VMEM((cuts, patterns.shape[1], link_rows // cuts, block_rows), BF16),
            pltpu.VMEM((states_dev, members), BF16),
            dma((cuts,)),
            dma,
            pltpu.VMEM((16, link_rows // cuts, block_rows), F32),
            pltpu.VMEM((16, link_rows // cuts, block_rows), F32),
            pltpu.VMEM((2 * SPAN, link_blocks * link_rows // cuts, block_rows), BF16),
            pltpu.VMEM((table_rows, 128), jnp.int32),
            pltpu.SMEM((table_rows, 128), jnp.int32),
            dma,
            pltpu.VMEM((link_blocks * link_rows, members), F32),
            pltpu.VMEM((pairs, rows, members), F32),
            pltpu.VMEM((pairs, rows, members), F32),
            pltpu.VMEM((pairs // 2, rows, members), F32),
            pltpu.VMEM((pairs // 2, rows, members), F32),
            pltpu.VMEM((members, members), F32),
            pltpu.VMEM((half, members), F32),
            pltpu.VMEM((half, members), F32),
            pltpu.VMEM((ring - 1, piece, members), F32),
            pltpu.VMEM((piece, members), F32),
            pltpu.VMEM((members, members), F32),
            dma((2 * steps,)), dma((2 * steps,)),
            dma((steps,)), dma((steps,)),
            dma((steps,)), dma((steps,)),
            dma, dma,
            dma((ring,)), dma((ring,)),
            dma((ring,)), dma((ring,)),
            dma, dma,
        ],
        compiler_params=pltpu.CompilerParams(
            collective_id=0, has_side_effects=True, vmem_limit_bytes=WIDE_GRANT
        ),
    )(
        jnp.transpose(pattern_ids, (2, 0, 1)), jnp.transpose(link_targets, (2, 0, 1)), live_counts,
        patterns[0], background, counts_obs, obs_var,
    )
    own_rows = states_dev // n_link
    return pl.pallas_call(
        update_kernel,
        out_shape=jax.ShapeDtypeStruct((own_rows, members), BF16),
        in_specs=[hbm, vmem, hbm],
        out_specs=hbm,
        scratch_shapes=[
            pltpu.SMEM((blocks_dev,), jnp.int32),
            pltpu.VMEM((own_rows, members), BF16),
            pltpu.VMEM((own_rows, members), BF16),
            dma,
            dma,
            dma((own_rows // block_rows,)),
        ],
        compiler_params=grant,
    )(live_counts, pltpu.with_memory_space_constraint(gram, pltpu.VMEM), background)


def solution(mesh):
    placed = (
        P("orig", None),
        P("orig"),
        P("link", "orig", None, None),
        P("link", "orig", None),
        P("link", "orig", None),
        P("link", "orig"),
        P("link", "orig"),
    )
    return jax.shard_map(
        per_device, mesh=mesh, in_specs=placed, out_specs=P(("orig", "link"), None), check_vma=False
    )
```

```python
import functools

import jax
import jax.numpy as jnp
from jax import lax
from jax.experimental import pallas as pl
from jax.experimental.pallas import tpu as pltpu
from jax.sharding import PartitionSpec as P

NS_ITERS = 4
CUTS = 4
SPAN = 8
WIDE_GRANT = 67043328-900*1024
MESH = pl.DeviceIdType.MESH
F32 = jnp.float32
BF16 = jnp.bfloat16


def repeat(count, body):
    if count <= 16:
        for step in range(count):
            body(step)
    else:
        lax.fori_loop(0, count, lambda step, carry: (body(step), carry)[1], 0)


def xor(a, b, size):
    total = 0
    bit = 1
    while bit < size:
        total = total + ((a // bit) % 2 + (b // bit) % 2) % 2 * bit
        bit *= 2
    return total


def split(x):
    high = x.astype(BF16)
    return high, (x - high.astype(F32)).astype(BF16)


def mm3(a, b):
    a_high, a_low = split(a)
    b_high, b_low = split(b)
    left = jnp.concatenate([a_high, a_low, a_high], axis=1)
    right = jnp.concatenate([b_low, b_high, b_high], axis=0)
    height = left.shape[0] // 2
    if height % 16:
        return jnp.dot(left, right, preferred_element_type=F32)
    return jnp.concatenate(
        [jnp.dot(left[0:height], right, preferred_element_type=F32), jnp.dot(left[height:], right, preferred_element_type=F32)],
        axis=0,
    )


def sort_slots(ids_ref, targets_ref, table_ref, tiles, link_blocks):
    slots = ids_ref.shape[0]
    bits = max(1, (tiles - 1).bit_length())
    per_word = 31 // bits
    targets = [targets_ref[slot] for slot in range(slots)]
    ones = [jnp.left_shift(jnp.ones_like(target), target * 4) for target in targets]
    tally = functools.reduce(lambda a, b: a + b, ones)
    starts = jnp.zeros_like(tally)
    for shift in range(1, 8):
        starts = starts + jnp.left_shift(tally, jnp.full_like(tally, 4 * shift))
    place = starts
    words = [jnp.zeros_like(tally) for _ in range(pl.cdiv(slots, per_word))]
    for slot in range(slots):
        rank = jnp.bitwise_and(jnp.right_shift(place, targets[slot] * 4), 15)
        place = place + ones[slot]
        tile = ids_ref[slot]
        for word in range(len(words)):
            local = rank - word * per_word
            inside = (local >= 0) & (local < per_word)
            shifted = jnp.left_shift(tile, jnp.where(inside, local * bits, 0))
            words[word] = words[word] + jnp.where(inside, shifted, 0)
    rows = []
    for slot in range(slots):
        amount = jnp.full_like(tally, slot % per_word * bits)
        rows.append(jnp.bitwise_and(jnp.right_shift(words[slot // per_word], amount), 2**bits - 1))
    for target in range(1, link_blocks):
        rows.append(jnp.bitwise_and(jnp.right_shift(starts, jnp.full_like(tally, 4 * target)), 15))
    for index, row in enumerate(rows):
        table_ref[index : index + 1, 0 : row.shape[1]] = row


def build_group(table_ref, tiles_ref, prefix_refs, lhs_ref, group, cut_index, slots, link_blocks):
    tiles, cut_rows, block_rows = tiles_ref.shape[1:]
    span = lhs_ref.shape[0] // 2
    for index in range(span):
        prefix_ref = prefix_refs[index % len(prefix_refs)]
        block = group * span + index
        total = jnp.zeros((cut_rows, block_rows), F32)
        for slot in range(slots):
            tile = table_ref[slot, block]
            total = total + tiles_ref[cut_index, tile].astype(F32)
            prefix_ref[slot + 1] = total
        before = None
        for target in range(link_blocks):
            upto = total
            if target < link_blocks - 1:
                end = table_ref[slots + target, block]
                upto = prefix_ref[end]
            high, low = split(upto if before is None else upto - before)
            before = upto
            rows = slice(target * cut_rows, (target + 1) * cut_rows)
            lhs_ref[index, rows] = high
            lhs_ref[span + index, rows] = low


def predict_cut(table_ref, tiles_ref, states_ref, prefix_refs, lhs_ref, term_ref, cut_index, cuts, slots):
    cut_rows, block_rows = tiles_ref.shape[2:]
    link_rows = cut_rows * cuts
    link_blocks = term_ref.shape[0] // link_rows
    span = lhs_ref.shape[0] // 2
    depth = span * block_rows
    groups = states_ref.shape[0] // depth

    def rows_of(target):
        return pl.ds(target * link_rows + cut_index * cut_rows, cut_rows)

    def build(place):
        cut_at = jnp.minimum(place // groups, cuts - 1)
        build_group(table_ref, tiles_ref, prefix_refs, lhs_ref, place % groups, cut_at, slots, link_blocks)

    for target in range(link_blocks):
        term_ref[rows_of(target)] = jnp.zeros((cut_rows, term_ref.shape[1]), F32)
    if cut_index == 0:
        build(0)

    def add_group(group, carry):
        states = states_ref[pl.ds(pl.multiple_of(group * depth, depth), depth)]
        left = jnp.concatenate([lhs_ref[index] for index in range(2 * span)], axis=1)
        product = jnp.dot(left, jnp.concatenate([states, states], axis=0), preferred_element_type=F32)
        build(cut_index * groups + group + 1)
        for target in range(link_blocks):
            term_ref[rows_of(target)] = term_ref[rows_of(target)] + product[target * cut_rows : (target + 1) * cut_rows]
        return carry

    lax.fori_loop(0, groups, add_group, 0)


def column_of(row):
    width = row.shape[1]
    return jnp.broadcast_to(row, (width, width)).T


def transform_of(gram, forcing):
    members = gram.shape[0]
    row = lax.broadcasted_iota(jnp.int32, (members, members), 0)
    column = lax.broadcasted_iota(jnp.int32, (members, members), 1)
    identity = (row == column).astype(F32)
    system = identity + gram * (1.0 / (members - 1.0))
    bound = jnp.max(jnp.sum(jnp.abs(system), axis=1, keepdims=True), axis=0, keepdims=True)
    root = system / bound
    middle = 1.5 * identity - 0.5 * root
    inverse = middle
    root = mm3(root, middle)
    for sweep in range(1, NS_ITERS):
        middle = 1.5 * identity - 0.5 * mm3(inverse, root)
        if sweep < NS_ITERS - 1:
            root = mm3(root, middle)
        inverse = mm3(middle, inverse)
    inner = jnp.sum(inverse * column_of(forcing), axis=0, keepdims=True)
    mean_weights = jnp.sum(inverse * inner, axis=1, keepdims=True) / (bound * (members - 1.0))
    whole = inverse / jnp.sqrt(bound) + mean_weights
    return whole + (1.0 - jnp.sum(whole, axis=0, keepdims=True)) / members


def gram_kernel(
    n_orig, n_link, cuts, ids_hbm, targets_hbm, counts_hbm, tiles_hbm, states_hbm, obs_hbm, var_hbm, out_ref,
    ids_ref, targets_ref, counts_ref, obs_ref, var_ref, small_sem, tiles_ref, states_ref, tiles_sem, states_sem, even_ref, odd_ref, lhs_ref, packed_ref, table_ref, table_sem, term_ref, first_in, sums, side_in, far_in, gram_ref, half_in, half_ref, piece_in, piece_ref, final_ref,
    send1, recv1, send2, recv2, send7, recv7, send3, recv3, send4, recv4, send5, recv5, send6, recv6,
):
    orig = lax.axis_index("orig")
    link = lax.axis_index("link")
    rows = obs_ref.shape[1]
    members = term_ref.shape[1]
    half = members // 2
    pairs = n_orig // 2
    parity = orig % 2
    place = orig // 2
    across = orig + 1 - 2 * parity
    side = link % 2
    twin = link + 1 - 2 * side
    ring = n_orig * n_link // 2
    rank = (link // 2) * n_orig + orig
    owners = min(ring, half // 8)
    piece = half // owners

    def device_of(other):
        return (other % n_orig, (other // n_orig) * 2 + side)

    load_small = [
        pltpu.make_async_copy(source, target, small_sem.at[index])
        for index, (source, target) in enumerate(
            [
                (ids_hbm, ids_ref), (targets_hbm, targets_ref), (counts_hbm, counts_ref),
                (obs_hbm, obs_ref), (var_hbm, var_ref),
            ]
        )
    ]
    for copy in load_small[:3]:
        copy.start()
    load_states = pltpu.make_async_copy(states_hbm, states_ref, states_sem)
    load_states.start()

    def load_tiles(index):
        part = tiles_ref.shape[2]
        return pltpu.make_async_copy(
            tiles_hbm.at[:, pl.ds(index * part, part)], tiles_ref.at[index], tiles_sem.at[index]
        )

    for index in range(cuts):
        load_tiles(index).start()
    for copy in load_small[3:]:
        copy.start()
    near = place % 2
    far = place // 2
    n_far = pairs // 2
    barrier = pltpu.get_barrier_semaphore()

    def greet(other_orig, other_link):
        pl.semaphore_signal(barrier, inc=1, device_id=(other_orig, other_link), device_id_type=MESH)

    greet(across, link)
    greet(2 * (far * 2 + 1 - near) + parity, link)
    repeat(n_far - 1, lambda step: greet(2 * (xor(far, step + 1, n_far) * 2 + near) + parity, link))
    repeat(n_link - 1, lambda step: greet(orig, (link + step + 1) % n_link))

    slots = ids_ref.shape[0]
    blocks = counts_ref.shape[0]
    block_rows = states_ref.shape[0] // blocks
    link_rows = tiles_ref.shape[2] * cuts
    load_small[0].wait()
    load_small[1].wait()
    sort_slots(ids_ref, targets_ref, packed_ref, tiles_ref.shape[1], rows * n_orig // link_rows)
    move_table = pltpu.make_async_copy(packed_ref, table_ref, table_sem)
    move_table.start()
    for prefix_ref in (even_ref, odd_ref):
        prefix_ref[...] = jnp.zeros(prefix_ref.shape, F32)
    position = lax.broadcasted_iota(jnp.int32, (block_rows, members), 0)
    load_small[2].wait()
    load_states.wait()

    def mask_block(block, carry):
        where = pl.ds(pl.multiple_of(block * block_rows, block_rows), block_rows)
        states = states_ref[where]
        states_ref[where] = jnp.where(position < counts_ref[block], states, jnp.zeros_like(states))
        return carry

    lax.fori_loop(0, blocks, mask_block, 0, unroll=2)
    for index in range(cuts):
        load_tiles(index).wait()
    move_table.wait()

    cut_rows = rows // cuts
    steps = n_far * cuts

    def owner(step, flip):
        other = xor(far, n_far - 1 - step // cuts, n_far)
        return other * 2 + (near + flip) % 2

    def term_rows(index, step):
        return pl.ds(pl.multiple_of(index * rows + step % cuts * cut_rows, cut_rows), cut_rows)

    def cut(step):
        return pl.ds(pl.multiple_of(step % cuts * cut_rows, cut_rows), cut_rows)

    def slot(step, flip):
        return step // cuts * 2 + 1 - flip

    def first(step, flip):
        index = slot(step, flip) * cuts + step % cuts
        return pltpu.make_async_remote_copy(
            src_ref=term_ref.at[term_rows(2 * owner(step, flip) + 1 - parity, step)],
            dst_ref=first_in.at[slot(step, flip), cut(step)],
            send_sem=send1.at[index], recv_sem=recv1.at[index],
            device_id=(across, link), device_id_type=MESH,
        )

    def beside(step):
        return pltpu.make_async_remote_copy(
            src_ref=sums.at[slot(step, 1), cut(step)], dst_ref=side_in.at[step // cuts, cut(step)],
            send_sem=send2.at[step], recv_sem=recv2.at[step],
            device_id=(2 * (far * 2 + 1 - near) + parity, link), device_id_type=MESH,
        )

    def beyond(step):
        return pltpu.make_async_remote_copy(
            src_ref=sums.at[slot(step, 0), cut(step)], dst_ref=far_in.at[step // cuts, cut(step)],
            send_sem=send7.at[step], recv_sem=recv7.at[step],
            device_id=(2 * owner(step, 0) + parity, link), device_id_type=MESH,
        )

    remote = steps - cuts
    lag = min(2, remote, cuts)

    for index in range(cuts):
        predict_cut(
            table_ref, tiles_ref, states_ref, (even_ref, odd_ref), lhs_ref, term_ref, index, cuts, slots
        )
        if index == 0:
            pl.semaphore_wait(barrier, n_far + n_link)

        def first_start(step):
            first(step * cuts + index, 1).start()
            first(step * cuts + index, 0).start()

        repeat(n_far - 1, first_start)
    repeat(cuts, lambda step: first(step + remote, 1).start())
    repeat(cuts, lambda step: first(step + remote, 0).start())

    def add_first(step, flip):
        first(step, flip).wait_recv()
        sums[slot(step, flip), cut(step)] = (
            term_ref[term_rows(2 * owner(step, flip) + parity, step)] + first_in[slot(step, flip), cut(step)]
        )
        if flip:
            beside(step).start()

    def add_beside(step):
        beside(step).wait_recv()
        sums[slot(step, 0), cut(step)] = sums[slot(step, 0), cut(step)] + side_in[step // cuts, cut(step)]

    def pass_on(step):
        add_beside(step)
        beyond(step).start()

    def enter(step):
        add_first(step, 1)
        add_first(step, 0)

    repeat(lag, enter)

    def middle_step(step):
        enter(step + lag)
        pass_on(step)

    repeat(remote - lag, middle_step)
    for step in range(cuts):
        add_first(step + remote, 1)
        if step < lag:
            pass_on(step + (remote - lag))
    for step in range(cuts):
        add_first(step + remote, 0)
        add_beside(step + remote)

    def gather(step):
        beyond(step).wait_recv()
        sums[pairs - 1, cut(step)] = sums[pairs - 1, cut(step)] + far_in[step // cuts, cut(step)]

    repeat(remote, gather)

    load_small[3].wait()
    load_small[4].wait()
    predicted = sums[pairs - 1]
    turned = predicted.T
    weights = 1.0 / var_ref[...]
    mean_row = jnp.sum(turned, axis=0, keepdims=True) / members
    spread = predicted - jnp.sum(predicted, axis=1, keepdims=True) / members
    spread_t = turned - mean_row
    gram = mm3(spread_t * weights, spread)
    pull = jnp.broadcast_to(weights * (obs_ref[...] - mean_row), (8, rows))
    forcing = mm3(pull, spread)
    row = lax.broadcasted_iota(jnp.int32, (half, half), 0)
    column = lax.broadcasted_iota(jnp.int32, (half, half), 1)
    corner = gram[half:, half:]
    halves = (gram[0:half, half:], jnp.where(row <= column, gram[0:half, 0:half], corner))
    diagonal = jnp.sum(jnp.where(row == column, corner, 0.0), axis=0, keepdims=True)
    extras = (forcing[0:1, 0:half], forcing[0:1, half:], diagonal)
    for which, values in enumerate(halves):
        for index in range(owners):
            gram_ref[which, index, 0:piece] = values[index * piece : (index + 1) * piece]
            extra = extras[index] if which == 0 and index < len(extras) else jnp.zeros((1, half), F32)
            gram_ref[which, index, pl.ds(piece, 1)] = extra

    swap = pltpu.make_async_remote_copy(
        src_ref=gram_ref.at[1 - side], dst_ref=half_in,
        send_sem=send3, recv_sem=recv3, device_id=(orig, twin), device_id_type=MESH,
    )
    swap.start()
    swap.wait_recv()
    half_ref[...] = gram_ref[side] + half_in[...]

    def scatter(step):
        other = xor(rank, ring - 1 - step, ring)
        return pltpu.make_async_remote_copy(
            src_ref=half_ref.at[other], dst_ref=piece_in.at[step],
            send_sem=send4.at[step], recv_sem=recv4.at[step],
            device_id=device_of(other), device_id_type=MESH,
        )

    def spread_out(source, step, other):
        return pltpu.make_async_remote_copy(
            src_ref=piece_ref, dst_ref=final_ref.at[side, source],
            send_sem=send5.at[step], recv_sem=recv5.at[step],
            device_id=device_of(other), device_id_type=MESH,
        )

    def guarded(condition, action):
        if owners == ring:
            action()
        else:
            pl.when(condition)(action)

    def scatter_start(step):
        guarded(xor(rank, ring - 1 - step, ring) < owners, lambda: scatter(step).start())

    repeat(ring - 1, scatter_start)

    def reduce_piece():
        piece_ref[...] = half_ref[rank]

        def add(step):
            scatter(step).wait_recv()
            piece_ref[...] = piece_ref[...] + piece_in[step]

        repeat(ring - 1, add)
        repeat(ring - 1, lambda step: spread_out(rank, step, xor(rank, ring - 1 - step, ring)).start())
        final_ref[side, rank] = piece_ref[...]

    guarded(rank < owners, reduce_piece)

    def spread_wait(step):
        other = xor(rank, ring - 1 - step, ring)
        guarded(other < owners, lambda: spread_out(other, step, other).wait_recv())

    repeat(ring - 1, spread_wait)
    share = pltpu.make_async_remote_copy(
        src_ref=final_ref.at[side], dst_ref=final_ref.at[side],
        send_sem=send6, recv_sem=recv6, device_id=(orig, twin), device_id_type=MESH,
    )
    share.start()
    share.wait_recv()

    out_ref[...] = final_ref[...]

    def first_end(step):
        first(step, 1).wait_send()
        first(step, 0).wait_send()
        beside(step).wait_send()

    repeat(steps, first_end)
    repeat(remote, lambda step: beyond(step).wait_send())
    swap.wait_send()

    def scatter_end(step):
        guarded(xor(rank, ring - 1 - step, ring) < owners, lambda: scatter(step).wait_send())

    repeat(ring - 1, scatter_end)
    guarded(
        rank < owners,
        lambda: repeat(
            ring - 1, lambda step: spread_out(rank, step, xor(rank, ring - 1 - step, ring)).wait_send()
        ),
    )
    share.wait_send()


def update_kernel(counts_hbm, final_ref, states_hbm, out_hbm, counts_ref, states_ref, done_ref, counts_sem, states_sem, done_sem):
    link = lax.axis_index("link")
    own_rows, members = done_ref.shape
    half = members // 2
    fetch = pltpu.make_async_copy(
        states_hbm.at[pl.ds(pl.multiple_of(link * own_rows, own_rows), own_rows)], states_ref, states_sem
    )
    fetch.start()
    fetch_counts = pltpu.make_async_copy(counts_hbm, counts_ref, counts_sem)
    fetch_counts.start()
    owners = final_ref.shape[1]
    piece = half // owners
    upper, mixed = [
        jnp.concatenate([final_ref[which, index, 0:piece] for index in range(owners)], axis=0) for which in range(2)
    ]
    first, second, diagonal = [final_ref[0, index, pl.ds(piece, 1)] for index in range(3)]
    row = lax.broadcasted_iota(jnp.int32, (half, half), 0)
    column = lax.broadcasted_iota(jnp.int32, (half, half), 1)
    turned = mixed.T
    head = jnp.where(row <= column, mixed, turned)
    tail = jnp.where(row == column, diagonal, jnp.where(row > column, mixed, turned))
    gram = jnp.concatenate(
        [jnp.concatenate([head, upper], axis=1), jnp.concatenate([upper.T, tail], axis=1)], axis=0
    )
    forcing = jnp.concatenate([first, second], axis=1)
    high, low = split(transform_of(gram, forcing))
    fetch.wait()
    fetch_counts.wait()
    block_rows = states_hbm.shape[0] // counts_ref.shape[0]
    blocks = own_rows // block_rows
    position = lax.broadcasted_iota(jnp.int32, (block_rows, members), 0)

    def store(index):
        where = slice(index * block_rows, (index + 1) * block_rows)
        return pltpu.make_async_copy(done_ref.at[where], out_hbm.at[where], done_sem.at[index])

    for index in range(blocks):
        states = states_ref[index * block_rows : (index + 1) * block_rows]
        updated = jnp.dot(states, low, preferred_element_type=F32) + jnp.dot(
            states, high, preferred_element_type=F32
        )
        living = position < counts_ref[link * blocks + index]
        done_ref[index * block_rows : (index + 1) * block_rows] = jnp.where(
            living, updated, states.astype(F32)
        ).astype(BF16)
        store(index).start()
    for index in range(blocks):
        store(index).wait()


def per_device(background, live_counts, patterns, pattern_ids, link_targets, counts_obs, obs_var):
    n_orig = lax.axis_size("orig")
    n_link = lax.axis_size("link")
    states_dev, members = background.shape
    blocks_dev = live_counts.shape[0]
    block_rows = states_dev // blocks_dev
    link_rows = patterns.shape[2]
    rows = counts_obs.shape[1]
    link_blocks = rows * n_orig // link_rows
    vmem = pl.BlockSpec(memory_space=pltpu.VMEM)
    hbm = pl.BlockSpec(memory_space=pl.ANY)
    dma = pltpu.SemaphoreType.DMA
    grant = pltpu.CompilerParams(vmem_limit_bytes=WIDE_GRANT)
    pairs = n_orig // 2
    ring = n_orig * n_link // 2
    half = members // 2
    owners = min(ring, half // 8)
    packed = (owners, half // owners + 1, half)
    cuts = CUTS if rows == link_rows else 1
    slots = pattern_ids.shape[2]
    table_rows = pl.cdiv(slots + link_blocks, 8) * 8
    steps = pairs // 2 * cuts
    gram = pl.pallas_call(
        functools.partial(gram_kernel, n_orig, n_link, cuts),
        out_shape=pltpu.VMEM((2,) + packed, F32),
        in_specs=[hbm] * 7,
        out_specs=vmem,
        scratch_shapes=[
            pltpu.VMEM((slots, 1, blocks_dev), jnp.int32),
            pltpu.VMEM((slots, 1, blocks_dev), jnp.int32),
            pltpu.SMEM((blocks_dev,), jnp.int32),
            pltpu.VMEM((1, rows), F32),
            pltpu.VMEM((1, rows), F32),
            dma((5,)),
            pltpu.VMEM((cuts, patterns.shape[1], link_rows // cuts, block_rows), BF16),
            pltpu.VMEM((states_dev, members), BF16),
            dma((cuts,)),
            dma,
            pltpu.VMEM((16, link_rows // cuts, block_rows), F32),
            pltpu.VMEM((16, link_rows // cuts, block_rows), F32),
            pltpu.VMEM((2 * SPAN, link_blocks * link_rows // cuts, block_rows), BF16),
            pltpu.VMEM((table_rows, 128), jnp.int32),
            pltpu.SMEM((table_rows, 128), jnp.int32),
            dma,
            pltpu.VMEM((link_blocks * link_rows, members), F32),
            pltpu.VMEM((pairs, rows, members), F32),
            pltpu.VMEM((pairs, rows, members), F32),
            pltpu.VMEM((pairs // 2, rows, members), F32),
            pltpu.VMEM((pairs // 2, rows, members), F32),
            pltpu.VMEM((2,) + packed, F32),
            pltpu.VMEM(packed, F32),
            pltpu.VMEM(packed, F32),
            pltpu.VMEM((ring - 1,) + packed[1:], F32),
            pltpu.VMEM(packed[1:], F32),
            pltpu.VMEM((2,) + packed, F32),
            dma((2 * steps,)), dma((2 * steps,)),
            dma((steps,)), dma((steps,)),
            dma((steps,)), dma((steps,)),
            dma, dma,
            dma((ring,)), dma((ring,)),
            dma((ring,)), dma((ring,)),
            dma, dma,
        ],
        compiler_params=pltpu.CompilerParams(
            collective_id=0, has_side_effects=True, vmem_limit_bytes=WIDE_GRANT
        ),
    )(
        jnp.transpose(pattern_ids, (2, 0, 1)), jnp.transpose(link_targets, (2, 0, 1)), live_counts,
        patterns[0], background, counts_obs, obs_var,
    )
    own_rows = states_dev // n_link
    return pl.pallas_call(
        update_kernel,
        out_shape=jax.ShapeDtypeStruct((own_rows, members), BF16),
        in_specs=[hbm, vmem, hbm],
        out_specs=hbm,
        scratch_shapes=[
            pltpu.SMEM((blocks_dev,), jnp.int32),
            pltpu.VMEM((own_rows, members), BF16),
            pltpu.VMEM((own_rows, members), BF16),
            dma,
            dma,
            dma((own_rows // block_rows,)),
        ],
        compiler_params=grant,
    )(live_counts, pltpu.with_memory_space_constraint(gram, pltpu.VMEM), background)


def solution(mesh):
    placed = (
        P("orig", None),
        P("orig"),
        P("link", "orig", None, None),
        P("link", "orig", None),
        P("link", "orig", None),
        P("link", "orig"),
        P("link", "orig"),
    )
    return jax.shard_map(
        per_device, mesh=mesh, in_specs=placed, out_specs=P(("orig", "link"), None), check_vma=False
    )
```

```python
import functools

import jax
import jax.numpy as jnp
from jax import lax
from jax.experimental import pallas as pl
from jax.experimental.pallas import tpu as pltpu
from jax.sharding import PartitionSpec as P

NS_ITERS = 4
CUTS = 4
SPAN = 8
WIDE_GRANT = 67043328-900*1024
MESH = pl.DeviceIdType.MESH
F32 = jnp.float32
BF16 = jnp.bfloat16


def repeat(count, body):
    if count <= 16:
        for step in range(count):
            body(step)
    else:
        lax.fori_loop(0, count, lambda step, carry: (body(step), carry)[1], 0)


def rolled(count, body):
    lax.fori_loop(0, count, lambda step, carry: (body(step), carry)[1], 0)


def xor(a, b, size):
    total = 0
    bit = 1
    while bit < size:
        total = total + ((a // bit) % 2 + (b // bit) % 2) % 2 * bit
        bit *= 2
    return total


def split(x):
    high = x.astype(BF16)
    return high, (x - high.astype(F32)).astype(BF16)


def mm3(a, b):
    a_high, a_low = split(a)
    b_high, b_low = split(b)
    left = jnp.concatenate([a_high, a_low, a_high], axis=1)
    right = jnp.concatenate([b_low, b_high, b_high], axis=0)
    height = left.shape[0] // 2
    if height % 16:
        return jnp.dot(left, right, preferred_element_type=F32)
    return jnp.concatenate(
        [jnp.dot(left[0:height], right, preferred_element_type=F32), jnp.dot(left[height:], right, preferred_element_type=F32)],
        axis=0,
    )


def sort_slots(ids_ref, targets_ref, table_ref, tiles, link_blocks):
    slots = ids_ref.shape[0]
    bits = max(1, (tiles - 1).bit_length())
    per_word = 31 // bits
    targets = [targets_ref[slot] for slot in range(slots)]
    ones = [jnp.left_shift(jnp.ones_like(target), target * 4) for target in targets]
    tally = functools.reduce(lambda a, b: a + b, ones)
    starts = jnp.zeros_like(tally)
    for shift in range(1, 8):
        starts = starts + jnp.left_shift(tally, jnp.full_like(tally, 4 * shift))
    place = starts
    words = [jnp.zeros_like(tally) for _ in range(pl.cdiv(slots, per_word))]
    for slot in range(slots):
        rank = jnp.bitwise_and(jnp.right_shift(place, targets[slot] * 4), 15)
        place = place + ones[slot]
        tile = ids_ref[slot]
        for word in range(len(words)):
            local = rank - word * per_word
            inside = (local >= 0) & (local < per_word)
            shifted = jnp.left_shift(tile, jnp.where(inside, local * bits, 0))
            words[word] = words[word] + jnp.where(inside, shifted, 0)
    rows = []
    for slot in range(slots):
        amount = jnp.full_like(tally, slot % per_word * bits)
        rows.append(jnp.bitwise_and(jnp.right_shift(words[slot // per_word], amount), 2**bits - 1))
    for target in range(1, link_blocks):
        rows.append(jnp.bitwise_and(jnp.right_shift(starts, jnp.full_like(tally, 4 * target)), 15))
    for index, row in enumerate(rows):
        table_ref[index : index + 1, 0 : row.shape[1]] = row


def build_group(table_ref, tiles_ref, prefix_refs, lhs_ref, group, cut_index, slots, link_blocks):
    tiles, cut_rows, block_rows = tiles_ref.shape[1:]
    span = lhs_ref.shape[0] // 2
    for index in range(span):
        prefix_ref = prefix_refs[index % len(prefix_refs)]
        block = group * span + index
        total = jnp.zeros((cut_rows, block_rows), F32)
        for slot in range(slots):
            tile = table_ref[slot, block]
            total = total + tiles_ref[cut_index, tile].astype(F32)
            prefix_ref[slot + 1] = total
        before = None
        for target in range(link_blocks):
            upto = total
            if target < link_blocks - 1:
                end = table_ref[slots + target, block]
                upto = prefix_ref[end]
            high, low = split(upto if before is None else upto - before)
            before = upto
            rows = slice(target * cut_rows, (target + 1) * cut_rows)
            lhs_ref[index, rows] = high
            lhs_ref[span + index, rows] = low


def predict(table_ref, tiles_ref, states_ref, prefix_refs, lhs_ref, term_ref, slots, after_cut):
    cuts, _, cut_rows, block_rows = tiles_ref.shape
    link_rows = cut_rows * cuts
    link_blocks = term_ref.shape[0] // link_rows
    span = lhs_ref.shape[0] // 2
    depth = span * block_rows
    groups = states_ref.shape[0] // depth

    def build(place):
        cut_at = jnp.minimum(place // groups, cuts - 1)
        build_group(table_ref, tiles_ref, prefix_refs, lhs_ref, place % groups, cut_at, slots, link_blocks)

    build(0)

    def add_group(place, carry):
        group = place % groups
        cut_index = place // groups
        states = states_ref[pl.ds(pl.multiple_of(group * depth, depth), depth)]
        left = jnp.concatenate([lhs_ref[index] for index in range(2 * span)], axis=1)
        product = jnp.dot(left, jnp.concatenate([states, states], axis=0), preferred_element_type=F32)
        build(place + 1)
        for target in range(link_blocks):
            where = pl.ds(pl.multiple_of(target * link_rows + cut_index * cut_rows, cut_rows), cut_rows)
            term_ref[where] = term_ref[where] + product[target * cut_rows : (target + 1) * cut_rows]

        @pl.when(group == groups - 1)
        def _():
            after_cut(cut_index)

        return carry

    lax.fori_loop(0, groups * cuts, add_group, 0)


def column_of(row):
    width = row.shape[1]
    return jnp.broadcast_to(row, (width, width)).T


def transform_of(gram, forcing, root_ref, inverse_ref):
    members = gram.shape[0]
    row = lax.broadcasted_iota(jnp.int32, (members, members), 0)
    column = lax.broadcasted_iota(jnp.int32, (members, members), 1)
    identity = (row == column).astype(F32)
    system = identity + gram * (1.0 / (members - 1.0))
    bound = jnp.max(jnp.sum(jnp.abs(system), axis=1, keepdims=True), axis=0, keepdims=True)
    root = system / bound
    middle = 1.5 * identity - 0.5 * root
    inverse_ref[...] = middle
    root_ref[...] = mm3(root, middle)

    def sweep(index, carry):
        root = root_ref[...]
        inverse = inverse_ref[...]
        middle = 1.5 * identity - 0.5 * mm3(inverse, root)
        root_ref[...] = mm3(root, middle)
        inverse_ref[...] = mm3(middle, inverse)
        return carry

    lax.fori_loop(1, NS_ITERS - 1, sweep, 0)
    inverse = inverse_ref[...]
    inverse = mm3(1.5 * identity - 0.5 * mm3(inverse, root_ref[...]), inverse)
    inner = jnp.sum(inverse * column_of(forcing), axis=0, keepdims=True)
    mean_weights = jnp.sum(inverse * inner, axis=1, keepdims=True) / (bound * (members - 1.0))
    whole = inverse / jnp.sqrt(bound) + mean_weights
    return whole + (1.0 - jnp.sum(whole, axis=0, keepdims=True)) / members


def gram_kernel(
    n_orig, n_link, cuts, ids_hbm, targets_hbm, counts_hbm, tiles_hbm, states_hbm, obs_hbm, var_hbm, out_ref,
    ids_ref, targets_ref, counts_ref, obs_ref, var_ref, small_sem, tiles_ref, states_ref, tiles_sem, states_sem, even_ref, odd_ref, lhs_ref, packed_ref, table_ref, table_sem, term_ref, first_in, sums, side_in, far_in, gram_ref, half_in, half_ref, piece_in, piece_ref, final_ref,
    send1, recv1, send2, recv2, send7, recv7, send3, recv3, send4, recv4, send5, recv5, send6, recv6,
):
    orig = lax.axis_index("orig")
    link = lax.axis_index("link")
    rows = obs_ref.shape[1]
    members = term_ref.shape[1]
    half = members // 2
    pairs = n_orig // 2
    parity = orig % 2
    place = orig // 2
    across = orig + 1 - 2 * parity
    side = link % 2
    twin = link + 1 - 2 * side
    ring = n_orig * n_link // 2
    rank = (link // 2) * n_orig + orig
    owners = min(ring, half // 8)
    piece = half // owners

    def device_of(other):
        return (other % n_orig, (other // n_orig) * 2 + side)

    load_small = [
        pltpu.make_async_copy(source, target, small_sem.at[index])
        for index, (source, target) in enumerate(
            [
                (ids_hbm, ids_ref), (targets_hbm, targets_ref), (counts_hbm, counts_ref),
                (obs_hbm, obs_ref), (var_hbm, var_ref),
            ]
        )
    ]
    for copy in load_small[:3]:
        copy.start()
    load_states = pltpu.make_async_copy(states_hbm, states_ref, states_sem)
    load_states.start()

    def load_tiles(index):
        part = tiles_ref.shape[2]
        return pltpu.make_async_copy(
            tiles_hbm.at[:, pl.ds(index * part, part)], tiles_ref.at[index], tiles_sem.at[index]
        )

    for index in range(cuts):
        load_tiles(index).start()
    for copy in load_small[3:]:
        copy.start()
    near = place % 2
    far = place // 2
    n_far = pairs // 2
    barrier = pltpu.get_barrier_semaphore()

    def greet(other_orig, other_link):
        pl.semaphore_signal(barrier, inc=1, device_id=(other_orig, other_link), device_id_type=MESH)

    greet(across, link)
    greet(2 * (far * 2 + 1 - near) + parity, link)
    repeat(n_far - 1, lambda step: greet(2 * (xor(far, step + 1, n_far) * 2 + near) + parity, link))
    repeat(n_link - 1, lambda step: greet(orig, (link + step + 1) % n_link))

    slots = ids_ref.shape[0]
    blocks = counts_ref.shape[0]
    block_rows = states_ref.shape[0] // blocks
    link_rows = tiles_ref.shape[2] * cuts
    load_small[0].wait()
    load_small[1].wait()
    sort_slots(ids_ref, targets_ref, packed_ref, tiles_ref.shape[1], rows * n_orig // link_rows)
    move_table = pltpu.make_async_copy(packed_ref, table_ref, table_sem)
    move_table.start()
    for prefix_ref in (even_ref, odd_ref):
        prefix_ref[...] = jnp.zeros(prefix_ref.shape, F32)
    position = lax.broadcasted_iota(jnp.int32, (block_rows, members), 0)
    term_ref[...] = jnp.zeros_like(term_ref)
    load_small[2].wait()
    load_states.wait()

    def mask_block(block, carry):
        where = pl.ds(pl.multiple_of(block * block_rows, block_rows), block_rows)
        states = states_ref[where]
        states_ref[where] = jnp.where(position < counts_ref[block], states, jnp.zeros_like(states))
        return carry

    lax.fori_loop(0, blocks, mask_block, 0, unroll=2)
    for index in range(cuts):
        load_tiles(index).wait()
    move_table.wait()

    cut_rows = rows // cuts
    steps = n_far * cuts

    def owner(step, flip):
        other = xor(far, n_far - 1 - step // cuts, n_far)
        return other * 2 + (near + flip) % 2

    def term_rows(index, step):
        return pl.ds(pl.multiple_of(index * rows + step % cuts * cut_rows, cut_rows), cut_rows)

    def cut(step):
        return pl.ds(pl.multiple_of(step % cuts * cut_rows, cut_rows), cut_rows)

    def slot(step, flip):
        return step // cuts * 2 + 1 - flip

    def first(step, flip):
        index = slot(step, flip) * cuts + step % cuts
        return pltpu.make_async_remote_copy(
            src_ref=term_ref.at[term_rows(2 * owner(step, flip) + 1 - parity, step)],
            dst_ref=first_in.at[slot(step, flip), cut(step)],
            send_sem=send1.at[index], recv_sem=recv1.at[index],
            device_id=(across, link), device_id_type=MESH,
        )

    def beside(step):
        return pltpu.make_async_remote_copy(
            src_ref=sums.at[slot(step, 1), cut(step)], dst_ref=side_in.at[step // cuts, cut(step)],
            send_sem=send2.at[step], recv_sem=recv2.at[step],
            device_id=(2 * (far * 2 + 1 - near) + parity, link), device_id_type=MESH,
        )

    def beyond(step):
        return pltpu.make_async_remote_copy(
            src_ref=sums.at[slot(step, 0), cut(step)], dst_ref=far_in.at[step // cuts, cut(step)],
            send_sem=send7.at[step], recv_sem=recv7.at[step],
            device_id=(2 * owner(step, 0) + parity, link), device_id_type=MESH,
        )

    remote = steps - cuts
    lag = min(2, remote, cuts)

    def after_cut(index):
        @pl.when(index == 0)
        def _():
            pl.semaphore_wait(barrier, n_far + n_link)

        def first_start(step):
            first(step * cuts + index, 1).start()
            first(step * cuts + index, 0).start()

        repeat(n_far - 1, first_start)

    predict(table_ref, tiles_ref, states_ref, (even_ref, odd_ref), lhs_ref, term_ref, slots, after_cut)
    repeat(cuts, lambda step: first(step + remote, 1).start())
    repeat(cuts, lambda step: first(step + remote, 0).start())

    def add_first(step, flip):
        first(step, flip).wait_recv()
        sums[slot(step, flip), cut(step)] = (
            term_ref[term_rows(2 * owner(step, flip) + parity, step)] + first_in[slot(step, flip), cut(step)]
        )
        if flip:
            beside(step).start()

    def add_beside(step):
        beside(step).wait_recv()
        sums[slot(step, 0), cut(step)] = sums[slot(step, 0), cut(step)] + side_in[step // cuts, cut(step)]

    def pass_on(step):
        add_beside(step)
        beyond(step).start()

    def enter(step):
        add_first(step, 1)
        add_first(step, 0)

    repeat(lag, enter)

    def middle_step(step):
        enter(step + lag)
        pass_on(step)

    repeat(remote - lag, middle_step)
    for step in range(cuts):
        add_first(step + remote, 1)
        if step < lag:
            pass_on(step + (remote - lag))
    for step in range(cuts):
        add_first(step + remote, 0)
        add_beside(step + remote)

    def gather(step):
        beyond(step).wait_recv()
        sums[pairs - 1, cut(step)] = sums[pairs - 1, cut(step)] + far_in[step // cuts, cut(step)]

    repeat(remote, gather)

    load_small[3].wait()
    load_small[4].wait()
    predicted = sums[pairs - 1]
    turned = predicted.T
    weights = 1.0 / var_ref[...]
    mean_row = jnp.sum(turned, axis=0, keepdims=True) / members
    spread = predicted - jnp.sum(predicted, axis=1, keepdims=True) / members
    spread_t = turned - mean_row
    gram = mm3(spread_t * weights, spread)
    pull = jnp.broadcast_to(weights * (obs_ref[...] - mean_row), (8, rows))
    forcing = mm3(pull, spread)
    row = lax.broadcasted_iota(jnp.int32, (half, half), 0)
    column = lax.broadcasted_iota(jnp.int32, (half, half), 1)
    corner = gram[half:, half:]
    halves = (gram[0:half, half:], jnp.where(row <= column, gram[0:half, 0:half], corner))
    diagonal = jnp.sum(jnp.where(row == column, corner, 0.0), axis=0, keepdims=True)
    extras = (forcing[0:1, 0:half], forcing[0:1, half:], diagonal)
    for which, values in enumerate(halves):
        for index in range(owners):
            gram_ref[which, index, 0:piece] = values[index * piece : (index + 1) * piece]
            extra = extras[index] if which == 0 and index < len(extras) else jnp.zeros((1, half), F32)
            gram_ref[which, index, pl.ds(piece, 1)] = extra

    swap = pltpu.make_async_remote_copy(
        src_ref=gram_ref.at[1 - side], dst_ref=half_in,
        send_sem=send3, recv_sem=recv3, device_id=(orig, twin), device_id_type=MESH,
    )
    swap.start()
    swap.wait_recv()
    half_ref[...] = gram_ref[side] + half_in[...]

    def scatter(step):
        other = xor(rank, ring - 1 - step, ring)
        return pltpu.make_async_remote_copy(
            src_ref=half_ref.at[other], dst_ref=piece_in.at[step],
            send_sem=send4.at[step], recv_sem=recv4.at[step],
            device_id=device_of(other), device_id_type=MESH,
        )

    def spread_out(source, step, other):
        return pltpu.make_async_remote_copy(
            src_ref=piece_ref, dst_ref=final_ref.at[side, source],
            send_sem=send5.at[step], recv_sem=recv5.at[step],
            device_id=device_of(other), device_id_type=MESH,
        )

    def guarded(condition, action):
        if owners == ring:
            action()
        else:
            pl.when(condition)(action)

    def scatter_start(step):
        guarded(xor(rank, ring - 1 - step, ring) < owners, lambda: scatter(step).start())

    repeat(ring - 1, scatter_start)

    def reduce_piece():
        def arrive(step):
            scatter(step).wait_recv()
            return piece_in[step]

        if ring <= 16:
            total = half_ref[rank]
            for step in range(ring - 1):
                total = total + arrive(step)
            piece_ref[...] = total
        else:
            piece_ref[...] = half_ref[rank]

            def add(step):
                piece_ref[...] = piece_ref[...] + arrive(step)

            repeat(ring - 1, add)
        repeat(ring - 1, lambda step: spread_out(rank, step, xor(rank, ring - 1 - step, ring)).start())
        final_ref[side, rank] = piece_ref[...]

    guarded(rank < owners, reduce_piece)

    def spread_wait(step):
        other = xor(rank, ring - 1 - step, ring)
        guarded(other < owners, lambda: spread_out(other, step, other).wait_recv())

    repeat(ring - 1, spread_wait)
    share = pltpu.make_async_remote_copy(
        src_ref=final_ref.at[side], dst_ref=final_ref.at[side],
        send_sem=send6, recv_sem=recv6, device_id=(orig, twin), device_id_type=MESH,
    )
    share.start()
    share.wait_recv()

    out_ref[...] = final_ref[...]

    def first_end(step):
        first(step, 1).wait_send()
        first(step, 0).wait_send()
        beside(step).wait_send()

    rolled(steps, first_end)
    rolled(remote, lambda step: beyond(step).wait_send())
    swap.wait_send()

    def scatter_end(step):
        guarded(xor(rank, ring - 1 - step, ring) < owners, lambda: scatter(step).wait_send())

    rolled(ring - 1, scatter_end)
    guarded(
        rank < owners,
        lambda: rolled(
            ring - 1, lambda step: spread_out(rank, step, xor(rank, ring - 1 - step, ring)).wait_send()
        ),
    )
    share.wait_send()


def update_kernel(counts_hbm, final_ref, states_hbm, out_hbm, counts_ref, states_ref, done_ref, counts_sem, states_sem, done_sem, root_ref, inverse_ref):
    link = lax.axis_index("link")
    own_rows, members = done_ref.shape
    half = members // 2
    fetch = pltpu.make_async_copy(
        states_hbm.at[pl.ds(pl.multiple_of(link * own_rows, own_rows), own_rows)], states_ref, states_sem
    )
    fetch.start()
    fetch_counts = pltpu.make_async_copy(counts_hbm, counts_ref, counts_sem)
    fetch_counts.start()
    owners = final_ref.shape[1]
    piece = half // owners
    upper, mixed = [
        jnp.concatenate([final_ref[which, index, 0:piece] for index in range(owners)], axis=0) for which in range(2)
    ]
    first, second, diagonal = [final_ref[0, index, pl.ds(piece, 1)] for index in range(3)]
    row = lax.broadcasted_iota(jnp.int32, (half, half), 0)
    column = lax.broadcasted_iota(jnp.int32, (half, half), 1)
    turned = mixed.T
    head = jnp.where(row <= column, mixed, turned)
    tail = jnp.where(row == column, diagonal, jnp.where(row > column, mixed, turned))
    gram = jnp.concatenate(
        [jnp.concatenate([head, upper], axis=1), jnp.concatenate([upper.T, tail], axis=1)], axis=0
    )
    forcing = jnp.concatenate([first, second], axis=1)
    high, low = split(transform_of(gram, forcing, root_ref, inverse_ref))
    fetch.wait()
    fetch_counts.wait()
    block_rows = states_hbm.shape[0] // counts_ref.shape[0]
    blocks = own_rows // block_rows
    position = lax.broadcasted_iota(jnp.int32, (block_rows, members), 0)

    def store(index):
        where = slice(index * block_rows, (index + 1) * block_rows)
        return pltpu.make_async_copy(done_ref.at[where], out_hbm.at[where], done_sem.at[index])

    for index in range(blocks):
        states = states_ref[index * block_rows : (index + 1) * block_rows]
        updated = jnp.dot(
            jnp.concatenate([states, states], axis=1), jnp.concatenate([low, high], axis=0), preferred_element_type=F32
        )
        living = position < counts_ref[link * blocks + index]
        done_ref[index * block_rows : (index + 1) * block_rows] = jnp.where(
            living, updated, states.astype(F32)
        ).astype(BF16)
        store(index).start()
    for index in range(blocks):
        store(index).wait()


def per_device(background, live_counts, patterns, pattern_ids, link_targets, counts_obs, obs_var):
    n_orig = lax.axis_size("orig")
    n_link = lax.axis_size("link")
    states_dev, members = background.shape
    blocks_dev = live_counts.shape[0]
    block_rows = states_dev // blocks_dev
    link_rows = patterns.shape[2]
    rows = counts_obs.shape[1]
    link_blocks = rows * n_orig // link_rows
    vmem = pl.BlockSpec(memory_space=pltpu.VMEM)
    hbm = pl.BlockSpec(memory_space=pl.ANY)
    dma = pltpu.SemaphoreType.DMA
    grant = pltpu.CompilerParams(vmem_limit_bytes=WIDE_GRANT)
    pairs = n_orig // 2
    ring = n_orig * n_link // 2
    half = members // 2
    owners = min(ring, half // 8)
    packed = (owners, half // owners + 1, half)
    cuts = CUTS if rows == link_rows else 1
    slots = pattern_ids.shape[2]
    table_rows = pl.cdiv(slots + link_blocks, 8) * 8
    steps = pairs // 2 * cuts
    gram = pl.pallas_call(
        functools.partial(gram_kernel, n_orig, n_link, cuts),
        out_shape=pltpu.VMEM((2,) + packed, F32),
        in_specs=[hbm] * 7,
        out_specs=vmem,
        scratch_shapes=[
            pltpu.VMEM((slots, 1, blocks_dev), jnp.int32),
            pltpu.VMEM((slots, 1, blocks_dev), jnp.int32),
            pltpu.SMEM((blocks_dev,), jnp.int32),
            pltpu.VMEM((1, rows), F32),
            pltpu.VMEM((1, rows), F32),
            dma((5,)),
            pltpu.VMEM((cuts, patterns.shape[1], link_rows // cuts, block_rows), BF16),
            pltpu.VMEM((states_dev, members), BF16),
            dma((cuts,)),
            dma,
            pltpu.VMEM((16, link_rows // cuts, block_rows), F32),
            pltpu.VMEM((16, link_rows // cuts, block_rows), F32),
            pltpu.VMEM((2 * SPAN, link_blocks * link_rows // cuts, block_rows), BF16),
            pltpu.VMEM((table_rows, 128), jnp.int32),
            pltpu.SMEM((table_rows, 128), jnp.int32),
            dma,
            pltpu.VMEM((link_blocks * link_rows, members), F32),
            pltpu.VMEM((pairs, rows, members), F32),
            pltpu.VMEM((pairs, rows, members), F32),
            pltpu.VMEM((pairs // 2, rows, members), F32),
            pltpu.VMEM((pairs // 2, rows, members), F32),
            pltpu.VMEM((2,) + packed, F32),
            pltpu.VMEM(packed, F32),
            pltpu.VMEM(packed, F32),
            pltpu.VMEM((ring - 1,) + packed[1:], F32),
            pltpu.VMEM(packed[1:], F32),
            pltpu.VMEM((2,) + packed, F32),
            dma((2 * steps,)), dma((2 * steps,)),
            dma((steps,)), dma((steps,)),
            dma((steps,)), dma((steps,)),
            dma, dma,
            dma((ring,)), dma((ring,)),
            dma((ring,)), dma((ring,)),
            dma, dma,
        ],
        compiler_params=pltpu.CompilerParams(
            collective_id=0, has_side_effects=True, vmem_limit_bytes=WIDE_GRANT
        ),
    )(
        jnp.transpose(pattern_ids, (2, 0, 1)), jnp.transpose(link_targets, (2, 0, 1)), live_counts,
        patterns[0], background, counts_obs, obs_var,
    )
    own_rows = states_dev // n_link
    return pl.pallas_call(
        update_kernel,
        out_shape=jax.ShapeDtypeStruct((own_rows, members), BF16),
        in_specs=[hbm, vmem, hbm],
        out_specs=hbm,
        scratch_shapes=[
            pltpu.SMEM((blocks_dev,), jnp.int32),
            pltpu.VMEM((own_rows, members), BF16),
            pltpu.VMEM((own_rows, members), BF16),
            dma,
            dma,
            dma((own_rows // block_rows,)),
            pltpu.VMEM((members, members), F32),
            pltpu.VMEM((members, members), F32),
        ],
        compiler_params=grant,
    )(live_counts, pltpu.with_memory_space_constraint(gram, pltpu.VMEM), background)


def solution(mesh):
    placed = (
        P("orig", None),
        P("orig"),
        P("link", "orig", None, None),
        P("link", "orig", None),
        P("link", "orig", None),
        P("link", "orig"),
        P("link", "orig"),
    )
    return jax.shard_map(
        per_device, mesh=mesh, in_specs=placed, out_specs=P(("orig", "link"), None), check_vma=False
    )
```

```python
import functools

import jax
import jax.numpy as jnp
from jax import lax
from jax.experimental import pallas as pl
from jax.experimental.pallas import tpu as pltpu
from jax.sharding import PartitionSpec as P

NS_ITERS = 4
CUTS = 4
SPAN = 8
WIDE_GRANT = 67043328-900*1024
MESH = pl.DeviceIdType.MESH
F32 = jnp.float32
BF16 = jnp.bfloat16


def repeat(count, body):
    if count <= 16:
        for step in range(count):
            body(step)
    else:
        lax.fori_loop(0, count, lambda step, carry: (body(step), carry)[1], 0)


def rolled(count, body):
    lax.fori_loop(0, count, lambda step, carry: (body(step), carry)[1], 0)


def xor(a, b, size):
    total = 0
    bit = 1
    while bit < size:
        total = total + ((a // bit) % 2 + (b // bit) % 2) % 2 * bit
        bit *= 2
    return total


def split(x):
    high = x.astype(BF16)
    return high, (x - high.astype(F32)).astype(BF16)


def mm3(a, b):
    a_high, a_low = split(a)
    b_high, b_low = split(b)
    left = jnp.concatenate([a_high, a_low, a_high], axis=1)
    right = jnp.concatenate([b_low, b_high, b_high], axis=0)
    height = left.shape[0] // 2
    if height % 16:
        return jnp.dot(left, right, preferred_element_type=F32)
    return jnp.concatenate(
        [jnp.dot(left[0:height], right, preferred_element_type=F32), jnp.dot(left[height:], right, preferred_element_type=F32)],
        axis=0,
    )


def sort_slots(ids_ref, targets_ref, table_ref, tiles, link_blocks):
    slots = ids_ref.shape[0]
    bits = max(1, (tiles - 1).bit_length())
    per_word = 31 // bits
    targets = [targets_ref[slot] for slot in range(slots)]
    ones = [jnp.left_shift(jnp.ones_like(target), target * 4) for target in targets]
    tally = functools.reduce(lambda a, b: a + b, ones)
    starts = jnp.zeros_like(tally)
    for shift in range(1, 8):
        starts = starts + jnp.left_shift(tally, jnp.full_like(tally, 4 * shift))
    place = starts
    words = [jnp.zeros_like(tally) for _ in range(pl.cdiv(slots, per_word))]
    for slot in range(slots):
        rank = jnp.bitwise_and(jnp.right_shift(place, targets[slot] * 4), 15)
        place = place + ones[slot]
        tile = ids_ref[slot]
        for word in range(len(words)):
            local = rank - word * per_word
            inside = (local >= 0) & (local < per_word)
            shifted = jnp.left_shift(tile, jnp.where(inside, local * bits, 0))
            words[word] = words[word] + jnp.where(inside, shifted, 0)
    rows = []
    for slot in range(slots):
        amount = jnp.full_like(tally, slot % per_word * bits)
        rows.append(jnp.bitwise_and(jnp.right_shift(words[slot // per_word], amount), 2**bits - 1))
    for target in range(1, link_blocks):
        rows.append(jnp.bitwise_and(jnp.right_shift(starts, jnp.full_like(tally, 4 * target)), 15))
    for index, row in enumerate(rows):
        table_ref[index : index + 1, 0 : row.shape[1]] = row


def build_group(table_ref, tiles_ref, prefix_refs, lhs_ref, group, cut_index, slots, link_blocks):
    tiles, cut_rows, block_rows = tiles_ref.shape[1:]
    span = lhs_ref.shape[0] // 2
    for index in range(span):
        prefix_ref = prefix_refs[index % len(prefix_refs)]
        block = group * span + index
        total = jnp.zeros((cut_rows, block_rows), F32)
        for slot in range(slots):
            tile = table_ref[slot, block]
            total = total + tiles_ref[cut_index, tile].astype(F32)
            prefix_ref[slot + 1] = total
        before = None
        for target in range(link_blocks):
            upto = total
            if target < link_blocks - 1:
                end = table_ref[slots + target, block]
                upto = prefix_ref[end]
            high, low = split(upto if before is None else upto - before)
            before = upto
            rows = slice(target * cut_rows, (target + 1) * cut_rows)
            lhs_ref[index, rows] = high
            lhs_ref[span + index, rows] = low


def predict(table_ref, tiles_ref, states_ref, prefix_refs, lhs_ref, term_ref, slots, after_cut):
    cuts, _, cut_rows, block_rows = tiles_ref.shape
    link_rows = cut_rows * cuts
    link_blocks = term_ref.shape[0] // link_rows
    span = lhs_ref.shape[0] // 2
    depth = span * block_rows
    groups = states_ref.shape[0] // depth

    def build(place):
        cut_at = jnp.minimum(place // groups, cuts - 1)
        build_group(table_ref, tiles_ref, prefix_refs, lhs_ref, place % groups, cut_at, slots, link_blocks)

    build(0)

    def add_group(place, carry):
        group = place % groups
        cut_index = place // groups
        states = states_ref[pl.ds(pl.multiple_of(group * depth, depth), depth)]
        left = jnp.concatenate([lhs_ref[index] for index in range(2 * span)], axis=1)
        product = jnp.dot(left, jnp.concatenate([states, states], axis=0), preferred_element_type=F32)
        build(place + 1)
        for target in range(link_blocks):
            where = pl.ds(pl.multiple_of(target * link_rows + cut_index * cut_rows, cut_rows), cut_rows)
            term_ref[where] = term_ref[where] + product[target * cut_rows : (target + 1) * cut_rows]

        @pl.when(group == groups - 1)
        def _():
            after_cut(cut_index)

        return carry

    lax.fori_loop(0, groups * cuts, add_group, 0)


def column_of(row):
    width = row.shape[1]
    return jnp.broadcast_to(row, (width, width)).T


def transform_of(gram, forcing, root_ref, inverse_ref):
    members = gram.shape[0]
    row = lax.broadcasted_iota(jnp.int32, (members, members), 0)
    column = lax.broadcasted_iota(jnp.int32, (members, members), 1)
    identity = (row == column).astype(F32)
    system = identity + gram * (1.0 / (members - 1.0))
    bound = jnp.max(jnp.sum(jnp.abs(system), axis=0, keepdims=True), axis=1, keepdims=True)
    shrink = 1.0 / bound
    root = system * shrink
    middle = 1.5 * identity - 0.5 * root
    inverse_ref[...] = middle
    root_ref[...] = mm3(root, middle)

    def sweep(index, carry):
        root = root_ref[...]
        inverse = inverse_ref[...]
        middle = 1.5 * identity - 0.5 * mm3(inverse, root)
        root_ref[...] = mm3(root, middle)
        inverse_ref[...] = mm3(middle, inverse)
        return carry

    lax.fori_loop(1, NS_ITERS - 1, sweep, 0)
    inverse = inverse_ref[...]
    inverse = mm3(1.5 * identity - 0.5 * mm3(inverse, root_ref[...]), inverse)
    scale = 1.0 / jnp.sqrt(bound)
    share = shrink / (members - 1.0)
    inner = jnp.sum(inverse * column_of(forcing), axis=0, keepdims=True)
    mean_weights = jnp.sum(inverse * inner, axis=1, keepdims=True) * share
    across = jnp.sum(inverse, axis=0, keepdims=True)
    total = across * scale + jnp.sum(across * inner, axis=1, keepdims=True) * share
    return inverse * scale + (1.0 - total) / members + mean_weights


def gram_kernel(
    n_orig, n_link, cuts, ids_hbm, targets_hbm, counts_hbm, tiles_hbm, states_hbm, obs_hbm, var_hbm, out_ref,
    ids_ref, targets_ref, counts_ref, obs_ref, var_ref, small_sem, tiles_ref, states_ref, tiles_sem, states_sem, even_ref, odd_ref, lhs_ref, packed_ref, table_ref, table_sem, term_ref, first_in, sums, side_in, far_in, gram_ref, half_in, half_ref, piece_in, piece_ref, final_ref,
    send1, recv1, send2, recv2, send7, recv7, send3, recv3, send4, recv4, send5, recv5, send6, recv6,
):
    orig = lax.axis_index("orig")
    link = lax.axis_index("link")
    rows = obs_ref.shape[1]
    members = term_ref.shape[1]
    half = members // 2
    pairs = n_orig // 2
    parity = orig % 2
    place = orig // 2
    across = orig + 1 - 2 * parity
    side = link % 2
    twin = link + 1 - 2 * side
    ring = n_orig * n_link // 2
    rank = (link // 2) * n_orig + orig
    owners = min(ring, half // 8)
    piece = half // owners

    def device_of(other):
        return (other % n_orig, (other // n_orig) * 2 + side)

    load_small = [
        pltpu.make_async_copy(source, target, small_sem.at[index])
        for index, (source, target) in enumerate(
            [
                (ids_hbm, ids_ref), (targets_hbm, targets_ref), (counts_hbm, counts_ref),
                (obs_hbm, obs_ref), (var_hbm, var_ref),
            ]
        )
    ]
    for copy in load_small[:3]:
        copy.start()
    load_states = pltpu.make_async_copy(states_hbm, states_ref, states_sem)
    load_states.start()

    def load_tiles(index):
        part = tiles_ref.shape[2]
        return pltpu.make_async_copy(
            tiles_hbm.at[:, pl.ds(index * part, part)], tiles_ref.at[index], tiles_sem.at[index]
        )

    for index in range(cuts):
        load_tiles(index).start()
    for copy in load_small[3:]:
        copy.start()
    near = place % 2
    far = place // 2
    n_far = pairs // 2
    barrier = pltpu.get_barrier_semaphore()

    def greet(other_orig, other_link):
        pl.semaphore_signal(barrier, inc=1, device_id=(other_orig, other_link), device_id_type=MESH)

    greet(across, link)
    greet(2 * (far * 2 + 1 - near) + parity, link)
    repeat(n_far - 1, lambda step: greet(2 * (xor(far, step + 1, n_far) * 2 + near) + parity, link))
    repeat(n_link - 1, lambda step: greet(orig, (link + step + 1) % n_link))

    slots = ids_ref.shape[0]
    blocks = counts_ref.shape[0]
    block_rows = states_ref.shape[0] // blocks
    link_rows = tiles_ref.shape[2] * cuts
    load_small[0].wait()
    load_small[1].wait()
    sort_slots(ids_ref, targets_ref, packed_ref, tiles_ref.shape[1], rows * n_orig // link_rows)
    move_table = pltpu.make_async_copy(packed_ref, table_ref, table_sem)
    move_table.start()
    for prefix_ref in (even_ref, odd_ref):
        prefix_ref[...] = jnp.zeros(prefix_ref.shape, F32)
    position = lax.broadcasted_iota(jnp.int32, (block_rows, members), 0)
    term_ref[...] = jnp.zeros_like(term_ref)
    load_small[2].wait()
    load_states.wait()

    def mask_block(block, carry):
        where = pl.ds(pl.multiple_of(block * block_rows, block_rows), block_rows)
        states = states_ref[where]
        states_ref[where] = jnp.where(position < counts_ref[block], states, jnp.zeros_like(states))
        return carry

    lax.fori_loop(0, blocks, mask_block, 0, unroll=2)
    for index in range(cuts):
        load_tiles(index).wait()
    move_table.wait()

    cut_rows = rows // cuts
    steps = n_far * cuts

    def owner(step, flip):
        other = xor(far, n_far - 1 - step // cuts, n_far)
        return other * 2 + (near + flip) % 2

    def term_rows(index, step):
        return pl.ds(pl.multiple_of(index * rows + step % cuts * cut_rows, cut_rows), cut_rows)

    def cut(step):
        return pl.ds(pl.multiple_of(step % cuts * cut_rows, cut_rows), cut_rows)

    def slot(step, flip):
        return step // cuts * 2 + 1 - flip

    def first(step, flip):
        index = slot(step, flip) * cuts + step % cuts
        return pltpu.make_async_remote_copy(
            src_ref=term_ref.at[term_rows(2 * owner(step, flip) + 1 - parity, step)],
            dst_ref=first_in.at[slot(step, flip), cut(step)],
            send_sem=send1.at[index], recv_sem=recv1.at[index],
            device_id=(across, link), device_id_type=MESH,
        )

    def beside(step):
        return pltpu.make_async_remote_copy(
            src_ref=sums.at[slot(step, 1), cut(step)], dst_ref=side_in.at[step // cuts, cut(step)],
            send_sem=send2.at[step], recv_sem=recv2.at[step],
            device_id=(2 * (far * 2 + 1 - near) + parity, link), device_id_type=MESH,
        )

    def beyond(step):
        return pltpu.make_async_remote_copy(
            src_ref=sums.at[slot(step, 0), cut(step)], dst_ref=far_in.at[step // cuts, cut(step)],
            send_sem=send7.at[step], recv_sem=recv7.at[step],
            device_id=(2 * owner(step, 0) + parity, link), device_id_type=MESH,
        )

    remote = steps - cuts
    lag = min(2, remote, cuts)

    def after_cut(index):
        @pl.when(index == 0)
        def _():
            pl.semaphore_wait(barrier, n_far + n_link)

        def first_start(step):
            first(step * cuts + index, 1).start()
            first(step * cuts + index, 0).start()

        repeat(n_far - 1, first_start)

    predict(table_ref, tiles_ref, states_ref, (even_ref, odd_ref), lhs_ref, term_ref, slots, after_cut)
    repeat(cuts, lambda step: first(step + remote, 1).start())
    repeat(cuts, lambda step: first(step + remote, 0).start())

    def add_first(step, flip):
        first(step, flip).wait_recv()
        sums[slot(step, flip), cut(step)] = (
            term_ref[term_rows(2 * owner(step, flip) + parity, step)] + first_in[slot(step, flip), cut(step)]
        )
        if flip:
            beside(step).start()

    def add_beside(step):
        beside(step).wait_recv()
        sums[slot(step, 0), cut(step)] = sums[slot(step, 0), cut(step)] + side_in[step // cuts, cut(step)]

    def pass_on(step):
        add_beside(step)
        beyond(step).start()

    def enter(step):
        add_first(step, 1)
        add_first(step, 0)

    repeat(lag, enter)

    def middle_step(step):
        enter(step + lag)
        pass_on(step)

    repeat(remote - lag, middle_step)
    for step in range(cuts):
        add_first(step + remote, 1)
        if step < lag:
            pass_on(step + (remote - lag))
    for step in range(cuts):
        add_first(step + remote, 0)
        add_beside(step + remote)

    def gather(step):
        beyond(step).wait_recv()
        sums[pairs - 1, cut(step)] = sums[pairs - 1, cut(step)] + far_in[step // cuts, cut(step)]

    repeat(remote, gather)

    load_small[3].wait()
    load_small[4].wait()
    predicted = sums[pairs - 1]
    turned = predicted.T
    weights = 1.0 / var_ref[...]
    mean_row = jnp.sum(turned, axis=0, keepdims=True) / members
    spread = predicted - jnp.sum(predicted, axis=1, keepdims=True) / members
    spread_t = turned - mean_row
    gram = mm3(spread_t * weights, spread)
    pull = jnp.broadcast_to(weights * (obs_ref[...] - mean_row), (8, rows))
    forcing = mm3(pull, spread)
    row = lax.broadcasted_iota(jnp.int32, (half, half), 0)
    column = lax.broadcasted_iota(jnp.int32, (half, half), 1)
    corner = gram[half:, half:]
    halves = (gram[0:half, half:], jnp.where(row <= column, gram[0:half, 0:half], corner))
    diagonal = jnp.sum(jnp.where(row == column, corner, 0.0), axis=0, keepdims=True)
    extras = (forcing[0:1, 0:half], forcing[0:1, half:], diagonal)
    for which, values in enumerate(halves):
        for index in range(owners):
            gram_ref[which, index, 0:piece] = values[index * piece : (index + 1) * piece]
            extra = extras[index] if which == 0 and index < len(extras) else jnp.zeros((1, half), F32)
            gram_ref[which, index, pl.ds(piece, 1)] = extra

    swap = pltpu.make_async_remote_copy(
        src_ref=gram_ref.at[1 - side], dst_ref=half_in,
        send_sem=send3, recv_sem=recv3, device_id=(orig, twin), device_id_type=MESH,
    )
    swap.start()
    swap.wait_recv()
    half_ref[...] = gram_ref[side] + half_in[...]

    def scatter(step):
        other = xor(rank, ring - 1 - step, ring)
        return pltpu.make_async_remote_copy(
            src_ref=half_ref.at[other], dst_ref=piece_in.at[step],
            send_sem=send4.at[step], recv_sem=recv4.at[step],
            device_id=device_of(other), device_id_type=MESH,
        )

    def spread_out(source, step, other):
        return pltpu.make_async_remote_copy(
            src_ref=piece_ref, dst_ref=final_ref.at[side, source],
            send_sem=send5.at[step], recv_sem=recv5.at[step],
            device_id=device_of(other), device_id_type=MESH,
        )

    def guarded(condition, action):
        if owners == ring:
            action()
        else:
            pl.when(condition)(action)

    def scatter_start(step):
        guarded(xor(rank, ring - 1 - step, ring) < owners, lambda: scatter(step).start())

    repeat(ring - 1, scatter_start)

    def first_end(step):
        first(step, 1).wait_send()
        first(step, 0).wait_send()
        beside(step).wait_send()

    rolled(steps, first_end)
    rolled(remote, lambda step: beyond(step).wait_send())
    swap.wait_send()


    def reduce_piece():
        def arrive(step):
            scatter(step).wait_recv()
            return piece_in[step]

        if ring <= 16:
            total = half_ref[rank]
            for step in range(ring - 1):
                total = total + arrive(step)
            piece_ref[...] = total
        else:
            piece_ref[...] = half_ref[rank]

            def add(step):
                piece_ref[...] = piece_ref[...] + arrive(step)

            repeat(ring - 1, add)
        repeat(ring - 1, lambda step: spread_out(rank, step, xor(rank, ring - 1 - step, ring)).start())
        final_ref[side, rank] = piece_ref[...]

    guarded(rank < owners, reduce_piece)

    def scatter_end(step):
        guarded(xor(rank, ring - 1 - step, ring) < owners, lambda: scatter(step).wait_send())

    rolled(ring - 1, scatter_end)
    def spread_wait(step):
        other = xor(rank, ring - 1 - step, ring)
        guarded(other < owners, lambda: spread_out(other, step, other).wait_recv())

    repeat(ring - 1, spread_wait)
    share = pltpu.make_async_remote_copy(
        src_ref=final_ref.at[side], dst_ref=final_ref.at[side],
        send_sem=send6, recv_sem=recv6, device_id=(orig, twin), device_id_type=MESH,
    )
    share.start()
    guarded(
        rank < owners,
        lambda: rolled(
            ring - 1, lambda step: spread_out(rank, step, xor(rank, ring - 1 - step, ring)).wait_send()
        ),
    )
    share.wait_recv()

    out_ref[...] = final_ref[...]


    share.wait_send()


def update_kernel(counts_hbm, final_ref, states_hbm, out_hbm, counts_ref, states_ref, done_ref, counts_sem, states_sem, done_sem, root_ref, inverse_ref):
    link = lax.axis_index("link")
    own_rows, members = done_ref.shape
    half = members // 2
    fetch = pltpu.make_async_copy(
        states_hbm.at[pl.ds(pl.multiple_of(link * own_rows, own_rows), own_rows)], states_ref, states_sem
    )
    fetch.start()
    fetch_counts = pltpu.make_async_copy(counts_hbm, counts_ref, counts_sem)
    fetch_counts.start()
    owners = final_ref.shape[1]
    piece = half // owners
    upper, mixed = [
        jnp.concatenate([final_ref[which, index, 0:piece] for index in range(owners)], axis=0) for which in range(2)
    ]
    first, second, diagonal = [final_ref[0, index, pl.ds(piece, 1)] for index in range(3)]
    row = lax.broadcasted_iota(jnp.int32, (half, half), 0)
    column = lax.broadcasted_iota(jnp.int32, (half, half), 1)
    turned = mixed.T
    head = jnp.where(row <= column, mixed, turned)
    tail = jnp.where(row == column, diagonal, jnp.where(row > column, mixed, turned))
    gram = jnp.concatenate(
        [jnp.concatenate([head, upper], axis=1), jnp.concatenate([upper.T, tail], axis=1)], axis=0
    )
    forcing = jnp.concatenate([first, second], axis=1)
    high, low = split(transform_of(gram, forcing, root_ref, inverse_ref))
    fetch.wait()
    fetch_counts.wait()
    block_rows = states_hbm.shape[0] // counts_ref.shape[0]
    blocks = own_rows // block_rows
    position = lax.broadcasted_iota(jnp.int32, (block_rows, members), 0)

    def store(index):
        where = slice(index * block_rows, (index + 1) * block_rows)
        return pltpu.make_async_copy(done_ref.at[where], out_hbm.at[where], done_sem.at[index])

    for index in range(blocks):
        states = states_ref[index * block_rows : (index + 1) * block_rows]
        updated = jnp.dot(
            jnp.concatenate([states, states], axis=1), jnp.concatenate([low, high], axis=0), preferred_element_type=F32
        )
        living = position < counts_ref[link * blocks + index]
        done_ref[index * block_rows : (index + 1) * block_rows] = jnp.where(
            living, updated, states.astype(F32)
        ).astype(BF16)
        store(index).start()
    for index in range(blocks):
        store(index).wait()


def per_device(background, live_counts, patterns, pattern_ids, link_targets, counts_obs, obs_var):
    n_orig = lax.axis_size("orig")
    n_link = lax.axis_size("link")
    states_dev, members = background.shape
    blocks_dev = live_counts.shape[0]
    block_rows = states_dev // blocks_dev
    link_rows = patterns.shape[2]
    rows = counts_obs.shape[1]
    link_blocks = rows * n_orig // link_rows
    vmem = pl.BlockSpec(memory_space=pltpu.VMEM)
    hbm = pl.BlockSpec(memory_space=pl.ANY)
    dma = pltpu.SemaphoreType.DMA
    grant = pltpu.CompilerParams(vmem_limit_bytes=WIDE_GRANT)
    pairs = n_orig // 2
    ring = n_orig * n_link // 2
    half = members // 2
    owners = min(ring, half // 8)
    packed = (owners, half // owners + 1, half)
    cuts = CUTS if rows == link_rows else 1
    slots = pattern_ids.shape[2]
    table_rows = pl.cdiv(slots + link_blocks, 8) * 8
    steps = pairs // 2 * cuts
    gram = pl.pallas_call(
        functools.partial(gram_kernel, n_orig, n_link, cuts),
        out_shape=pltpu.VMEM((2,) + packed, F32),
        in_specs=[hbm] * 7,
        out_specs=vmem,
        scratch_shapes=[
            pltpu.VMEM((slots, 1, blocks_dev), jnp.int32),
            pltpu.VMEM((slots, 1, blocks_dev), jnp.int32),
            pltpu.SMEM((blocks_dev,), jnp.int32),
            pltpu.VMEM((1, rows), F32),
            pltpu.VMEM((1, rows), F32),
            dma((5,)),
            pltpu.VMEM((cuts, patterns.shape[1], link_rows // cuts, block_rows), BF16),
            pltpu.VMEM((states_dev, members), BF16),
            dma((cuts,)),
            dma,
            pltpu.VMEM((16, link_rows // cuts, block_rows), F32),
            pltpu.VMEM((16, link_rows // cuts, block_rows), F32),
            pltpu.VMEM((2 * SPAN, link_blocks * link_rows // cuts, block_rows), BF16),
            pltpu.VMEM((table_rows, 128), jnp.int32),
            pltpu.SMEM((table_rows, 128), jnp.int32),
            dma,
            pltpu.VMEM((link_blocks * link_rows, members), F32),
            pltpu.VMEM((pairs, rows, members), F32),
            pltpu.VMEM((pairs, rows, members), F32),
            pltpu.VMEM((pairs // 2, rows, members), F32),
            pltpu.VMEM((pairs // 2, rows, members), F32),
            pltpu.VMEM((2,) + packed, F32),
            pltpu.VMEM(packed, F32),
            pltpu.VMEM(packed, F32),
            pltpu.VMEM((ring - 1,) + packed[1:], F32),
            pltpu.VMEM(packed[1:], F32),
            pltpu.VMEM((2,) + packed, F32),
            dma((2 * steps,)), dma((2 * steps,)),
            dma((steps,)), dma((steps,)),
            dma((steps,)), dma((steps,)),
            dma, dma,
            dma((ring,)), dma((ring,)),
            dma((ring,)), dma((ring,)),
            dma, dma,
        ],
        compiler_params=pltpu.CompilerParams(
            collective_id=0, has_side_effects=True, vmem_limit_bytes=WIDE_GRANT
        ),
    )(
        jnp.transpose(pattern_ids, (2, 0, 1)), jnp.transpose(link_targets, (2, 0, 1)), live_counts,
        patterns[0], background, counts_obs, obs_var,
    )
    own_rows = states_dev // n_link
    return pl.pallas_call(
        update_kernel,
        out_shape=jax.ShapeDtypeStruct((own_rows, members), BF16),
        in_specs=[hbm, vmem, hbm],
        out_specs=hbm,
        scratch_shapes=[
            pltpu.SMEM((blocks_dev,), jnp.int32),
            pltpu.VMEM((own_rows, members), BF16),
            pltpu.VMEM((own_rows, members), BF16),
            dma,
            dma,
            dma((own_rows // block_rows,)),
            pltpu.VMEM((members, members), F32),
            pltpu.VMEM((members, members), F32),
        ],
        compiler_params=grant,
    )(live_counts, pltpu.with_memory_space_constraint(gram, pltpu.VMEM), background)


def solution(mesh):
    placed = (
        P("orig", None),
        P("orig"),
        P("link", "orig", None, None),
        P("link", "orig", None),
        P("link", "orig", None),
        P("link", "orig"),
        P("link", "orig"),
    )
    return jax.shard_map(
        per_device, mesh=mesh, in_specs=placed, out_specs=P(("orig", "link"), None), check_vma=False
    )
```

```python
import functools

import jax
import jax.numpy as jnp
from jax import lax
from jax.experimental import pallas as pl
from jax.experimental.pallas import tpu as pltpu
from jax.sharding import PartitionSpec as P

NS_ITERS = 4
CUTS = 4
SPAN = 8
WIDE_GRANT = 67043328-900*1024
MESH = pl.DeviceIdType.MESH
F32 = jnp.float32
BF16 = jnp.bfloat16


def repeat(count, body):
    if count <= 16:
        for step in range(count):
            body(step)
    else:
        lax.fori_loop(0, count, lambda step, carry: (body(step), carry)[1], 0)


def rolled(count, body):
    lax.fori_loop(0, count, lambda step, carry: (body(step), carry)[1], 0)


def xor(a, b, size):
    total = 0
    bit = 1
    while bit < size:
        total = total + ((a // bit) % 2 + (b // bit) % 2) % 2 * bit
        bit *= 2
    return total


def split(x):
    high = x.astype(BF16)
    return high, (x - high.astype(F32)).astype(BF16)


def mm3(a, b):
    a_high, a_low = split(a)
    b_high, b_low = split(b)
    left = jnp.concatenate([a_high, a_low, a_high], axis=1)
    right = jnp.concatenate([b_low, b_high, b_high], axis=0)
    height = left.shape[0] // 2
    if height % 16:
        return jnp.dot(left, right, preferred_element_type=F32)
    return jnp.concatenate(
        [jnp.dot(left[0:height], right, preferred_element_type=F32), jnp.dot(left[height:], right, preferred_element_type=F32)],
        axis=0,
    )


def sort_slots(ids_ref, targets_ref, table_ref, tiles, link_blocks):
    slots = ids_ref.shape[0]
    bits = max(1, (tiles - 1).bit_length())
    per_word = 31 // bits
    targets = [targets_ref[slot] for slot in range(slots)]
    ones = [jnp.left_shift(jnp.ones_like(target), target * 4) for target in targets]
    tally = functools.reduce(lambda a, b: a + b, ones)
    starts = jnp.zeros_like(tally)
    for shift in range(1, 8):
        starts = starts + jnp.left_shift(tally, jnp.full_like(tally, 4 * shift))
    place = starts
    words = [jnp.zeros_like(tally) for _ in range(pl.cdiv(slots, per_word))]
    for slot in range(slots):
        rank = jnp.bitwise_and(jnp.right_shift(place, targets[slot] * 4), 15)
        place = place + ones[slot]
        tile = ids_ref[slot]
        for word in range(len(words)):
            local = rank - word * per_word
            inside = (local >= 0) & (local < per_word)
            shifted = jnp.left_shift(tile, jnp.where(inside, local * bits, 0))
            words[word] = words[word] + jnp.where(inside, shifted, 0)
    rows = []
    for slot in range(slots):
        amount = jnp.full_like(tally, slot % per_word * bits)
        rows.append(jnp.bitwise_and(jnp.right_shift(words[slot // per_word], amount), 2**bits - 1))
    for target in range(1, link_blocks):
        rows.append(jnp.bitwise_and(jnp.right_shift(starts, jnp.full_like(tally, 4 * target)), 15))
    for index, row in enumerate(rows):
        table_ref[index : index + 1, 0 : row.shape[1]] = row


def build_group(table_ref, tiles_ref, prefix_refs, lhs_ref, group, cut_index, slots, link_blocks):
    tiles, cut_rows, block_rows = tiles_ref.shape[1:]
    span = lhs_ref.shape[0] // 2
    for index in range(span):
        prefix_ref = prefix_refs[index % len(prefix_refs)]
        block = group * span + index
        total = jnp.zeros((cut_rows, block_rows), F32)
        for slot in range(slots):
            tile = table_ref[slot, block]
            total = total + tiles_ref[cut_index, tile].astype(F32)
            prefix_ref[slot + 1] = total
        before = None
        for target in range(link_blocks):
            upto = total
            if target < link_blocks - 1:
                end = table_ref[slots + target, block]
                upto = prefix_ref[end]
            high, low = split(upto if before is None else upto - before)
            before = upto
            rows = slice(target * cut_rows, (target + 1) * cut_rows)
            lhs_ref[index, rows] = high
            lhs_ref[span + index, rows] = low


def predict(table_ref, tiles_ref, states_ref, prefix_refs, lhs_ref, term_ref, slots, after_cut):
    cuts, _, cut_rows, block_rows = tiles_ref.shape
    link_rows = cut_rows * cuts
    link_blocks = term_ref.shape[0] // link_rows
    span = lhs_ref.shape[0] // 2
    depth = span * block_rows
    groups = states_ref.shape[0] // depth

    def build(place):
        cut_at = jnp.minimum(place // groups, cuts - 1)
        build_group(table_ref, tiles_ref, prefix_refs, lhs_ref, place % groups, cut_at, slots, link_blocks)

    build(0)

    def add_group(place, carry):
        group = place % groups
        cut_index = place // groups
        states = states_ref[pl.ds(pl.multiple_of(group * depth, depth), depth)]
        left = jnp.concatenate([lhs_ref[index] for index in range(2 * span)], axis=1)
        product = jnp.dot(left, jnp.concatenate([states, states], axis=0), preferred_element_type=F32)
        build(place + 1)
        for target in range(link_blocks):
            where = pl.ds(pl.multiple_of(target * link_rows + cut_index * cut_rows, cut_rows), cut_rows)
            term_ref[where] = term_ref[where] + product[target * cut_rows : (target + 1) * cut_rows]

        @pl.when(group == groups - 1)
        def _():
            after_cut(cut_index)

        return carry

    lax.fori_loop(0, groups * cuts, add_group, 0)


def column_of(row):
    width = row.shape[1]
    return jnp.broadcast_to(row, (width, width)).T


def transform_of(gram, forcing, root_ref, inverse_ref):
    members = gram.shape[0]
    row = lax.broadcasted_iota(jnp.int32, (members, members), 0)
    column = lax.broadcasted_iota(jnp.int32, (members, members), 1)
    identity = (row == column).astype(F32)
    system = identity + gram * (1.0 / (members - 1.0))
    bound = jnp.max(jnp.sum(jnp.abs(system), axis=0, keepdims=True), axis=1, keepdims=True)
    shrink = 1.0 / bound
    root = system * shrink
    middle = 1.5 * identity - 0.5 * root
    inverse_ref[...] = middle
    root_ref[...] = mm3(root, middle)

    def sweep(index, carry):
        root = root_ref[...]
        inverse = inverse_ref[...]
        middle = 1.5 * identity - 0.5 * mm3(inverse, root)
        root_ref[...] = mm3(root, middle)
        inverse_ref[...] = mm3(middle, inverse)
        return carry

    lax.fori_loop(1, NS_ITERS - 1, sweep, 0)
    inverse = inverse_ref[...]
    inverse = mm3(1.5 * identity - 0.5 * mm3(inverse, root_ref[...]), inverse)
    scale = 1.0 / jnp.sqrt(bound)
    share = shrink / (members - 1.0)
    inner = jnp.sum(inverse * column_of(forcing), axis=0, keepdims=True)
    mean_weights = jnp.sum(inverse * inner, axis=1, keepdims=True) * share
    across = jnp.sum(inverse, axis=0, keepdims=True)
    total = across * scale + jnp.sum(across * inner, axis=1, keepdims=True) * share
    return inverse * scale + (1.0 - total) / members + mean_weights


def gram_kernel(
    n_orig, n_link, cuts, ids_hbm, targets_hbm, counts_hbm, tiles_hbm, states_hbm, obs_hbm, var_hbm, out_ref,
    ids_ref, targets_ref, counts_ref, obs_ref, var_ref, small_sem, tiles_ref, states_ref, tiles_sem, states_sem, even_ref, odd_ref, lhs_ref, packed_ref, table_ref, table_sem, term_ref, first_in, sums, side_in, far_in, gram_ref, half_in, half_ref, piece_in, piece_ref, final_ref,
    send1, recv1, send2, recv2, send7, recv7, send3, recv3, send4, recv4, send5, recv5, send6, recv6,
):
    orig = lax.axis_index("orig")
    link = lax.axis_index("link")
    rows = obs_ref.shape[1]
    members = term_ref.shape[1]
    half = members // 2
    pairs = n_orig // 2
    parity = orig % 2
    place = orig // 2
    across = orig + 1 - 2 * parity
    side = link % 2
    twin = link + 1 - 2 * side
    ring = n_orig * n_link // 2
    rank = (link // 2) * n_orig + orig
    owners = min(ring, half // 8)
    piece = half // owners

    def device_of(other):
        return (other % n_orig, (other // n_orig) * 2 + side)

    load_small = [
        pltpu.make_async_copy(source, target, small_sem.at[index])
        for index, (source, target) in enumerate(
            [
                (ids_hbm, ids_ref), (targets_hbm, targets_ref), (counts_hbm, counts_ref),
                (obs_hbm, obs_ref), (var_hbm, var_ref),
            ]
        )
    ]
    for copy in load_small[:3]:
        copy.start()
    load_states = pltpu.make_async_copy(states_hbm, states_ref, states_sem)
    load_states.start()

    def load_tiles(index):
        part = tiles_ref.shape[2]
        return pltpu.make_async_copy(
            tiles_hbm.at[:, pl.ds(index * part, part)], tiles_ref.at[index], tiles_sem.at[index]
        )

    for index in range(cuts):
        load_tiles(index).start()
    for copy in load_small[3:]:
        copy.start()
    near = place % 2
    far = place // 2
    n_far = pairs // 2
    barrier = pltpu.get_barrier_semaphore()

    def greet(other_orig, other_link):
        pl.semaphore_signal(barrier, inc=1, device_id=(other_orig, other_link), device_id_type=MESH)

    greet(across, link)
    greet(2 * (far * 2 + 1 - near) + parity, link)
    repeat(n_far - 1, lambda step: greet(2 * (xor(far, step + 1, n_far) * 2 + near) + parity, link))
    repeat(n_link - 1, lambda step: greet(orig, (link + step + 1) % n_link))

    slots = ids_ref.shape[0]
    blocks = counts_ref.shape[0]
    block_rows = states_ref.shape[0] // blocks
    link_rows = tiles_ref.shape[2] * cuts
    for prefix_ref in (even_ref, odd_ref):
        prefix_ref[...] = jnp.zeros(prefix_ref.shape, F32)
    term_ref[...] = jnp.zeros_like(term_ref)
    load_small[0].wait()
    load_small[1].wait()
    sort_slots(ids_ref, targets_ref, packed_ref, tiles_ref.shape[1], rows * n_orig // link_rows)
    move_table = pltpu.make_async_copy(packed_ref, table_ref, table_sem)
    move_table.start()
    position = lax.broadcasted_iota(jnp.int32, (block_rows, members), 0)
    load_small[2].wait()
    load_states.wait()

    def mask_block(block, carry):
        where = pl.ds(pl.multiple_of(block * block_rows, block_rows), block_rows)
        states = states_ref[where]
        states_ref[where] = jnp.where(position < counts_ref[block], states, jnp.zeros_like(states))
        return carry

    lax.fori_loop(0, blocks, mask_block, 0, unroll=2)
    for index in range(cuts):
        load_tiles(index).wait()
    move_table.wait()

    cut_rows = rows // cuts
    steps = n_far * cuts

    def owner(step, flip):
        other = xor(far, n_far - 1 - step // cuts, n_far)
        return other * 2 + (near + flip) % 2

    def term_rows(index, step):
        return pl.ds(pl.multiple_of(index * rows + step % cuts * cut_rows, cut_rows), cut_rows)

    def cut(step):
        return pl.ds(pl.multiple_of(step % cuts * cut_rows, cut_rows), cut_rows)

    def slot(step, flip):
        return step // cuts * 2 + 1 - flip

    def first(step, flip):
        index = slot(step, flip) * cuts + step % cuts
        return pltpu.make_async_remote_copy(
            src_ref=term_ref.at[term_rows(2 * owner(step, flip) + 1 - parity, step)],
            dst_ref=first_in.at[slot(step, flip), cut(step)],
            send_sem=send1.at[index], recv_sem=recv1.at[index],
            device_id=(across, link), device_id_type=MESH,
        )

    def beside(step):
        return pltpu.make_async_remote_copy(
            src_ref=sums.at[slot(step, 1), cut(step)], dst_ref=side_in.at[step // cuts, cut(step)],
            send_sem=send2.at[step], recv_sem=recv2.at[step],
            device_id=(2 * (far * 2 + 1 - near) + parity, link), device_id_type=MESH,
        )

    def beyond(step):
        return pltpu.make_async_remote_copy(
            src_ref=sums.at[slot(step, 0), cut(step)], dst_ref=far_in.at[step // cuts, cut(step)],
            send_sem=send7.at[step], recv_sem=recv7.at[step],
            device_id=(2 * owner(step, 0) + parity, link), device_id_type=MESH,
        )

    remote = steps - cuts
    lag = min(2, remote, cuts)

    def after_cut(index):
        @pl.when(index == 0)
        def _():
            pl.semaphore_wait(barrier, n_far + n_link)

        def first_start(step):
            first(step * cuts + index, 1).start()
            first(step * cuts + index, 0).start()

        repeat(n_far - 1, first_start)

    predict(table_ref, tiles_ref, states_ref, (even_ref, odd_ref), lhs_ref, term_ref, slots, after_cut)
    repeat(cuts, lambda step: first(step + remote, 1).start())
    repeat(cuts, lambda step: first(step + remote, 0).start())

    def add_first(step, flip):
        first(step, flip).wait_recv()
        sums[slot(step, flip), cut(step)] = (
            term_ref[term_rows(2 * owner(step, flip) + parity, step)] + first_in[slot(step, flip), cut(step)]
        )
        if flip:
            beside(step).start()

    def add_beside(step):
        beside(step).wait_recv()
        sums[slot(step, 0), cut(step)] = sums[slot(step, 0), cut(step)] + side_in[step // cuts, cut(step)]

    def pass_on(step):
        add_beside(step)
        beyond(step).start()

    def enter(step):
        add_first(step, 1)
        add_first(step, 0)

    repeat(lag, enter)

    def middle_step(step):
        enter(step + lag)
        pass_on(step)

    repeat(remote - lag, middle_step)
    for step in range(cuts):
        add_first(step + remote, 1)
        if step < lag:
            pass_on(step + (remote - lag))
    for step in range(cuts):
        add_first(step + remote, 0)
        add_beside(step + remote)

    def gather(step):
        beyond(step).wait_recv()
        sums[pairs - 1, cut(step)] = sums[pairs - 1, cut(step)] + far_in[step // cuts, cut(step)]

    repeat(remote, gather)

    load_small[3].wait()
    load_small[4].wait()
    predicted = sums[pairs - 1]
    turned = predicted.T
    weights = 1.0 / var_ref[...]
    mean_row = jnp.sum(turned, axis=0, keepdims=True) / members
    spread = predicted - jnp.sum(predicted, axis=1, keepdims=True) / members
    spread_t = turned - mean_row
    gram = mm3(spread_t * weights, spread)
    pull = jnp.broadcast_to(weights * (obs_ref[...] - mean_row), (8, rows))
    forcing = mm3(pull, spread)
    row = lax.broadcasted_iota(jnp.int32, (half, half), 0)
    column = lax.broadcasted_iota(jnp.int32, (half, half), 1)
    corner = gram[half:, half:]
    halves = (gram[0:half, half:], jnp.where(row <= column, gram[0:half, 0:half], corner))
    diagonal = jnp.sum(jnp.where(row == column, corner, 0.0), axis=0, keepdims=True)
    extras = (forcing[0:1, 0:half], forcing[0:1, half:], diagonal)
    for which, values in enumerate(halves):
        for index in range(owners):
            gram_ref[which, index, 0:piece] = values[index * piece : (index + 1) * piece]
            extra = extras[index] if which == 0 and index < len(extras) else jnp.zeros((1, half), F32)
            gram_ref[which, index, pl.ds(piece, 1)] = extra

    swap = pltpu.make_async_remote_copy(
        src_ref=gram_ref.at[1 - side], dst_ref=half_in,
        send_sem=send3, recv_sem=recv3, device_id=(orig, twin), device_id_type=MESH,
    )
    swap.start()
    swap.wait_recv()
    half_ref[...] = gram_ref[side] + half_in[...]

    def scatter(step):
        other = xor(rank, ring - 1 - step, ring)
        return pltpu.make_async_remote_copy(
            src_ref=half_ref.at[other], dst_ref=piece_in.at[step],
            send_sem=send4.at[step], recv_sem=recv4.at[step],
            device_id=device_of(other), device_id_type=MESH,
        )

    def spread_out(source, step, other):
        return pltpu.make_async_remote_copy(
            src_ref=piece_ref, dst_ref=final_ref.at[side, source],
            send_sem=send5.at[step], recv_sem=recv5.at[step],
            device_id=device_of(other), device_id_type=MESH,
        )

    def guarded(condition, action):
        if owners == ring:
            action()
        else:
            pl.when(condition)(action)

    def scatter_start(step):
        guarded(xor(rank, ring - 1 - step, ring) < owners, lambda: scatter(step).start())

    repeat(ring - 1, scatter_start)

    def first_end(step):
        first(step, 1).wait_send()
        first(step, 0).wait_send()
        beside(step).wait_send()

    rolled(steps, first_end)
    rolled(remote, lambda step: beyond(step).wait_send())
    swap.wait_send()


    def reduce_piece():
        def arrive(step):
            scatter(step).wait_recv()
            return piece_in[step]

        if ring <= 16:
            total = half_ref[rank]
            for step in range(ring - 1):
                total = total + arrive(step)
            piece_ref[...] = total
        else:
            piece_ref[...] = half_ref[rank]

            def add(step):
                piece_ref[...] = piece_ref[...] + arrive(step)

            repeat(ring - 1, add)
        repeat(ring - 1, lambda step: spread_out(rank, step, xor(rank, ring - 1 - step, ring)).start())
        final_ref[side, rank] = piece_ref[...]

    guarded(rank < owners, reduce_piece)

    def scatter_end(step):
        guarded(xor(rank, ring - 1 - step, ring) < owners, lambda: scatter(step).wait_send())

    rolled(ring - 1, scatter_end)
    def spread_wait(step):
        other = xor(rank, ring - 1 - step, ring)
        guarded(other < owners, lambda: spread_out(other, step, other).wait_recv())

    repeat(ring - 1, spread_wait)
    share = pltpu.make_async_remote_copy(
        src_ref=final_ref.at[side], dst_ref=final_ref.at[side],
        send_sem=send6, recv_sem=recv6, device_id=(orig, twin), device_id_type=MESH,
    )
    share.start()
    guarded(
        rank < owners,
        lambda: rolled(
            ring - 1, lambda step: spread_out(rank, step, xor(rank, ring - 1 - step, ring)).wait_send()
        ),
    )
    share.wait_recv()

    out_ref[...] = final_ref[...]


    share.wait_send()


def update_kernel(counts_hbm, final_ref, states_hbm, out_hbm, counts_ref, states_ref, done_ref, counts_sem, states_sem, done_sem, root_ref, inverse_ref):
    link = lax.axis_index("link")
    own_rows, members = done_ref.shape
    half = members // 2
    fetch = pltpu.make_async_copy(
        states_hbm.at[pl.ds(pl.multiple_of(link * own_rows, own_rows), own_rows)], states_ref, states_sem
    )
    fetch.start()
    fetch_counts = pltpu.make_async_copy(counts_hbm, counts_ref, counts_sem)
    fetch_counts.start()
    owners = final_ref.shape[1]
    piece = half // owners
    upper, mixed = [
        jnp.concatenate([final_ref[which, index, 0:piece] for index in range(owners)], axis=0) for which in range(2)
    ]
    first, second, diagonal = [final_ref[0, index, pl.ds(piece, 1)] for index in range(3)]
    row = lax.broadcasted_iota(jnp.int32, (half, half), 0)
    column = lax.broadcasted_iota(jnp.int32, (half, half), 1)
    turned = mixed.T
    head = jnp.where(row <= column, mixed, turned)
    tail = jnp.where(row == column, diagonal, jnp.where(row > column, mixed, turned))
    gram = jnp.concatenate(
        [jnp.concatenate([head, upper], axis=1), jnp.concatenate([upper.T, tail], axis=1)], axis=0
    )
    forcing = jnp.concatenate([first, second], axis=1)
    high, low = split(transform_of(gram, forcing, root_ref, inverse_ref))
    fetch.wait()
    fetch_counts.wait()
    block_rows = states_hbm.shape[0] // counts_ref.shape[0]
    blocks = own_rows // block_rows
    position = lax.broadcasted_iota(jnp.int32, (block_rows, members), 0)

    def store(index):
        where = slice(index * block_rows, (index + 1) * block_rows)
        return pltpu.make_async_copy(done_ref.at[where], out_hbm.at[where], done_sem.at[index])

    for index in range(blocks):
        states = states_ref[index * block_rows : (index + 1) * block_rows]
        updated = jnp.dot(
            jnp.concatenate([states, states], axis=1), jnp.concatenate([low, high], axis=0), preferred_element_type=F32
        )
        living = position < counts_ref[link * blocks + index]
        done_ref[index * block_rows : (index + 1) * block_rows] = jnp.where(
            living, updated, states.astype(F32)
        ).astype(BF16)
        store(index).start()
    for index in range(blocks):
        store(index).wait()


def per_device(background, live_counts, patterns, pattern_ids, link_targets, counts_obs, obs_var):
    n_orig = lax.axis_size("orig")
    n_link = lax.axis_size("link")
    states_dev, members = background.shape
    blocks_dev = live_counts.shape[0]
    block_rows = states_dev // blocks_dev
    link_rows = patterns.shape[2]
    rows = counts_obs.shape[1]
    link_blocks = rows * n_orig // link_rows
    vmem = pl.BlockSpec(memory_space=pltpu.VMEM)
    hbm = pl.BlockSpec(memory_space=pl.ANY)
    dma = pltpu.SemaphoreType.DMA
    grant = pltpu.CompilerParams(vmem_limit_bytes=WIDE_GRANT)
    pairs = n_orig // 2
    ring = n_orig * n_link // 2
    half = members // 2
    owners = min(ring, half // 8)
    packed = (owners, half // owners + 1, half)
    cuts = CUTS if rows == link_rows else 1
    slots = pattern_ids.shape[2]
    table_rows = pl.cdiv(slots + link_blocks, 8) * 8
    steps = pairs // 2 * cuts
    gram = pl.pallas_call(
        functools.partial(gram_kernel, n_orig, n_link, cuts),
        out_shape=pltpu.VMEM((2,) + packed, F32),
        in_specs=[hbm] * 7,
        out_specs=vmem,
        scratch_shapes=[
            pltpu.VMEM((slots, 1, blocks_dev), jnp.int32),
            pltpu.VMEM((slots, 1, blocks_dev), jnp.int32),
            pltpu.SMEM((blocks_dev,), jnp.int32),
            pltpu.VMEM((1, rows), F32),
            pltpu.VMEM((1, rows), F32),
            dma((5,)),
            pltpu.VMEM((cuts, patterns.shape[1], link_rows // cuts, block_rows), BF16),
            pltpu.VMEM((states_dev, members), BF16),
            dma((cuts,)),
            dma,
            pltpu.VMEM((16, link_rows // cuts, block_rows), F32),
            pltpu.VMEM((16, link_rows // cuts, block_rows), F32),
            pltpu.VMEM((2 * SPAN, link_blocks * link_rows // cuts, block_rows), BF16),
            pltpu.VMEM((table_rows, 128), jnp.int32),
            pltpu.SMEM((table_rows, 128), jnp.int32),
            dma,
            pltpu.VMEM((link_blocks * link_rows, members), F32),
            pltpu.VMEM((pairs, rows, members), F32),
            pltpu.VMEM((pairs, rows, members), F32),
            pltpu.VMEM((pairs // 2, rows, members), F32),
            pltpu.VMEM((pairs // 2, rows, members), F32),
            pltpu.VMEM((2,) + packed, F32),
            pltpu.VMEM(packed, F32),
            pltpu.VMEM(packed, F32),
            pltpu.VMEM((ring - 1,) + packed[1:], F32),
            pltpu.VMEM(packed[1:], F32),
            pltpu.VMEM((2,) + packed, F32),
            dma((2 * steps,)), dma((2 * steps,)),
            dma((steps,)), dma((steps,)),
            dma((steps,)), dma((steps,)),
            dma, dma,
            dma((ring,)), dma((ring,)),
            dma((ring,)), dma((ring,)),
            dma, dma,
        ],
        compiler_params=pltpu.CompilerParams(
            collective_id=0, has_side_effects=True, vmem_limit_bytes=WIDE_GRANT
        ),
    )(
        jnp.transpose(pattern_ids, (2, 0, 1)), jnp.transpose(link_targets, (2, 0, 1)), live_counts,
        patterns[0], background, counts_obs, obs_var,
    )
    own_rows = states_dev // n_link
    return pl.pallas_call(
        update_kernel,
        out_shape=jax.ShapeDtypeStruct((own_rows, members), BF16),
        in_specs=[hbm, vmem, hbm],
        out_specs=hbm,
        scratch_shapes=[
            pltpu.SMEM((blocks_dev,), jnp.int32),
            pltpu.VMEM((own_rows, members), BF16),
            pltpu.VMEM((own_rows, members), BF16),
            dma,
            dma,
            dma((own_rows // block_rows,)),
            pltpu.VMEM((members, members), F32),
            pltpu.VMEM((members, members), F32),
        ],
        compiler_params=grant,
    )(live_counts, pltpu.with_memory_space_constraint(gram, pltpu.VMEM), background)


def solution(mesh):
    placed = (
        P("orig", None),
        P("orig"),
        P("link", "orig", None, None),
        P("link", "orig", None),
        P("link", "orig", None),
        P("link", "orig"),
        P("link", "orig"),
    )
    return jax.shard_map(
        per_device, mesh=mesh, in_specs=placed, out_specs=P(("orig", "link"), None), check_vma=False
    )
```

```python
import functools

import jax
import jax.numpy as jnp
from jax import lax
from jax.experimental import pallas as pl
from jax.experimental.pallas import tpu as pltpu
from jax.sharding import PartitionSpec as P

NS_ITERS = 4
CUTS = 4
SPAN = 8
WIDE_GRANT = 67043328-900*1024
MESH = pl.DeviceIdType.MESH
F32 = jnp.float32
BF16 = jnp.bfloat16


def repeat(count, body):
    if count <= 16:
        for step in range(count):
            body(step)
    else:
        lax.fori_loop(0, count, lambda step, carry: (body(step), carry)[1], 0)


def rolled(count, body):
    lax.fori_loop(0, count, lambda step, carry: (body(step), carry)[1], 0)


def xor(a, b, size):
    total = 0
    bit = 1
    while bit < size:
        total = total + ((a // bit) % 2 + (b // bit) % 2) % 2 * bit
        bit *= 2
    return total


def split(x):
    high = x.astype(BF16)
    return high, (x - high.astype(F32)).astype(BF16)


def mm3(a, b):
    a_high, a_low = split(a)
    b_high, b_low = split(b)
    left = jnp.concatenate([a_high, a_low, a_high], axis=1)
    right = jnp.concatenate([b_low, b_high, b_high], axis=0)
    height = left.shape[0] // 2
    if height % 16:
        return jnp.dot(left, right, preferred_element_type=F32)
    return jnp.concatenate(
        [jnp.dot(left[0:height], right, preferred_element_type=F32), jnp.dot(left[height:], right, preferred_element_type=F32)],
        axis=0,
    )


def sort_slots(ids_ref, targets_ref, table_ref, tiles, link_blocks):
    slots = ids_ref.shape[0]
    bits = max(1, (tiles - 1).bit_length())
    per_word = 31 // bits
    targets = [targets_ref[slot] for slot in range(slots)]
    ones = [jnp.left_shift(jnp.ones_like(target), target * 4) for target in targets]
    tally = functools.reduce(lambda a, b: a + b, ones)
    starts = jnp.zeros_like(tally)
    for shift in range(1, 8):
        starts = starts + jnp.left_shift(tally, jnp.full_like(tally, 4 * shift))
    place = starts
    words = [jnp.zeros_like(tally) for _ in range(pl.cdiv(slots, per_word))]
    for slot in range(slots):
        rank = jnp.bitwise_and(jnp.right_shift(place, targets[slot] * 4), 15)
        place = place + ones[slot]
        tile = ids_ref[slot]
        for word in range(len(words)):
            local = rank - word * per_word
            inside = (local >= 0) & (local < per_word)
            shifted = jnp.left_shift(tile, jnp.where(inside, local * bits, 0))
            words[word] = words[word] + jnp.where(inside, shifted, 0)
    rows = []
    for slot in range(slots):
        amount = jnp.full_like(tally, slot % per_word * bits)
        rows.append(jnp.bitwise_and(jnp.right_shift(words[slot // per_word], amount), 2**bits - 1))
    for target in range(1, link_blocks):
        rows.append(jnp.bitwise_and(jnp.right_shift(starts, jnp.full_like(tally, 4 * target)), 15))
    for index, row in enumerate(rows):
        table_ref[index : index + 1, 0 : row.shape[1]] = row


def build_group(table_ref, tiles_ref, prefix_refs, lhs_ref, group, cut_index, slots, link_blocks):
    tiles, cut_rows, block_rows = tiles_ref.shape[1:]
    span = lhs_ref.shape[0] // 2
    for index in range(span):
        prefix_ref = prefix_refs[index % len(prefix_refs)]
        block = group * span + index
        total = jnp.zeros((cut_rows, block_rows), F32)
        for slot in range(slots):
            tile = table_ref[slot, block]
            total = total + tiles_ref[cut_index, tile].astype(F32)
            prefix_ref[slot + 1] = total
        before = None
        for target in range(link_blocks):
            upto = total
            if target < link_blocks - 1:
                end = table_ref[slots + target, block]
                upto = prefix_ref[end]
            high, low = split(upto if before is None else upto - before)
            before = upto
            rows = slice(target * cut_rows, (target + 1) * cut_rows)
            lhs_ref[index, rows] = high
            lhs_ref[span + index, rows] = low


def predict(table_ref, tiles_ref, states_ref, prefix_refs, lhs_ref, term_ref, slots, after_cut):
    cuts, _, cut_rows, block_rows = tiles_ref.shape
    link_rows = cut_rows * cuts
    link_blocks = term_ref.shape[0] // link_rows
    span = lhs_ref.shape[0] // 2
    depth = span * block_rows
    groups = states_ref.shape[0] // depth

    def build(place):
        cut_at = jnp.minimum(place // groups, cuts - 1)
        build_group(table_ref, tiles_ref, prefix_refs, lhs_ref, place % groups, cut_at, slots, link_blocks)

    build(0)

    def add_group(place, carry):
        group = place % groups
        cut_index = place // groups
        states = states_ref[pl.ds(pl.multiple_of(group * depth, depth), depth)]
        left = jnp.concatenate([lhs_ref[index] for index in range(2 * span)], axis=1)
        product = jnp.dot(left, jnp.concatenate([states, states], axis=0), preferred_element_type=F32)
        build(place + 1)
        for target in range(link_blocks):
            where = pl.ds(pl.multiple_of(target * link_rows + cut_index * cut_rows, cut_rows), cut_rows)
            term_ref[where] = term_ref[where] + product[target * cut_rows : (target + 1) * cut_rows]

        @pl.when(group == groups - 1)
        def _():
            after_cut(cut_index)

        return carry

    lax.fori_loop(0, groups * cuts, add_group, 0)


def column_of(row):
    width = row.shape[1]
    return jnp.broadcast_to(row, (width, width)).T


def transform_of(gram, forcing, root_ref, inverse_ref):
    members = gram.shape[0]
    row = lax.broadcasted_iota(jnp.int32, (members, members), 0)
    column = lax.broadcasted_iota(jnp.int32, (members, members), 1)
    identity = (row == column).astype(F32)
    system = identity + gram * (1.0 / (members - 1.0))
    bound = jnp.max(jnp.sum(jnp.abs(system), axis=0, keepdims=True), axis=1, keepdims=True)
    shrink = 1.0 / bound
    root = system * shrink
    middle = 1.5 * identity - 0.5 * root
    inverse_ref[...] = middle
    root_ref[...] = mm3(root, middle)

    def sweep(index, carry):
        root = root_ref[...]
        inverse = inverse_ref[...]
        middle = 1.5 * identity - 0.5 * mm3(inverse, root)
        root_ref[...] = mm3(root, middle)
        inverse_ref[...] = mm3(middle, inverse)
        return carry

    lax.fori_loop(1, NS_ITERS - 1, sweep, 0)
    inverse = inverse_ref[...]
    inverse = mm3(1.5 * identity - 0.5 * mm3(inverse, root_ref[...]), inverse)
    scale = 1.0 / jnp.sqrt(bound)
    share = shrink / (members - 1.0)
    inner = jnp.sum(inverse * column_of(forcing), axis=0, keepdims=True)
    mean_weights = jnp.sum(inverse * inner, axis=1, keepdims=True) * share
    across = jnp.sum(inverse, axis=0, keepdims=True)
    total = across * scale + jnp.sum(across * inner, axis=1, keepdims=True) * share
    return inverse * scale + (1.0 - total) / members + mean_weights


def gram_kernel(
    n_orig, n_link, cuts, ids_hbm, targets_hbm, counts_hbm, tiles_hbm, states_hbm, obs_hbm, var_hbm, out_ref,
    ids_ref, targets_ref, counts_ref, obs_ref, var_ref, small_sem, tiles_ref, states_ref, tiles_sem, states_sem, even_ref, odd_ref, lhs_ref, packed_ref, table_ref, table_sem, term_ref, first_in, sums, side_in, far_in, gram_ref, half_in, half_ref, piece_in, piece_ref, final_ref,
    send1, recv1, send2, recv2, send7, recv7, send3, recv3, send4, recv4, send5, recv5, send6, recv6,
):
    orig = lax.axis_index("orig")
    link = lax.axis_index("link")
    rows = obs_ref.shape[1]
    members = term_ref.shape[1]
    half = members // 2
    pairs = n_orig // 2
    parity = orig % 2
    place = orig // 2
    across = orig + 1 - 2 * parity
    side = link % 2
    twin = link + 1 - 2 * side
    ring = n_orig * n_link // 2
    rank = (link // 2) * n_orig + orig
    owners = min(ring, half // 8)
    piece = half // owners

    def device_of(other):
        return (other % n_orig, (other // n_orig) * 2 + side)

    load_small = [
        pltpu.make_async_copy(source, target, small_sem.at[index])
        for index, (source, target) in enumerate(
            [
                (ids_hbm, ids_ref), (targets_hbm, targets_ref), (counts_hbm, counts_ref),
                (obs_hbm, obs_ref), (var_hbm, var_ref),
            ]
        )
    ]
    for copy in load_small[:3]:
        copy.start()
    load_states = pltpu.make_async_copy(states_hbm, states_ref, states_sem)
    load_states.start()

    def load_tiles(index):
        part = tiles_ref.shape[2]
        return pltpu.make_async_copy(
            tiles_hbm.at[:, pl.ds(index * part, part)], tiles_ref.at[index], tiles_sem.at[index]
        )

    for index in range(cuts):
        load_tiles(index).start()
    for copy in load_small[3:]:
        copy.start()
    near = place % 2
    far = place // 2
    n_far = pairs // 2
    barrier = pltpu.get_barrier_semaphore()

    def greet(other_orig, other_link):
        pl.semaphore_signal(barrier, inc=1, device_id=(other_orig, other_link), device_id_type=MESH)

    greet(across, link)
    greet(2 * (far * 2 + 1 - near) + parity, link)
    repeat(n_far - 1, lambda step: greet(2 * (xor(far, step + 1, n_far) * 2 + near) + parity, link))
    repeat(n_link - 1, lambda step: greet(orig, (link + step + 1) % n_link))

    slots = ids_ref.shape[0]
    blocks = counts_ref.shape[0]
    block_rows = states_ref.shape[0] // blocks
    link_rows = tiles_ref.shape[2] * cuts
    load_small[0].wait()
    load_small[1].wait()
    sort_slots(ids_ref, targets_ref, packed_ref, tiles_ref.shape[1], rows * n_orig // link_rows)
    move_table = pltpu.make_async_copy(packed_ref, table_ref, table_sem)
    move_table.start()
    for prefix_ref in (even_ref, odd_ref):
        prefix_ref[...] = jnp.zeros(prefix_ref.shape, F32)
    position = lax.broadcasted_iota(jnp.int32, (block_rows, members), 0)
    term_ref[...] = jnp.zeros_like(term_ref)
    load_small[2].wait()
    load_states.wait()

    def mask_block(block, carry):
        where = pl.ds(pl.multiple_of(block * block_rows, block_rows), block_rows)
        states = states_ref[where]
        states_ref[where] = jnp.where(position < counts_ref[block], states, jnp.zeros_like(states))
        return carry

    lax.fori_loop(0, blocks, mask_block, 0, unroll=2)
    for index in range(cuts):
        load_tiles(index).wait()
    move_table.wait()

    cut_rows = rows // cuts
    steps = n_far * cuts

    def owner(step, flip):
        other = xor(far, n_far - 1 - step // cuts, n_far)
        return other * 2 + (near + flip) % 2

    def term_rows(index, step):
        return pl.ds(pl.multiple_of(index * rows + step % cuts * cut_rows, cut_rows), cut_rows)

    def cut(step):
        return pl.ds(pl.multiple_of(step % cuts * cut_rows, cut_rows), cut_rows)

    def slot(step, flip):
        return step // cuts * 2 + 1 - flip

    def first(step, flip):
        index = slot(step, flip) * cuts + step % cuts
        return pltpu.make_async_remote_copy(
            src_ref=term_ref.at[term_rows(2 * owner(step, flip) + 1 - parity, step)],
            dst_ref=first_in.at[slot(step, flip), cut(step)],
            send_sem=send1.at[index], recv_sem=recv1.at[index],
            device_id=(across, link), device_id_type=MESH,
        )

    def beside(step):
        return pltpu.make_async_remote_copy(
            src_ref=sums.at[slot(step, 1), cut(step)], dst_ref=side_in.at[step // cuts, cut(step)],
            send_sem=send2.at[step], recv_sem=recv2.at[step],
            device_id=(2 * (far * 2 + 1 - near) + parity, link), device_id_type=MESH,
        )

    def beyond(step):
        return pltpu.make_async_remote_copy(
            src_ref=sums.at[slot(step, 0), cut(step)], dst_ref=far_in.at[step // cuts, cut(step)],
            send_sem=send7.at[step], recv_sem=recv7.at[step],
            device_id=(2 * owner(step, 0) + parity, link), device_id_type=MESH,
        )

    remote = steps - cuts
    lag = min(2, remote, cuts)

    def after_cut(index):
        @pl.when(index == 0)
        def _():
            pl.semaphore_wait(barrier, n_far + n_link)

        def first_start(step):
            first(step * cuts + index, 1).start()
            first(step * cuts + index, 0).start()

        repeat(n_far - 1, first_start)

    predict(table_ref, tiles_ref, states_ref, (even_ref, odd_ref), lhs_ref, term_ref, slots, after_cut)
    repeat(cuts, lambda step: first(step + remote, 1).start())
    repeat(cuts, lambda step: first(step + remote, 0).start())

    def add_first(step, flip):
        first(step, flip).wait_recv()
        sums[slot(step, flip), cut(step)] = (
            term_ref[term_rows(2 * owner(step, flip) + parity, step)] + first_in[slot(step, flip), cut(step)]
        )
        if flip:
            beside(step).start()

    def add_beside(step):
        beside(step).wait_recv()
        sums[slot(step, 0), cut(step)] = sums[slot(step, 0), cut(step)] + side_in[step // cuts, cut(step)]

    def pass_on(step):
        add_beside(step)
        beyond(step).start()

    def enter(step):
        add_first(step, 1)
        add_first(step, 0)

    repeat(lag, enter)

    def middle_step(step):
        enter(step + lag)
        pass_on(step)

    repeat(remote - lag, middle_step)
    for step in range(cuts):
        add_first(step + remote, 1)
        if step < lag:
            pass_on(step + (remote - lag))
    for step in range(cuts):
        add_first(step + remote, 0)
        add_beside(step + remote)

    def gather(step):
        beyond(step).wait_recv()
        sums[pairs - 1, cut(step)] = sums[pairs - 1, cut(step)] + far_in[step // cuts, cut(step)]

    rolled(remote, gather)

    load_small[3].wait()
    load_small[4].wait()
    predicted = sums[pairs - 1]
    turned = predicted.T
    weights = 1.0 / var_ref[...]
    mean_row = jnp.sum(turned, axis=0, keepdims=True) / members
    spread = predicted - jnp.sum(predicted, axis=1, keepdims=True) / members
    spread_t = turned - mean_row
    gram = mm3(spread_t * weights, spread)
    pull = jnp.broadcast_to(weights * (obs_ref[...] - mean_row), (8, rows))
    forcing = mm3(pull, spread)
    row = lax.broadcasted_iota(jnp.int32, (half, half), 0)
    column = lax.broadcasted_iota(jnp.int32, (half, half), 1)
    corner = gram[half:, half:]
    halves = (gram[0:half, half:], jnp.where(row <= column, gram[0:half, 0:half], corner))
    diagonal = jnp.sum(jnp.where(row == column, corner, 0.0), axis=0, keepdims=True)
    extras = (forcing[0:1, 0:half], forcing[0:1, half:], diagonal)
    for which, values in enumerate(halves):
        for index in range(owners):
            gram_ref[which, index, 0:piece] = values[index * piece : (index + 1) * piece]
            extra = extras[index] if which == 0 and index < len(extras) else jnp.zeros((1, half), F32)
            gram_ref[which, index, pl.ds(piece, 1)] = extra

    swap = pltpu.make_async_remote_copy(
        src_ref=gram_ref.at[1 - side], dst_ref=half_in,
        send_sem=send3, recv_sem=recv3, device_id=(orig, twin), device_id_type=MESH,
    )
    swap.start()
    swap.wait_recv()
    half_ref[...] = gram_ref[side] + half_in[...]

    def scatter(step):
        other = xor(rank, ring - 1 - step, ring)
        return pltpu.make_async_remote_copy(
            src_ref=half_ref.at[other], dst_ref=piece_in.at[step],
            send_sem=send4.at[step], recv_sem=recv4.at[step],
            device_id=device_of(other), device_id_type=MESH,
        )

    def spread_out(source, step, other):
        return pltpu.make_async_remote_copy(
            src_ref=piece_ref, dst_ref=final_ref.at[side, source],
            send_sem=send5.at[step], recv_sem=recv5.at[step],
            device_id=device_of(other), device_id_type=MESH,
        )

    def guarded(condition, action):
        if owners == ring:
            action()
        else:
            pl.when(condition)(action)

    def scatter_start(step):
        guarded(xor(rank, ring - 1 - step, ring) < owners, lambda: scatter(step).start())

    repeat(ring - 1, scatter_start)

    def first_end(step):
        first(step, 1).wait_send()
        first(step, 0).wait_send()
        beside(step).wait_send()

    rolled(steps, first_end)
    rolled(remote, lambda step: beyond(step).wait_send())
    swap.wait_send()


    def reduce_piece():
        def arrive(step):
            scatter(step).wait_recv()
            return piece_in[step]

        if ring <= 16:
            total = half_ref[rank]
            for step in range(ring - 1):
                total = total + arrive(step)
            piece_ref[...] = total
        else:
            piece_ref[...] = half_ref[rank]

            def add(step):
                piece_ref[...] = piece_ref[...] + arrive(step)

            repeat(ring - 1, add)
        repeat(ring - 1, lambda step: spread_out(rank, step, xor(rank, ring - 1 - step, ring)).start())
        final_ref[side, rank] = piece_ref[...]

    guarded(rank < owners, reduce_piece)

    def scatter_end(step):
        guarded(xor(rank, ring - 1 - step, ring) < owners, lambda: scatter(step).wait_send())

    rolled(ring - 1, scatter_end)
    def spread_wait(step):
        other = xor(rank, ring - 1 - step, ring)
        guarded(other < owners, lambda: spread_out(other, step, other).wait_recv())

    repeat(ring - 1, spread_wait)
    share = pltpu.make_async_remote_copy(
        src_ref=final_ref.at[side], dst_ref=final_ref.at[side],
        send_sem=send6, recv_sem=recv6, device_id=(orig, twin), device_id_type=MESH,
    )
    share.start()
    guarded(
        rank < owners,
        lambda: rolled(
            ring - 1, lambda step: spread_out(rank, step, xor(rank, ring - 1 - step, ring)).wait_send()
        ),
    )
    share.wait_recv()

    out_ref[...] = final_ref[...]


    share.wait_send()


def update_kernel(counts_hbm, final_ref, states_hbm, out_hbm, counts_ref, states_ref, done_ref, counts_sem, states_sem, done_sem, root_ref, inverse_ref):
    link = lax.axis_index("link")
    own_rows, members = done_ref.shape
    half = members // 2
    fetch = pltpu.make_async_copy(
        states_hbm.at[pl.ds(pl.multiple_of(link * own_rows, own_rows), own_rows)], states_ref, states_sem
    )
    fetch.start()
    fetch_counts = pltpu.make_async_copy(counts_hbm, counts_ref, counts_sem)
    fetch_counts.start()
    owners = final_ref.shape[1]
    piece = half // owners
    upper, mixed = [
        jnp.concatenate([final_ref[which, index, 0:piece] for index in range(owners)], axis=0) for which in range(2)
    ]
    first, second, diagonal = [final_ref[0, index, pl.ds(piece, 1)] for index in range(3)]
    row = lax.broadcasted_iota(jnp.int32, (half, half), 0)
    column = lax.broadcasted_iota(jnp.int32, (half, half), 1)
    turned = mixed.T
    head = jnp.where(row <= column, mixed, turned)
    tail = jnp.where(row == column, diagonal, jnp.where(row > column, mixed, turned))
    gram = jnp.concatenate(
        [jnp.concatenate([head, upper], axis=1), jnp.concatenate([upper.T, tail], axis=1)], axis=0
    )
    forcing = jnp.concatenate([first, second], axis=1)
    high, low = split(transform_of(gram, forcing, root_ref, inverse_ref))
    fetch.wait()
    fetch_counts.wait()
    block_rows = states_hbm.shape[0] // counts_ref.shape[0]
    blocks = own_rows // block_rows
    position = lax.broadcasted_iota(jnp.int32, (block_rows, members), 0)

    def store(index):
        where = slice(index * block_rows, (index + 1) * block_rows)
        return pltpu.make_async_copy(done_ref.at[where], out_hbm.at[where], done_sem.at[index])

    for index in range(blocks):
        states = states_ref[index * block_rows : (index + 1) * block_rows]
        updated = jnp.dot(
            jnp.concatenate([states, states], axis=1), jnp.concatenate([low, high], axis=0), preferred_element_type=F32
        )
        living = position < counts_ref[link * blocks + index]
        done_ref[index * block_rows : (index + 1) * block_rows] = jnp.where(
            living, updated, states.astype(F32)
        ).astype(BF16)
        store(index).start()
    for index in range(blocks):
        store(index).wait()


def per_device(background, live_counts, patterns, pattern_ids, link_targets, counts_obs, obs_var):
    n_orig = lax.axis_size("orig")
    n_link = lax.axis_size("link")
    states_dev, members = background.shape
    blocks_dev = live_counts.shape[0]
    block_rows = states_dev // blocks_dev
    link_rows = patterns.shape[2]
    rows = counts_obs.shape[1]
    link_blocks = rows * n_orig // link_rows
    vmem = pl.BlockSpec(memory_space=pltpu.VMEM)
    hbm = pl.BlockSpec(memory_space=pl.ANY)
    dma = pltpu.SemaphoreType.DMA
    grant = pltpu.CompilerParams(vmem_limit_bytes=WIDE_GRANT)
    pairs = n_orig // 2
    ring = n_orig * n_link // 2
    half = members // 2
    owners = min(ring, half // 8)
    packed = (owners, half // owners + 1, half)
    cuts = CUTS if rows == link_rows else 1
    slots = pattern_ids.shape[2]
    table_rows = pl.cdiv(slots + link_blocks, 8) * 8
    steps = pairs // 2 * cuts
    gram = pl.pallas_call(
        functools.partial(gram_kernel, n_orig, n_link, cuts),
        out_shape=pltpu.VMEM((2,) + packed, F32),
        in_specs=[hbm] * 7,
        out_specs=vmem,
        scratch_shapes=[
            pltpu.VMEM((slots, 1, blocks_dev), jnp.int32),
            pltpu.VMEM((slots, 1, blocks_dev), jnp.int32),
            pltpu.SMEM((blocks_dev,), jnp.int32),
            pltpu.VMEM((1, rows), F32),
            pltpu.VMEM((1, rows), F32),
            dma((5,)),
            pltpu.VMEM((cuts, patterns.shape[1], link_rows // cuts, block_rows), BF16),
            pltpu.VMEM((states_dev, members), BF16),
            dma((cuts,)),
            dma,
            pltpu.VMEM((16, link_rows // cuts, block_rows), F32),
            pltpu.VMEM((16, link_rows // cuts, block_rows), F32),
            pltpu.VMEM((2 * SPAN, link_blocks * link_rows // cuts, block_rows), BF16),
            pltpu.VMEM((table_rows, 128), jnp.int32),
            pltpu.SMEM((table_rows, 128), jnp.int32),
            dma,
            pltpu.VMEM((link_blocks * link_rows, members), F32),
            pltpu.VMEM((pairs, rows, members), F32),
            pltpu.VMEM((pairs, rows, members), F32),
            pltpu.VMEM((pairs // 2, rows, members), F32),
            pltpu.VMEM((pairs // 2, rows, members), F32),
            pltpu.VMEM((2,) + packed, F32),
            pltpu.VMEM(packed, F32),
            pltpu.VMEM(packed, F32),
            pltpu.VMEM((ring - 1,) + packed[1:], F32),
            pltpu.VMEM(packed[1:], F32),
            pltpu.VMEM((2,) + packed, F32),
            dma((2 * steps,)), dma((2 * steps,)),
            dma((steps,)), dma((steps,)),
            dma((steps,)), dma((steps,)),
            dma, dma,
            dma((ring,)), dma((ring,)),
            dma((ring,)), dma((ring,)),
            dma, dma,
        ],
        compiler_params=pltpu.CompilerParams(
            collective_id=0, has_side_effects=True, vmem_limit_bytes=WIDE_GRANT
        ),
    )(
        jnp.transpose(pattern_ids, (2, 0, 1)), jnp.transpose(link_targets, (2, 0, 1)), live_counts,
        patterns[0], background, counts_obs, obs_var,
    )
    own_rows = states_dev // n_link
    return pl.pallas_call(
        update_kernel,
        out_shape=jax.ShapeDtypeStruct((own_rows, members), BF16),
        in_specs=[hbm, vmem, hbm],
        out_specs=hbm,
        scratch_shapes=[
            pltpu.SMEM((blocks_dev,), jnp.int32),
            pltpu.VMEM((own_rows, members), BF16),
            pltpu.VMEM((own_rows, members), BF16),
            dma,
            dma,
            dma((own_rows // block_rows,)),
            pltpu.VMEM((members, members), F32),
            pltpu.VMEM((members, members), F32),
        ],
        compiler_params=grant,
    )(live_counts, pltpu.with_memory_space_constraint(gram, pltpu.VMEM), background)


def solution(mesh):
    placed = (
        P("orig", None),
        P("orig"),
        P("link", "orig", None, None),
        P("link", "orig", None),
        P("link", "orig", None),
        P("link", "orig"),
        P("link", "orig"),
    )
    return jax.shard_map(
        per_device, mesh=mesh, in_specs=placed, out_specs=P(("orig", "link"), None), check_vma=False
    )
```
